32 devices in a mesh: lon: 8 (over z, x), lat: 4 (over y, core).
Axes of the slice: x: 2, y: 2, z: 4, core: 2. Of those that a mesh axis runs over, the one named last changes fastest.
Arguments:
- tracers: float32 [40, 8, 32, 1024], P(None, None, 'lat', 'lon'), may hold values from -6 to 6
- kmt: int32 [32, 1024], P('lat', 'lon'), may hold values from 0 to 8
Outputs:
- updated: float32 [40, 8, 32, 1024], P(None, None, 'lat', 'lon')
The draws below stay inside these ranges and needn't reach their ends.
Inputs may be any that keep to these rules, and one draw needn't show every extreme that they name: Level k of column (j, i) is ocean exactly when k < kmt[j, i].
All inputs are finite; a program needn't handle non-finite values.
Results may differ from the reference program's by a relative error of at most 0.00002.
Values sent between devices are 32-bit elements; how exact they have to be, the bound alone decides.
A program may use at most 64 MiB of HBM per device.

```python
import jax
import jax.numpy as jnp
from jax import lax

NTRAC = 40
NZ = 8
NY = 32
NX = 1024


def with_ends(array, rng, least, largest):
    longest = array.shape.index(max(array.shape))
    spots = []
    for shift in (0, 1):
        where = [jax.random.randint(jax.random.fold_in(rng, axis), (), 0, length) for axis, length in enumerate(array.shape)]
        where[longest] = (where[longest] + shift) % array.shape[longest]
        spots.append(tuple(where))
    return array.at[spots[0]].set(least).at[spots[1]].set(largest)


def block_scale(key, extent, pieces, least, largest):
    level, own = 1.0, jax.random.fold_in(key, 6)
    for dim, blocks in pieces:
        heights = jnp.exp(jax.random.uniform(jax.random.fold_in(own, dim), (blocks,), jnp.float32, least / len(pieces), largest / len(pieces)))
        level = level * jnp.repeat(heights, extent[dim] // blocks).reshape([-1 if axis == dim else 1 for axis in range(len(extent))])
    return level


def normal_values(rng, dims, scale, bound, pieces=(), kind=jnp.bfloat16):
    level = block_scale(rng, dims, pieces, -0.22, 0.18) if pieces else 1.0
    values = jax.random.normal(rng, dims, jnp.float32) * scale * level
    return jnp.minimum(jnp.maximum(values, -bound), bound).astype(kind)


def setup_inputs(seed: int = 0) -> dict:
    streams_of = jax.random.split(jax.random.key(seed), 3)
    tracers = normal_values(streams_of[0], (NTRAC, NZ, NY, NX), 1.0, 6.0, ((2, 4), (3, 8)), jnp.float32)
    kmt = with_ends(jax.random.randint(streams_of[1], (NY, NX), 0, NZ + 1), jax.random.fold_in(streams_of[1], 1), 0, NZ).astype(jnp.int32)
    return dict(tracers=tracers, kmt=kmt)


THERMAL = 0.2
HALINE = 0.8
REDI_COEF = 0.1
SKEW_COEF = 0.05
SLOPE_MAX = 0.6
SLOPE_WIDTH = 0.2


def taper(slope):
    return slope * 0.5 * (1.0 + jnp.tanh((SLOPE_MAX - jnp.abs(slope)) / SLOPE_WIDTH))


def pad_levels(values):
    zero_layer = jnp.zeros_like(values[..., :1, :, :])
    return jnp.concatenate([zero_layer, values, zero_layer], axis=-3)


def slope_fields(density, wet_mask):
    level_mask = wet_mask[1:] * wet_mask[:-1]
    strat = (density[1:] - density[:-1]) * level_mask
    strat_pad = pad_levels(strat)
    strat_cell = 0.5 * (strat_pad[:-1] + strat_pad[1:])
    east_mask = wet_mask[:, 1:-1, :-1] * wet_mask[:, 1:-1, 1:]
    north_mask = wet_mask[:, :-1, 1:-1] * wet_mask[:, 1:, 1:-1]
    grad_east = (density[:, 1:-1, 1:] - density[:, 1:-1, :-1]) * east_mask
    strat_east = 0.5 * (strat_cell[:, 1:-1, 1:] + strat_cell[:, 1:-1, :-1])
    slope_x = taper(grad_east / jnp.maximum(strat_east, 1.0))
    grad_north = (density[:, 1:, 1:-1] - density[:, :-1, 1:-1]) * north_mask
    strat_north = 0.5 * (strat_cell[:, 1:, 1:-1] + strat_cell[:, :-1, 1:-1])
    slope_y = taper(grad_north / jnp.maximum(strat_north, 1.0))
    cell_x = 0.5 * (slope_x[..., :-1] + slope_x[..., 1:])
    cell_y = 0.5 * (slope_y[:, :-1, :] + slope_y[:, 1:, :])
    level_x = 0.5 * (cell_x[:-1] + cell_x[1:])
    level_y = 0.5 * (cell_y[:-1] + cell_y[1:])
    return (level_mask, east_mask, north_mask, slope_x, slope_y, level_x, level_y)


def tracer_step(field, fields):
    level_mask, east_mask, north_mask, slope_x, slope_y, level_x, level_y = fields
    vert_diff = (field[..., 1:, :, :] - field[..., :-1, :, :]) * level_mask
    vert_pad = pad_levels(vert_diff)
    vert_cell = 0.5 * (vert_pad[..., :-1, :, :] + vert_pad[..., 1:, :, :])
    grad_x = (field[..., 1:-1, 1:] - field[..., 1:-1, :-1]) * east_mask
    grad_y = (field[..., 1:, 1:-1] - field[..., :-1, 1:-1]) * north_mask
    flux_x = -(REDI_COEF * grad_x + (REDI_COEF - SKEW_COEF) * slope_x
               * 0.5 * (vert_cell[..., 1:-1, 1:] + vert_cell[..., 1:-1, :-1])) * east_mask
    flux_y = -(REDI_COEF * grad_y + (REDI_COEF - SKEW_COEF) * slope_y
               * 0.5 * (vert_cell[..., 1:, 1:-1] + vert_cell[..., :-1, 1:-1])) * north_mask
    cell_gx = 0.5 * (grad_x[..., :-1] + grad_x[..., 1:])
    cell_gy = 0.5 * (grad_y[..., :-1, :] + grad_y[..., 1:, :])
    level_gx = 0.5 * (cell_gx[..., :-1, :, :] + cell_gx[..., 1:, :, :])
    level_gy = 0.5 * (cell_gy[..., :-1, :, :] + cell_gy[..., 1:, :, :])
    flux_z = -((REDI_COEF + SKEW_COEF) * (level_x * level_gx + level_y * level_gy)
               + REDI_COEF * (level_x * level_x + level_y * level_y) * vert_diff[..., 1:-1, 1:-1]) * level_mask[:, 1:-1, 1:-1]
    flux_pad = pad_levels(flux_z)
    tendency = -((flux_x[..., 1:] - flux_x[..., :-1]) + (flux_y[..., 1:, :] - flux_y[..., :-1, :])
                 + (flux_pad[..., 1:, :, :] - flux_pad[..., :-1, :, :]))
    return field[..., 1:-1, 1:-1] + tendency


def extend(field):
    beside_all = jnp.concatenate([field[..., -1:], field, field[..., :1]], axis=-1)
    north_row = beside_all[..., -1:, ::-1]
    south_row = jnp.zeros_like(beside_all[..., :1, :])
    return jnp.concatenate([south_row, beside_all, north_row], axis=-2)


def reference(tracers, kmt):
    level_index = lax.broadcasted_iota(jnp.int32, (NZ, NY, NX), 0)
    wet_mask = (level_index < kmt[None]).astype(jnp.float32)
    density = HALINE * tracers[1] - THERMAL * tracers[0]
    fields = slope_fields(extend(density), extend(wet_mask))
    return lax.map(lambda single: tracer_step(extend(single), fields), tracers)
```

```python
import functools

import jax
import jax.numpy as jnp
from jax import lax
from jax.experimental import pallas as pl
from jax.experimental.pallas import tpu as pltpu
from jax.sharding import PartitionSpec as P

THERMAL = 0.2
HALINE = 0.8
REDI = 0.1
SKEW = 0.05
SLOPE_MAX = 0.6
SLOPE_WIDTH = 0.2

MESH = pl.DeviceIdType.MESH
TOGETHER = 2
QUAD = 4
C, E, W, N, S = range(5)


def taper(slope):
    return slope * 0.5 * (1.0 + jnp.tanh((SLOPE_MAX - jnp.abs(slope)) / SLOPE_WIDTH))


def column(rho, wet, up, dn):
    hi = wet * dn(wet)
    strat = (dn(rho) - rho) * hi
    return rho, wet, hi, up(hi), 0.5 * (strat + up(strat))


def line(c, p, m, up, dn):
    c_rho, c_wet, c_hi, c_lo, c_cell = c
    p_rho, p_wet, p_hi, p_lo, p_cell = p
    m_rho, m_wet, m_hi, m_lo, m_cell = m
    mp, mm = c_wet * p_wet, c_wet * m_wet
    sp = taper((p_rho - c_rho) * mp / jnp.maximum(0.5 * (p_cell + c_cell), 1.0))
    sm = taper((c_rho - m_rho) * mm / jnp.maximum(0.5 * (m_cell + c_cell), 1.0))
    cx = 0.5 * (sp + sm)
    sw = 0.5 * (cx + dn(cx))
    fh = ((REDI + SKEW) * 0.25) * sw * c_hi
    zh = REDI * (sw * sw) * c_hi
    fl, zl = up(fh), up(zh)
    pp = ((REDI - SKEW) * 0.25) * sp * mp
    pm = -((REDI - SKEW) * 0.25) * sm * mm
    own_p, own_m = mp * (fh - fl), mm * (fl - fh)
    mph, mmh = dn(mp) * fh, dn(mm) * fh
    mpl, mml = up(mp) * fl, up(mm) * fl
    q = pp + pm
    return (
        (mpl - mml - q * c_lo + zl,
         q * (c_lo - c_hi) - REDI * (mp + mm) - (own_p + own_m) - (zh + zl),
         mmh - mph + q * c_hi + zh),
        (-pp * p_lo - mpl, REDI * mp + pp * (p_lo - p_hi) + own_p, pp * p_hi + mph),
        (mml - pm * m_lo, REDI * mm + pm * (m_lo - m_hi) + own_m, pm * m_hi - mmh),
    )


def total(terms):
    result = terms[0]
    for term in terms[1:]:
        result = result + term
    return result


def kernel(
    sizes, x_ref, kmt_ref, out_ref,
    xv, kmt_int, coef, wcol, ecol, inner_w, inner_e, west, east, from_n, from_s, kmt_n, kmt_s,
    load_sem, send_sem, recv_sem,
):
    tracers, levels, rows, lanes, n_lon, n_lat = sizes
    lon, lat = lax.axis_index("lon"), lax.axis_index("lat")
    at_top = lat == n_lat - 1
    below_top = jnp.logical_not(at_top)
    inner = lat > 0
    at_bottom = jnp.logical_not(inner)
    e_dev = (lax.rem(lon + 1, n_lon), lat)
    w_dev = (lax.rem(lon + n_lon - 1, n_lon), lat)
    n_dev, s_dev = (lon, lat + 1), (lon, lat - 1)
    fold_dev = (n_lon - 1 - lon, lat)
    tiles = tracers * levels
    plane = levels * rows
    quad = lanes // QUAD
    head = tiles % lanes
    regs = tiles // lanes + 1
    quads = tiles // quad
    per_piece = head // quad
    piece = head
    pieces = tiles // piece
    bounds = [0] + [head + lanes * j for j in range(regs)]

    barrier = pltpu.get_barrier_semaphore()

    def greet(dev):
        pl.semaphore_signal(barrier, inc=1, device_id=dev, device_id_type=MESH)

    with jax.named_scope("greet"):
        greet(e_dev)
        greet(w_dev)

        @pl.when(at_top)
        def _():
            greet(fold_dev)

        @pl.when(below_top)
        def _():
            greet(n_dev)

        @pl.when(inner)
        def _():
            greet(s_dev)

    load_kmt = pltpu.make_async_copy(kmt_ref, kmt_int, load_sem.at[pieces])
    load_kmt.start()
    loads = []
    for i in range(pieces):
        span = pl.ds(i * piece, piece)
        copy = pltpu.make_async_copy(x_ref.at[span], xv.at[span], load_sem.at[i])
        copy.start()
        loads.append(copy)
    flat = xv.reshape(tiles * rows, lanes)

    zeros = jnp.zeros((rows, lanes), jnp.float32)
    lane = lax.broadcasted_iota(jnp.int32, (rows, lanes), 1)
    row = lax.broadcasted_iota(jnp.int32, (rows, lanes), 0)
    spot = lane // QUAD
    part = lane // quad

    def pick(value, index):
        return jnp.take_along_axis(value, index, axis=1)

    def pack_quad(g):
        acc = zeros
        for q in range(quad):
            value = flat[pl.ds((g * quad + q) * rows, rows), :]
            value = pltpu.roll(value, (QUAD * q + QUAD // 2) % lanes, 1)
            acc = value if q == 0 else jnp.where(spot == q, value, acc)
        return acc

    def spread(group, off):
        index = QUAD * (lane % quad) + off
        acc = None
        for g, value in enumerate(group):
            value = pick(value, index)
            acc = value if g == 0 else jnp.where(part == g, value, acc)
        return acc

    def send(src, dst, s, r, dev):
        return pltpu.make_async_remote_copy(
            src_ref=src, dst_ref=dst, send_sem=send_sem.at[s], recv_sem=recv_sem.at[r],
            device_id=dev, device_id_type=MESH,
        )

    r_w, r_e = 4, 4 + regs
    first_row, last_row = xv.at[:, 0, :], xv.at[:, rows - 1, :]
    fold = [send(kmt_int, kmt_n, 0, 0, fold_dev), send(last_row, from_n, 1, 1, fold_dev)]
    to_n = [send(kmt_int, kmt_s, 0, 2, n_dev), send(last_row, from_s, 1, 3, n_dev)]
    to_s = [send(kmt_int, kmt_n, 2, 0, s_dev), send(first_row, from_n, 3, 1, s_dev)]
    to_e, to_w = [], []
    for j in range(regs):
        span = pl.ds(j * rows, rows)
        to_e.append(send(ecol.at[span], west.at[span], 4, r_w + j, e_dev))
        to_w.append(send(wcol.at[span], east.at[span], 5, r_e + j, w_dev))
    all_e = send(ecol, west, 4, r_w, e_dev)
    all_w = send(wcol, east, 5, r_e, w_dev)

    def send_rows(i):
        @pl.when(at_top)
        def _():
            fold[i].start()

        @pl.when(below_top)
        def _():
            to_n[i].start()

        @pl.when(inner)
        def _():
            to_s[i].start()

    packed = []

    def pack_reg(j):
        first, last = bounds[j] // quad, bounds[j + 1] // quad
        group = []
        for g in range(first, last):
            if g % per_piece == 0:
                loads[g // per_piece].wait()
            group.append(pack_quad(g))
        e, w = spread(group, 1), spread(group, 2)
        if j == 0:
            e = jnp.where(lane >= head, jnp.broadcast_to(kmt_own[:, lanes - 1 :], (rows, lanes)), e)
            w = jnp.where(lane >= head, jnp.broadcast_to(kmt_own[:, :1], (rows, lanes)), w)
        ecol[pl.ds(j * rows, rows), :] = e
        wcol[pl.ds(j * rows, rows), :] = w
        packed.append(group)

    with jax.named_scope("pack0"):
        load_kmt.wait()
        kmt_own = kmt_int[...].astype(jnp.float32)
        pack_reg(0)

    with jax.named_scope("barrier"):

        @pl.when(inner)
        def _():
            pl.semaphore_wait(barrier, 4)

        @pl.when(at_bottom)
        def _():
            pl.semaphore_wait(barrier, 3)

    with jax.named_scope("pack"):
        send_rows(0)
        to_e[0].start()
        to_w[0].start()
        for j in range(1, regs):
            pack_reg(j)
            to_e[j].start()
            to_w[j].start()
        send_rows(1)

    with jax.named_scope("inner"):
        for j in range(regs):
            inner_e[pl.ds(j * rows, rows), :] = spread(packed[j], 0)
            inner_w[pl.ds(j * rows, rows), :] = spread(packed[j], 3)

        @pl.when(at_bottom)
        def _():
            kmt_s[...] = jnp.zeros((rows, lanes), jnp.int32)
            for t in range(tracers):
                from_s[pl.ds(t * levels, levels), :] = jnp.zeros((levels, lanes), jnp.float32)

    def put(d, dk, k, value):
        coef[pl.ds(((d * 3 + dk) * levels + k) * rows, rows), :] = value

    def piece_of(d, dk, k):
        return coef[pl.ds(((d * 3 + dk) * levels + k) * rows, rows), :]

    with jax.named_scope("coefs"):
        none = jnp.zeros((1, rows, lanes), jnp.float32)

        def up3(v):
            return jnp.concatenate([none, v[:-1]], axis=0)

        def dn3(v):
            return jnp.concatenate([v[1:], none], axis=0)

        def shifted(v, by, axis):
            return jnp.stack([pltpu.roll(v[k], by, axis) for k in range(levels)])

        own_rho = jnp.stack(
            [HALINE * flat[pl.ds(plane + k * rows, rows), :] - THERMAL * flat[pl.ds(k * rows, rows), :]
             for k in range(levels)]
        )
        own_wet = jnp.stack([(kmt_own > float(k)).astype(jnp.float32) for k in range(levels)])
        c3 = column(own_rho, own_wet, up3, dn3)

        def moved(by, axis):
            return tuple(shifted(v, by, axis) for v in c3)

        mid_lane = jnp.logical_and(lane > 0, lane < lanes - 1)
        xc, xe, xw = line(c3, moved(lanes - 1, 1), moved(1, 1), up3, dn3)
        for dk in range(3):
            for k in range(levels):
                put(E, dk, k, jnp.where(mid_lane, xe[dk][k], 0.0))
                put(W, dk, k, jnp.where(mid_lane, xw[dk][k], 0.0))
                put(C, dk, k, jnp.where(mid_lane, xc[dk][k], 0.0))
        mid_row = jnp.logical_and(row > 0, row < rows - 1)
        yc, yn, ys = line(c3, moved(rows - 1, 0), moved(1, 0), up3, dn3)
        for dk in range(3):
            for k in range(levels):
                put(N, dk, k, jnp.where(mid_row, yn[dk][k], 0.0))
                put(S, dk, k, jnp.where(mid_row, ys[dk][k], 0.0))
                both = piece_of(C, dk, k) + jnp.where(mid_row, yc[dk][k], 0.0)
                put(C, dk, k, both + 1.0 if dk == 1 else both)

    with jax.named_scope("main"):

        @pl.loop(0, tracers // TOGETHER)
        def _(i):
            fields = []
            for u in range(TOGETHER):
                base = pl.multiple_of((i * TOGETHER + u) * plane, rows)
                field = []
                for k in range(levels):
                    own = flat[pl.ds(base + k * rows, rows), :]
                    field.append((
                        own, pltpu.roll(own, lanes - 1, 1), pltpu.roll(own, 1, 1),
                        pltpu.roll(own, rows - 1, 0), pltpu.roll(own, 1, 0),
                    ))
                fields.append(field)
            for k in range(levels):
                sums = [None] * TOGETHER
                for d in range(5):
                    for dk in range(3):
                        if not 0 <= k + dk - 1 < levels:
                            continue
                        c = piece_of(d, dk, k)
                        for u in range(TOGETHER):
                            term = c * fields[u][k + dk - 1][d]
                            sums[u] = term if sums[u] is None else sums[u] + term
                for u in range(TOGETHER):
                    base = pl.multiple_of((i * TOGETHER + u) * plane, rows)
                    out_ref[pl.ds(base + k * rows, rows), :] = sums[u]

    level = lax.broadcasted_iota(jnp.int32, (levels, lanes), 0)
    level_f = level.astype(jnp.float32)

    def up_s(v):
        return jnp.where(level == 0, 0.0, pltpu.roll(v, 1, 0))

    def dn_s(v):
        return jnp.where(level == levels - 1, 0.0, pltpu.roll(v, levels - 1, 0))

    def at_row(t, r):
        return flat[pl.ds(t * plane + r, levels, stride=rows), :]

    def row_column(t0, t1, kmt):
        wet = (jnp.broadcast_to(kmt, (levels, lanes)) > level_f).astype(jnp.float32)
        return column(HALINE * t1 - THERMAL * t0, wet, up_s, dn_s)

    def own_row(r):
        return row_column(at_row(0, r), at_row(1, r), kmt_own[r : r + 1, :])

    def fix_rows(source, kmt_row, r, r_in, north, turn):
        def halo(t):
            h = source[pl.ds(t * levels, levels), :]
            return pick(h, lanes - 1 - lane) if turn else h

        k = jnp.broadcast_to(kmt_row, (rows, lanes)).astype(jnp.float32)
        k = (pick(k, lanes - 1 - lane) if turn else k)[:1, :]
        out_c, in_c = row_column(halo(0), halo(1), k), own_row(r_in)
        p, m = (out_c, in_c) if north else (in_c, out_c)
        cc, cp, cm = line(own_row(r), p, m, up_s, dn_s)
        c_out, c_in = (cp, cm) if north else (cm, cp)
        table = (cc, c_out, c_in)
        lo = [pltpu.roll(c[0], levels - 1, 0) for c in table]
        mid = [c[1] for c in table]
        hi = [pltpu.roll(c[2], 1, 0) for c in table]

        @pl.loop(0, tracers // 8)
        def _(i):
            for u in range(8):
                t = i * 8 + u
                values = (at_row(t, r), halo(t), at_row(t, r_in))
                above = total([c * v for c, v in zip(lo, values)])
                same = total([c * v for c, v in zip(mid, values)])
                below = total([c * v for c, v in zip(hi, values)])
                place = pl.ds(t * plane + r, levels, stride=rows)
                out_ref[place, :] = (
                    out_ref[place, :] + same + pltpu.roll(above, 1, 0) + pltpu.roll(below, levels - 1, 0)
                )

    def fix_n(turn):
        for copy in fold:
            copy.wait_recv()
        at = rows - 1 if turn else 0
        fix_rows(from_n, kmt_n[at : at + 1, :], rows - 1, rows - 2, True, turn)

    with jax.named_scope("fixs"):

        @pl.when(inner)
        def _():
            for copy in to_n:
                copy.wait_recv()

        fix_rows(from_s, kmt_s[rows - 1 : rows, :], 0, 1, False, False)

    with jax.named_scope("fixn"):

        @pl.when(below_top)
        def _():
            fix_n(False)

    deep = lane % levels

    def up_l(v):
        return jnp.where(deep == 0, 0.0, pltpu.roll(v, 1, 1))

    def dn_l(v):
        return jnp.where(deep == levels - 1, 0.0, pltpu.roll(v, lanes - 1, 1))

    def lane_column(reg, kmt):
        rho = pick(HALINE * pltpu.roll(reg, lanes - levels, 1) - THERMAL * reg, deep)
        wet = (kmt > deep.astype(jnp.float32)).astype(jnp.float32)
        return column(rho, wet, up_l, dn_l)

    def own_kmt(at):
        return jnp.broadcast_to(kmt_own[:, at : at + 1], (rows, lanes))

    def reg_of(ref, j):
        return ref[pl.ds(j * rows, rows), :]

    def halo_column(ref):
        reg = reg_of(ref, 0)
        return lane_column(reg, jnp.broadcast_to(reg[:, head : head + 1], (rows, lanes)))

    with jax.named_scope("fixc"):
        ends = jnp.logical_or(lane == 0, lane == lanes - 1)
        even = lane % 2 == 0
        w_own = lane_column(reg_of(wcol, 0), own_kmt(0))
        w_in = lane_column(reg_of(inner_w, 0), own_kmt(1))
        e_own = lane_column(reg_of(ecol, 0), own_kmt(lanes - 1))
        e_in = lane_column(reg_of(inner_e, 0), own_kmt(lanes - 2))
        to_e[0].wait_recv()
        to_w[0].wait_recv()
        wc, wp, wm = line(w_own, w_in, halo_column(west), up_l, dn_l)
        ec, ep, em = line(e_own, halo_column(east), e_in, up_l, dn_l)

        def side(table, values):
            above = total([pltpu.roll(c[0], lanes - 1, 1) * v for c, v in zip(table, values)])
            same = total([c[1] * v for c, v in zip(table, values)])
            below = total([pltpu.roll(c[2], 1, 1) * v for c, v in zip(table, values)])
            return same + pltpu.roll(above, 1, 1) + pltpu.roll(below, lanes - 1, 1)

        for j in range(regs):
            if j:
                to_e[j].wait_recv()
                to_w[j].wait_recv()
            w = side((wc, wp, wm), (reg_of(wcol, j), reg_of(inner_w, j), reg_of(west, j)))
            e = side((ec, ep, em), (reg_of(ecol, j), reg_of(east, j), reg_of(inner_e, j)))
            e = pltpu.roll(e, lanes - 1, 1)
            mixed = (jnp.where(even, w, e), jnp.where(even, e, w))
            for q in range(bounds[j + 1] - bounds[j]):
                add = pltpu.roll(mixed[q % 2], (lanes - q) % lanes, 1)
                place = pl.ds((bounds[j] + q) * rows, rows)
                out_ref[place, :] = out_ref[place, :] + jnp.where(ends, add, 0.0)

    with jax.named_scope("fixtop"):

        @pl.when(at_top)
        def _():
            fix_n(True)

    with jax.named_scope("end"):
        for i in range(2):
            fold[i].wait_send()

            @pl.when(inner)
            def _():
                to_s[i].wait_send()

        all_e.wait_send()
        all_w.wait_send()


def solution(mesh):
    n_lon, n_lat = mesh.shape["lon"], mesh.shape["lat"]

    def local(tracers, kmt):
        nt, levels, rows, lanes = tracers.shape
        tiles = nt * levels
        regs = tiles // lanes + 1
        assert levels == rows and tiles % lanes and lanes % (tiles % lanes) == 0

        def vmem(*shape):
            return pltpu.VMEM(shape, jnp.float32)

        out = pl.pallas_call(
            functools.partial(kernel, (nt, levels, rows, lanes, n_lon, n_lat)),
            out_shape=pltpu.VMEM((tiles * rows, lanes), jnp.float32),
            in_specs=[pl.BlockSpec(memory_space=pltpu.HBM), pl.BlockSpec(memory_space=pltpu.HBM)],
            out_specs=pl.BlockSpec(memory_space=pltpu.VMEM),
            scratch_shapes=[
                vmem(tiles, rows, lanes),
                pltpu.VMEM((rows, lanes), jnp.int32),
                vmem(15 * levels * rows, lanes),
            ]
            + [vmem(regs * rows, lanes)] * 6
            + [vmem(tiles, lanes)] * 2
            + [pltpu.VMEM((rows, lanes), jnp.int32)] * 2
            + [
                pltpu.SemaphoreType.DMA((tiles // (tiles % lanes) + 1,)),
                pltpu.SemaphoreType.DMA((6,)),
                pltpu.SemaphoreType.DMA((4 + 2 * regs,)),
            ],
            compiler_params=pltpu.CompilerParams(collective_id=0, has_side_effects=True),
        )(tracers.reshape(tiles, rows, lanes), kmt)
        return out.reshape(nt, levels, rows, lanes)

    return jax.shard_map(
        local,
        mesh=mesh,
        in_specs=(P(None, None, "lat", "lon"), P("lat", "lon")),
        out_specs=P(None, None, "lat", "lon"),
        check_vma=False,
    )
```

```python
import functools

import jax
import jax.numpy as jnp
from jax import lax
from jax.experimental import pallas as pl
from jax.experimental.pallas import tpu as pltpu
from jax.sharding import PartitionSpec as P

THERMAL = 0.2
HALINE = 0.8
REDI = 0.1
SKEW = 0.05
SLOPE_MAX = 0.6
SLOPE_WIDTH = 0.2

MESH = pl.DeviceIdType.MESH
TOGETHER = 2
C, E, W, N, S = range(5)


def taper(slope):
    return slope * 0.5 * (1.0 + jnp.tanh((SLOPE_MAX - jnp.abs(slope)) / SLOPE_WIDTH))


def column(rho, wet, up, dn):
    hi = wet * dn(wet)
    strat = (dn(rho) - rho) * hi
    return rho, wet, hi, up(hi), 0.5 * (strat + up(strat))


def line(c, p, m, up, dn):
    c_rho, c_wet, c_hi, c_lo, c_cell = c
    p_rho, p_wet, p_hi, p_lo, p_cell = p
    m_rho, m_wet, m_hi, m_lo, m_cell = m
    mp, mm = c_wet * p_wet, c_wet * m_wet
    sp = taper((p_rho - c_rho) * mp / jnp.maximum(0.5 * (p_cell + c_cell), 1.0))
    sm = taper((c_rho - m_rho) * mm / jnp.maximum(0.5 * (m_cell + c_cell), 1.0))
    cx = 0.5 * (sp + sm)
    sw = 0.5 * (cx + dn(cx))
    fh = ((REDI + SKEW) * 0.25) * sw * c_hi
    zh = REDI * (sw * sw) * c_hi
    fl, zl = up(fh), up(zh)
    pp = ((REDI - SKEW) * 0.25) * sp * mp
    pm = -((REDI - SKEW) * 0.25) * sm * mm
    own_p, own_m = mp * (fh - fl), mm * (fl - fh)
    mph, mmh = dn(mp) * fh, dn(mm) * fh
    mpl, mml = up(mp) * fl, up(mm) * fl
    q = pp + pm
    return (
        (mpl - mml - q * c_lo + zl,
         q * (c_lo - c_hi) - REDI * (mp + mm) - (own_p + own_m) - (zh + zl),
         mmh - mph + q * c_hi + zh),
        (-pp * p_lo - mpl, REDI * mp + pp * (p_lo - p_hi) + own_p, pp * p_hi + mph),
        (mml - pm * m_lo, REDI * mm + pm * (m_lo - m_hi) + own_m, pm * m_hi - mmh),
    )


def total(terms):
    result = terms[0]
    for term in terms[1:]:
        result = result + term
    return result


def kernel(
    sizes, x_ref, kmt_ref, out_ref,
    xv, kmt_int, coef, wcol, ecol, inner_w, inner_e, west, east, relay, from_n, from_s,
    load_sem, send_sem, recv_sem,
):
    tracers, levels, rows, lanes, n_lon, n_lat, pieces = sizes
    lon, lat = lax.axis_index("lon"), lax.axis_index("lat")
    at_top = lat == n_lat - 1
    below_top = jnp.logical_not(at_top)
    inner = lat > 0
    at_bottom = jnp.logical_not(inner)
    even_lat = lat < 0
    odd_lat = lat < 0
    relayed = jnp.logical_and(lon == 0, even_lat)
    relays = jnp.logical_and(lon == 0, odd_lat)
    far = jnp.logical_and(lon == n_lon - 1, even_lat)
    direct, near = jnp.logical_not(relayed), jnp.logical_not(far)
    early = jnp.logical_and(lon == 0, direct)
    late = jnp.logical_not(early)
    late_top, late_below = jnp.logical_and(late, at_top), jnp.logical_and(late, below_top)
    e_dev = (lax.rem(lon + 1, n_lon), lat)
    w_dev = (lax.rem(lon + n_lon - 1, n_lon), lat)
    n_dev, s_dev = (lon, lat + 1), (lon, lat - 1)
    fold_dev = (n_lon - 1 - lon, lat)
    tiles = tracers * levels
    plane = levels * rows
    group = tracers // pieces
    piece = group * levels
    slot = tracers + 2
    per = (lanes - 2) // slot
    regs = (levels + per - 1) // per

    barrier = pltpu.get_barrier_semaphore()

    def greet(dev):
        pl.semaphore_signal(barrier, inc=1, device_id=dev, device_id_type=MESH)

    with jax.named_scope("greet"):
        greet(w_dev)

        @pl.when(near)
        def _():
            greet(e_dev)

        @pl.when(far)
        def _():
            greet((0, lat + 1))

        @pl.when(at_top)
        def _():
            greet(fold_dev)

        @pl.when(below_top)
        def _():
            greet(n_dev)

        @pl.when(inner)
        def _():
            greet(s_dev)

    load_kmt = pltpu.make_async_copy(kmt_ref, kmt_int, load_sem.at[pieces])
    load_kmt.start()
    loads = []
    for i in range(pieces):
        span = pl.ds(i * piece, piece)
        copy = pltpu.make_async_copy(x_ref.at[span], xv.at[span], load_sem.at[i])
        copy.start()
        loads.append(copy)
    flat = xv.reshape((tiles + 1) * rows, lanes)

    lane = lax.broadcasted_iota(jnp.int32, (rows, lanes), 1)
    row = lax.broadcasted_iota(jnp.int32, (rows, lanes), 0)

    def pick(value, index):
        return jnp.take_along_axis(value, index, axis=1)

    def send(src, dst, s, r, dev):
        return pltpu.make_async_remote_copy(
            src_ref=src, dst_ref=dst, send_sem=send_sem.at[s], recv_sem=recv_sem.at[r],
            device_id=dev, device_id_type=MESH,
        )

    def rows_of(r, span, dst, s, dev):
        return send(xv.at[span, r, :], dst.at[span], s, s, dev)

    every = pl.ds(0, tiles + 1)
    fold = rows_of(rows - 1, every, from_n, 0, fold_dev)
    to_n = send(xv.at[every, rows - 1, :], from_s.at[every], 0, 1, n_dev)
    to_s = send(xv.at[every, 0, :], from_n.at[every], 1, 0, s_dev)
    cuts = [i * piece for i in range(pieces)] + [tiles + 1]
    folds = [
        rows_of(rows - 1, pl.ds(cuts[i], cuts[i + 1] - cuts[i]), from_n, 0, fold_dev) for i in range(pieces)
    ]
    to_e = send(ecol, west, 2, 2, e_dev)
    to_w = send(wcol, east, 3, 3, w_dev)
    to_relay = send(wcol, relay, 3, 4, n_dev)
    onward = send(relay, east, 4, 3, (n_lon - 1, lat - 1))

    def tile(t, k):
        return flat[pl.ds(t * plane + k * rows, rows), :]

    def density(k):
        return HALINE * tile(1, k) - THERMAL * tile(0, k)

    def gather_columns(e_ref, w_ref, e_off, w_off, before=None):
        zeros = jnp.zeros((rows, lanes), jnp.float32)
        es, ws = [zeros] * regs, [zeros] * regs

        def place(value, at, reg):
            value = pltpu.roll(value, at + 1, 1)
            es[reg] = jnp.where(lane == (at + e_off) % lanes, value, es[reg])
            ws[reg] = jnp.where(lane == (at + w_off) % lanes, value, ws[reg])

        for i in range(pieces):
            if before is not None:
                before(i)
            if i == 0:
                place(kmt_own, per * slot, 0)
                for k in range(levels):
                    place(density(k), k % per * slot + tracers, k // per)
            for t in range(i * group, (i + 1) * group):
                for k in range(levels):
                    place(tile(t, k), k % per * slot + t, k // per)
        for j in range(regs):
            e_ref[pl.ds(j * rows, rows), :] = es[j]
            w_ref[pl.ds(j * rows, rows), :] = ws[j]

    def enter():
        @pl.when(at_bottom)
        def _():
            pl.semaphore_wait(barrier, 3)

        @pl.when(jnp.logical_and(inner, jnp.logical_not(jnp.logical_or(relayed, relays))))
        def _():
            pl.semaphore_wait(barrier, 4)

        @pl.when(relayed)
        def _():
            pl.semaphore_wait(barrier, 3)

        @pl.when(relays)
        def _():
            pl.semaphore_wait(barrier, 5)

    def send_inner_rows():
        @pl.when(below_top)
        def _():
            to_n.start()

        @pl.when(inner)
        def _():
            to_s.start()

    held = max(pieces - 2, 1)

    def before(i):
        with jax.named_scope(f"load{i}"):
            loads[i].wait()
        if i == 0:

            @pl.when(late_top)
            def _():
                enter()

        if i < held:

            @pl.when(late_top)
            def _():
                folds[i].start()

        if i == pieces - 1:

            @pl.when(late_below)
            def _():
                with jax.named_scope("barrier"):
                    enter()

            @pl.when(late)
            def _():
                send_inner_rows()

    with jax.named_scope("loadk"):
        load_kmt.wait()
    kmt_own = kmt_int[...].astype(jnp.float32)
    xv[tiles, :, :] = kmt_own
    gather_columns(ecol, wcol, 0, 1, before)
    with jax.named_scope("send"):

        @pl.when(late)
        def _():
            to_e.start()

        @pl.when(jnp.logical_and(late, direct))
        def _():
            to_w.start()

        @pl.when(relayed)
        def _():
            to_relay.start()

        @pl.when(late_top)
        def _():
            for i in range(held, pieces):
                folds[i].start()

    with jax.named_scope("inner"):
        gather_columns(inner_e, inner_w, -1, 2)

        @pl.when(at_bottom)
        def _():
            for t in range(tracers + 1):
                from_s[pl.ds(t * levels, levels), :] = jnp.zeros((levels, lanes), jnp.float32)

    def put(d, dk, k, value):
        coef[pl.ds(((d * 3 + dk) * levels + k) * rows, rows), :] = value

    def piece_of(d, dk, k):
        return coef[pl.ds(((d * 3 + dk) * levels + k) * rows, rows), :]

    with jax.named_scope("coefs"):
        none = jnp.zeros((1, rows, lanes), jnp.float32)

        def up3(v):
            return jnp.concatenate([none, v[:-1]], axis=0)

        def dn3(v):
            return jnp.concatenate([v[1:], none], axis=0)

        def shifted(v, by, axis):
            return jnp.stack([pltpu.roll(v[k], by, axis) for k in range(levels)])

        own_rho = jnp.stack([density(k) for k in range(levels)])
        own_wet = jnp.stack([(kmt_own > float(k)).astype(jnp.float32) for k in range(levels)])
        c3 = column(own_rho, own_wet, up3, dn3)

        def moved(by, axis):
            return tuple(shifted(v, by, axis) for v in c3)

        mid_lane = jnp.logical_and(lane > 0, lane < lanes - 1)
        xc, xe, xw = line(c3, moved(lanes - 1, 1), moved(1, 1), up3, dn3)
        for dk in range(3):
            for k in range(levels):
                put(E, dk, k, jnp.where(mid_lane, xe[dk][k], 0.0))
                put(W, dk, k, jnp.where(mid_lane, xw[dk][k], 0.0))
                put(C, dk, k, jnp.where(mid_lane, xc[dk][k], 0.0))
        mid_row = jnp.logical_and(row > 0, row < rows - 1)
        yc, yn, ys = line(c3, moved(rows - 1, 0), moved(1, 0), up3, dn3)
        for dk in range(3):
            for k in range(levels):
                put(N, dk, k, jnp.where(mid_row, yn[dk][k], 0.0))
                put(S, dk, k, jnp.where(mid_row, ys[dk][k], 0.0))
                both = piece_of(C, dk, k) + jnp.where(mid_row, yc[dk][k], 0.0)
                put(C, dk, k, both + 1.0 if dk == 1 else both)

    with jax.named_scope("main"):

        @pl.loop(0, tracers // TOGETHER)
        def _(i):
            fields = []
            for u in range(TOGETHER):
                base = pl.multiple_of((i * TOGETHER + u) * plane, rows)
                field = []
                for k in range(levels):
                    own = flat[pl.ds(base + k * rows, rows), :]
                    field.append((
                        own, pltpu.roll(own, lanes - 1, 1), pltpu.roll(own, 1, 1),
                        pltpu.roll(own, rows - 1, 0), pltpu.roll(own, 1, 0),
                    ))
                fields.append(field)
            for k in range(levels):
                sums = [None] * TOGETHER
                for d in range(5):
                    for dk in range(3):
                        if not 0 <= k + dk - 1 < levels:
                            continue
                        c = piece_of(d, dk, k)
                        for u in range(TOGETHER):
                            term = c * fields[u][k + dk - 1][d]
                            sums[u] = term if sums[u] is None else sums[u] + term
                for u in range(TOGETHER):
                    base = pl.multiple_of((i * TOGETHER + u) * plane, rows)
                    out_ref[pl.ds(base + k * rows, rows), :] = sums[u]

    @pl.when(early)
    def _():
        with jax.named_scope("barrier"):
            enter()
        to_e.start()
        to_w.start()
        send_inner_rows()

        @pl.when(at_top)
        def _():
            fold.start()

    @pl.when(relays)
    def _():
        to_relay.wait_recv()
        onward.start()

    level = lax.broadcasted_iota(jnp.int32, (levels, lanes), 0)
    level_f = level.astype(jnp.float32)

    def up_s(v):
        return jnp.where(level == 0, 0.0, pltpu.roll(v, 1, 0))

    def dn_s(v):
        return jnp.where(level == levels - 1, 0.0, pltpu.roll(v, levels - 1, 0))

    def at_row(t, r):
        return flat[pl.ds(t * plane + r, levels, stride=rows), :]

    def row_column(t0, t1, kmt):
        wet = (jnp.broadcast_to(kmt, (levels, lanes)) > level_f).astype(jnp.float32)
        return column(HALINE * t1 - THERMAL * t0, wet, up_s, dn_s)

    def own_row(r):
        return row_column(at_row(0, r), at_row(1, r), kmt_own[r : r + 1, :])

    def fix_rows(source, r, r_in, north, turn):
        def halo(t):
            h = source[pl.ds(t * levels, levels), :]
            return pick(h, lanes - 1 - lane) if turn else h

        k = halo(tracers)[:1, :]
        out_c, in_c = row_column(halo(0), halo(1), k), own_row(r_in)
        p, m = (out_c, in_c) if north else (in_c, out_c)
        cc, cp, cm = line(own_row(r), p, m, up_s, dn_s)
        c_out, c_in = (cp, cm) if north else (cm, cp)
        table = (cc, c_out, c_in)
        lo = [pltpu.roll(c[0], levels - 1, 0) for c in table]
        mid = [c[1] for c in table]
        hi = [pltpu.roll(c[2], 1, 0) for c in table]

        batch = tracers // 2 if turn else group

        @pl.loop(0, tracers // batch)
        def _(i):
            for u in range(batch):
                t = i * batch + u
                values = (at_row(t, r), halo(t), at_row(t, r_in))
                above = total([c * v for c, v in zip(lo, values)])
                same = total([c * v for c, v in zip(mid, values)])
                below = total([c * v for c, v in zip(hi, values)])
                place = pl.ds(t * plane + r, levels, stride=rows)
                out_ref[place, :] = (
                    out_ref[place, :] + same + pltpu.roll(above, 1, 0) + pltpu.roll(below, levels - 1, 0)
                )

    def fix_n(turn):
        fold.wait_recv()
        fix_rows(from_n, rows - 1, rows - 2, True, turn)

    with jax.named_scope("fixs"):

        @pl.when(inner)
        def _():
            to_n.wait_recv()

        fix_rows(from_s, 0, 1, False, False)

    with jax.named_scope("fixn"):

        @pl.when(below_top)
        def _():
            fix_n(False)

    west_side = lane % 2 == 0
    spot = jnp.minimum((lane + 1) // 2 % (lanes // 2), tracers - 1)

    def both(w_ref, e_ref, w_off, e_off, at, k):
        base, span = k % per * slot, pl.ds(k // per * rows, rows)
        w_at = (base + at + w_off + lanes) % lanes
        e_at = (base + at + e_off + lanes) % lanes
        return jnp.where(west_side, pick(w_ref[span, :], w_at), pick(e_ref[span, :], e_at))

    def edge(w_ref, e_ref, w_off, e_off):
        args = (w_ref, e_ref, w_off, e_off)
        fixed = jnp.full((rows, lanes), tracers, jnp.int32)
        values = jnp.stack([both(*args, spot, k) for k in range(levels)])
        rho = jnp.stack([both(*args, fixed, k) for k in range(levels)])
        kmt = both(*args, jnp.full((rows, lanes), per * slot, jnp.int32), 0)
        wet = jnp.stack([(kmt > float(k)).astype(jnp.float32) for k in range(levels)])
        return values, column(rho, wet, up3, dn3)

    with jax.named_scope("fixc0"):
        own, own_c = edge(wcol, ecol, 1, 0)
        ins, ins_c = edge(inner_w, inner_e, 2, -1)
    with jax.named_scope("waitc"):
        to_e.wait_recv()
        to_w.wait_recv()
    with jax.named_scope("fixc1"):
        outs, outs_c = edge(west, east, 0, 1)
        table = line(own_c, outs_c, ins_c, up3, dn3)
        values = (own, outs, ins)
        above = total([c[0] * up3(v) for c, v in zip(table, values)])
        same = total([c[1] * v for c, v in zip(table, values)])
        below = total([c[2] * dn3(v) for c, v in zip(table, values)])
        add = same + above + below
        ends = jnp.logical_or(lane == 0, lane == lanes - 1)
        for t in range(tracers):
            for k in range(levels):
                term = pltpu.roll(add[k], (lanes - 2 * t) % lanes, 1)
                place = pl.ds(t * plane + k * rows, rows)
                out_ref[place, :] = out_ref[place, :] + jnp.where(ends, term, 0.0)

    with jax.named_scope("fixtop"):

        @pl.when(at_top)
        def _():
            fix_n(True)

    with jax.named_scope("end"):
        fold.wait_send()

        @pl.when(inner)
        def _():
            to_s.wait_send()

        to_e.wait_send()
        to_w.wait_send()

        @pl.when(relays)
        def _():
            onward.wait_send()


def solution(mesh):
    n_lon, n_lat = mesh.shape["lon"], mesh.shape["lat"]

    def local(tracers, kmt):
        nt, levels, rows, lanes = tracers.shape
        tiles = nt * levels
        per = (lanes - 2) // (nt + 2)
        regs = (levels + per - 1) // per
        pieces = 5 if nt % 5 == 0 else 1
        assert levels == rows and per > 0

        def vmem(*shape):
            return pltpu.VMEM(shape, jnp.float32)

        out = pl.pallas_call(
            functools.partial(kernel, (nt, levels, rows, lanes, n_lon, n_lat, pieces)),
            out_shape=pltpu.VMEM((tiles * rows, lanes), jnp.float32),
            in_specs=[pl.BlockSpec(memory_space=pltpu.HBM), pl.BlockSpec(memory_space=pltpu.HBM)],
            out_specs=pl.BlockSpec(memory_space=pltpu.VMEM),
            scratch_shapes=[
                vmem(tiles + 1, rows, lanes),
                pltpu.VMEM((rows, lanes), jnp.int32),
                vmem(15 * levels * rows, lanes),
            ]
            + [vmem(regs * rows, lanes)] * 7
            + [vmem(tiles + rows, lanes)] * 2
            + [
                pltpu.SemaphoreType.DMA((pieces + 1,)),
                pltpu.SemaphoreType.DMA((5,)),
                pltpu.SemaphoreType.DMA((5,)),
            ],
            compiler_params=pltpu.CompilerParams(collective_id=0, has_side_effects=True),
        )(tracers.reshape(tiles, rows, lanes), kmt)
        return out.reshape(nt, levels, rows, lanes)

    return jax.shard_map(
        local,
        mesh=mesh,
        in_specs=(P(None, None, "lat", "lon"), P("lat", "lon")),
        out_specs=P(None, None, "lat", "lon"),
        check_vma=False,
    )
```

```python
import functools

import jax
import jax.numpy as jnp
from jax import lax
from jax.experimental import pallas as pl
from jax.experimental.pallas import tpu as pltpu
from jax.sharding import PartitionSpec as P

THERMAL = 0.2
HALINE = 0.8
REDI = 0.1
SKEW = 0.05
SLOPE_MAX = 0.6
SLOPE_WIDTH = 0.2

MESH = pl.DeviceIdType.MESH
TOGETHER = 2
C, E, W, N, S = range(5)


def taper(slope):
    return slope * 0.5 * (1.0 + jnp.tanh((SLOPE_MAX - jnp.abs(slope)) / SLOPE_WIDTH))


def column(rho, wet, up, dn):
    hi = wet * dn(wet)
    strat = (dn(rho) - rho) * hi
    return rho, wet, hi, up(hi), 0.5 * (strat + up(strat))


def line(c, p, m, up, dn):
    c_rho, c_wet, c_hi, c_lo, c_cell = c
    p_rho, p_wet, p_hi, p_lo, p_cell = p
    m_rho, m_wet, m_hi, m_lo, m_cell = m
    mp, mm = c_wet * p_wet, c_wet * m_wet
    sp = taper((p_rho - c_rho) * mp / jnp.maximum(0.5 * (p_cell + c_cell), 1.0))
    sm = taper((c_rho - m_rho) * mm / jnp.maximum(0.5 * (m_cell + c_cell), 1.0))
    cx = 0.5 * (sp + sm)
    sw = 0.5 * (cx + dn(cx))
    fh = ((REDI + SKEW) * 0.25) * sw * c_hi
    zh = REDI * (sw * sw) * c_hi
    fl, zl = up(fh), up(zh)
    pp = ((REDI - SKEW) * 0.25) * sp * mp
    pm = -((REDI - SKEW) * 0.25) * sm * mm
    own_p, own_m = mp * (fh - fl), mm * (fl - fh)
    mph, mmh = dn(mp) * fh, dn(mm) * fh
    mpl, mml = up(mp) * fl, up(mm) * fl
    q = pp + pm
    return (
        (mpl - mml - q * c_lo + zl,
         q * (c_lo - c_hi) - REDI * (mp + mm) - (own_p + own_m) - (zh + zl),
         mmh - mph + q * c_hi + zh),
        (-pp * p_lo - mpl, REDI * mp + pp * (p_lo - p_hi) + own_p, pp * p_hi + mph),
        (mml - pm * m_lo, REDI * mm + pm * (m_lo - m_hi) + own_m, pm * m_hi - mmh),
    )


def total(terms):
    result = terms[0]
    for term in terms[1:]:
        result = result + term
    return result


def kernel(
    sizes, x_ref, kmt_ref, out_ref,
    xv, kmt_int, coef, wcol, ecol, inner_w, inner_e, west, east, relay, from_n, from_s,
    load_sem, send_sem, recv_sem,
):
    tracers, levels, rows, lanes, n_lon, n_lat, pieces = sizes
    lon, lat = lax.axis_index("lon"), lax.axis_index("lat")
    at_top = lat == n_lat - 1
    below_top = jnp.logical_not(at_top)
    inner = lat > 0
    at_bottom = jnp.logical_not(inner)
    even_lat = jnp.logical_and(inner, jnp.logical_and(lat % 2 == 0, below_top))
    odd_lat = jnp.logical_and(lat > 1, lat % 2 == 1)
    relayed = jnp.logical_and(lon == 0, even_lat)
    relays = jnp.logical_and(lon == 0, odd_lat)
    far = jnp.logical_and(lon == n_lon - 1, even_lat)
    direct, near = jnp.logical_not(relayed), jnp.logical_not(far)
    early = jnp.logical_and(lon == 0, direct)
    late = jnp.logical_not(early)
    late_top, late_below = jnp.logical_and(late, at_top), jnp.logical_and(late, below_top)
    e_dev = (lax.rem(lon + 1, n_lon), lat)
    w_dev = (lax.rem(lon + n_lon - 1, n_lon), lat)
    n_dev, s_dev = (lon, lat + 1), (lon, lat - 1)
    lat_up, lat_down = lax.rem(lat + 1, n_lat), lax.rem(lat + n_lat - 1, n_lat)
    fold_dev = (n_lon - 1 - lon, lat)
    tiles = tracers * levels
    plane = levels * rows
    group = tracers // pieces
    piece = group * levels
    slot = tracers + 2
    per = (lanes - 2) // slot
    regs = (levels + per - 1) // per

    barrier = pltpu.get_barrier_semaphore()

    def greet(dev):
        pl.semaphore_signal(barrier, inc=1, device_id=dev, device_id_type=MESH)

    with jax.named_scope("greet"):
        greet(w_dev)

        @pl.when(near)
        def _():
            greet(e_dev)

        @pl.when(far)
        def _():
            greet((0, lat_up))

        @pl.when(at_top)
        def _():
            greet(fold_dev)

        @pl.when(below_top)
        def _():
            greet(n_dev)

        @pl.when(inner)
        def _():
            greet(s_dev)

    load_kmt = pltpu.make_async_copy(kmt_ref, kmt_int, load_sem.at[pieces])
    load_kmt.start()
    loads = []
    for i in range(pieces):
        span = pl.ds(i * piece, piece)
        copy = pltpu.make_async_copy(x_ref.at[span], xv.at[span], load_sem.at[i])
        copy.start()
        loads.append(copy)
    flat = xv.reshape((tiles + 1) * rows, lanes)

    lane = lax.broadcasted_iota(jnp.int32, (rows, lanes), 1)
    row = lax.broadcasted_iota(jnp.int32, (rows, lanes), 0)

    def pick(value, index):
        return jnp.take_along_axis(value, index, axis=1)

    def send(src, dst, s, r, dev):
        return pltpu.make_async_remote_copy(
            src_ref=src, dst_ref=dst, send_sem=send_sem.at[s], recv_sem=recv_sem.at[r],
            device_id=dev, device_id_type=MESH,
        )

    def rows_of(r, span, dst, s, dev):
        return send(xv.at[span, r, :], dst.at[span], s, s, dev)

    every = pl.ds(0, tiles + 1)
    fold = rows_of(rows - 1, every, from_n, 0, fold_dev)
    to_n = send(xv.at[every, rows - 1, :], from_s.at[every], 0, 1, n_dev)
    to_s = send(xv.at[every, 0, :], from_n.at[every], 1, 0, s_dev)
    cuts = [i * piece for i in range(pieces)] + [tiles + 1]
    folds = [
        rows_of(rows - 1, pl.ds(cuts[i], cuts[i + 1] - cuts[i]), from_n, 0, fold_dev) for i in range(pieces)
    ]
    to_e = send(ecol, west, 2, 2, e_dev)
    to_w = send(wcol, east, 3, 3, w_dev)
    to_relay = send(wcol, relay, 3, 4, (lon, lat_up))
    onward = send(relay, east, 4, 3, (n_lon - 1, lat_down))

    def tile(t, k):
        return flat[pl.ds(t * plane + k * rows, rows), :]

    def density(k):
        return HALINE * tile(1, k) - THERMAL * tile(0, k)

    def gather_columns(e_ref, w_ref, e_off, w_off, before=None):
        zeros = jnp.zeros((rows, lanes), jnp.float32)
        es, ws = [zeros] * regs, [zeros] * regs

        def place(value, at, reg):
            value = pltpu.roll(value, at + 1, 1)
            es[reg] = jnp.where(lane == (at + e_off) % lanes, value, es[reg])
            ws[reg] = jnp.where(lane == (at + w_off) % lanes, value, ws[reg])

        for i in range(pieces):
            if before is not None:
                before(i)
            if i == 0:
                place(kmt_own, per * slot, 0)
                for k in range(levels):
                    place(density(k), k % per * slot + tracers, k // per)
            for t in range(i * group, (i + 1) * group):
                for k in range(levels):
                    place(tile(t, k), k % per * slot + t, k // per)
        for j in range(regs):
            e_ref[pl.ds(j * rows, rows), :] = es[j]
            w_ref[pl.ds(j * rows, rows), :] = ws[j]

    def enter():
        @pl.when(at_bottom)
        def _():
            pl.semaphore_wait(barrier, 3)

        @pl.when(jnp.logical_and(inner, jnp.logical_not(jnp.logical_or(relayed, relays))))
        def _():
            pl.semaphore_wait(barrier, 4)

        @pl.when(relayed)
        def _():
            pl.semaphore_wait(barrier, 3)

        @pl.when(relays)
        def _():
            pl.semaphore_wait(barrier, 5)

    def send_inner_rows():
        @pl.when(below_top)
        def _():
            to_n.start()

        @pl.when(inner)
        def _():
            to_s.start()

    held = max(pieces - 2, 1)

    def before(i):
        with jax.named_scope(f"load{i}"):
            loads[i].wait()
        if i == 0:

            @pl.when(late_top)
            def _():
                enter()

        if i < held:

            @pl.when(late_top)
            def _():
                folds[i].start()

        if i == pieces - 1:

            @pl.when(late_below)
            def _():
                with jax.named_scope("barrier"):
                    enter()

            @pl.when(late)
            def _():
                send_inner_rows()

    with jax.named_scope("loadk"):
        load_kmt.wait()
    kmt_own = kmt_int[...].astype(jnp.float32)
    xv[tiles, :, :] = kmt_own
    gather_columns(ecol, wcol, 0, 1, before)
    with jax.named_scope("send"):

        @pl.when(late)
        def _():
            to_e.start()

        @pl.when(jnp.logical_and(late, direct))
        def _():
            to_w.start()

        @pl.when(relayed)
        def _():
            to_relay.start()

        @pl.when(late_top)
        def _():
            for i in range(held, pieces):
                folds[i].start()

    with jax.named_scope("inner"):
        gather_columns(inner_e, inner_w, -1, 2)

        @pl.when(at_bottom)
        def _():
            for t in range(tracers + 1):
                from_s[pl.ds(t * levels, levels), :] = jnp.zeros((levels, lanes), jnp.float32)

    def put(d, dk, k, value):
        coef[pl.ds(((d * 3 + dk) * levels + k) * rows, rows), :] = value

    def piece_of(d, dk, k):
        return coef[pl.ds(((d * 3 + dk) * levels + k) * rows, rows), :]

    with jax.named_scope("coefs"):
        none = jnp.zeros((1, rows, lanes), jnp.float32)

        def up3(v):
            return jnp.concatenate([none, v[:-1]], axis=0)

        def dn3(v):
            return jnp.concatenate([v[1:], none], axis=0)

        def shifted(v, by, axis):
            return jnp.stack([pltpu.roll(v[k], by, axis) for k in range(levels)])

        own_rho = jnp.stack([density(k) for k in range(levels)])
        own_wet = jnp.stack([(kmt_own > float(k)).astype(jnp.float32) for k in range(levels)])
        c3 = column(own_rho, own_wet, up3, dn3)

        def moved(by, axis):
            return tuple(shifted(v, by, axis) for v in c3)

        mid_lane = jnp.logical_and(lane > 0, lane < lanes - 1)
        xc, xe, xw = line(c3, moved(lanes - 1, 1), moved(1, 1), up3, dn3)
        for dk in range(3):
            for k in range(levels):
                put(E, dk, k, jnp.where(mid_lane, xe[dk][k], 0.0))
                put(W, dk, k, jnp.where(mid_lane, xw[dk][k], 0.0))
                put(C, dk, k, jnp.where(mid_lane, xc[dk][k], 0.0))
        mid_row = jnp.logical_and(row > 0, row < rows - 1)
        yc, yn, ys = line(c3, moved(rows - 1, 0), moved(1, 0), up3, dn3)
        for dk in range(3):
            for k in range(levels):
                put(N, dk, k, jnp.where(mid_row, yn[dk][k], 0.0))
                put(S, dk, k, jnp.where(mid_row, ys[dk][k], 0.0))
                both = piece_of(C, dk, k) + jnp.where(mid_row, yc[dk][k], 0.0)
                put(C, dk, k, both + 1.0 if dk == 1 else both)

    with jax.named_scope("main"):

        @pl.loop(0, tracers // TOGETHER)
        def _(i):
            fields = []
            for u in range(TOGETHER):
                base = pl.multiple_of((i * TOGETHER + u) * plane, rows)
                field = []
                for k in range(levels):
                    own = flat[pl.ds(base + k * rows, rows), :]
                    field.append((
                        own, pltpu.roll(own, lanes - 1, 1), pltpu.roll(own, 1, 1),
                        pltpu.roll(own, rows - 1, 0), pltpu.roll(own, 1, 0),
                    ))
                fields.append(field)
            for k in range(levels):
                sums = [None] * TOGETHER
                for d in range(5):
                    for dk in range(3):
                        if not 0 <= k + dk - 1 < levels:
                            continue
                        c = piece_of(d, dk, k)
                        for u in range(TOGETHER):
                            term = c * fields[u][k + dk - 1][d]
                            sums[u] = term if sums[u] is None else sums[u] + term
                for u in range(TOGETHER):
                    base = pl.multiple_of((i * TOGETHER + u) * plane, rows)
                    out_ref[pl.ds(base + k * rows, rows), :] = sums[u]

    @pl.when(early)
    def _():
        with jax.named_scope("barrier"):
            enter()
        to_e.start()
        to_w.start()
        send_inner_rows()

        @pl.when(at_top)
        def _():
            fold.start()

    @pl.when(relays)
    def _():
        to_relay.wait_recv()
        onward.start()

    level = lax.broadcasted_iota(jnp.int32, (levels, lanes), 0)
    level_f = level.astype(jnp.float32)

    def up_s(v):
        return jnp.where(level == 0, 0.0, pltpu.roll(v, 1, 0))

    def dn_s(v):
        return jnp.where(level == levels - 1, 0.0, pltpu.roll(v, levels - 1, 0))

    def at_row(t, r):
        return flat[pl.ds(t * plane + r, levels, stride=rows), :]

    def row_column(t0, t1, kmt):
        wet = (jnp.broadcast_to(kmt, (levels, lanes)) > level_f).astype(jnp.float32)
        return column(HALINE * t1 - THERMAL * t0, wet, up_s, dn_s)

    def own_row(r):
        return row_column(at_row(0, r), at_row(1, r), kmt_own[r : r + 1, :])

    def fix_rows(source, r, r_in, north, turn):
        def halo(t):
            h = source[pl.ds(t * levels, levels), :]
            return pick(h, lanes - 1 - lane) if turn else h

        k = halo(tracers)[:1, :]
        out_c, in_c = row_column(halo(0), halo(1), k), own_row(r_in)
        p, m = (out_c, in_c) if north else (in_c, out_c)
        cc, cp, cm = line(own_row(r), p, m, up_s, dn_s)
        c_out, c_in = (cp, cm) if north else (cm, cp)
        table = (cc, c_out, c_in)
        lo = [pltpu.roll(c[0], levels - 1, 0) for c in table]
        mid = [c[1] for c in table]
        hi = [pltpu.roll(c[2], 1, 0) for c in table]

        batch = tracers // 2 if turn else group

        @pl.loop(0, tracers // batch)
        def _(i):
            for u in range(batch):
                t = i * batch + u
                values = (at_row(t, r), halo(t), at_row(t, r_in))
                above = total([c * v for c, v in zip(lo, values)])
                same = total([c * v for c, v in zip(mid, values)])
                below = total([c * v for c, v in zip(hi, values)])
                place = pl.ds(t * plane + r, levels, stride=rows)
                out_ref[place, :] = (
                    out_ref[place, :] + same + pltpu.roll(above, 1, 0) + pltpu.roll(below, levels - 1, 0)
                )

    def fix_n(turn):
        fold.wait_recv()
        fix_rows(from_n, rows - 1, rows - 2, True, turn)

    with jax.named_scope("fixs"):

        @pl.when(inner)
        def _():
            to_n.wait_recv()

        fix_rows(from_s, 0, 1, False, False)

    with jax.named_scope("fixn"):

        @pl.when(below_top)
        def _():
            fix_n(False)

    west_side = lane % 2 == 0
    spot = jnp.minimum((lane + 1) // 2 % (lanes // 2), tracers - 1)

    def both(w_ref, e_ref, w_off, e_off, at, k):
        base, span = k % per * slot, pl.ds(k // per * rows, rows)
        w_at = (base + at + w_off + lanes) % lanes
        e_at = (base + at + e_off + lanes) % lanes
        return jnp.where(west_side, pick(w_ref[span, :], w_at), pick(e_ref[span, :], e_at))

    def edge(w_ref, e_ref, w_off, e_off):
        args = (w_ref, e_ref, w_off, e_off)
        fixed = jnp.full((rows, lanes), tracers, jnp.int32)
        values = jnp.stack([both(*args, spot, k) for k in range(levels)])
        rho = jnp.stack([both(*args, fixed, k) for k in range(levels)])
        kmt = both(*args, jnp.full((rows, lanes), per * slot, jnp.int32), 0)
        wet = jnp.stack([(kmt > float(k)).astype(jnp.float32) for k in range(levels)])
        return values, column(rho, wet, up3, dn3)

    with jax.named_scope("fixc0"):
        own, own_c = edge(wcol, ecol, 1, 0)
        ins, ins_c = edge(inner_w, inner_e, 2, -1)
    with jax.named_scope("waitc"):
        to_e.wait_recv()
        to_w.wait_recv()
    with jax.named_scope("fixc1"):
        outs, outs_c = edge(west, east, 0, 1)
        table = line(own_c, outs_c, ins_c, up3, dn3)
        values = (own, outs, ins)
        above = total([c[0] * up3(v) for c, v in zip(table, values)])
        same = total([c[1] * v for c, v in zip(table, values)])
        below = total([c[2] * dn3(v) for c, v in zip(table, values)])
        add = same + above + below
        ends = jnp.logical_or(lane == 0, lane == lanes - 1)
        for t in range(tracers):
            for k in range(levels):
                term = pltpu.roll(add[k], (lanes - 2 * t) % lanes, 1)
                place = pl.ds(t * plane + k * rows, rows)
                out_ref[place, :] = out_ref[place, :] + jnp.where(ends, term, 0.0)

    with jax.named_scope("fixtop"):

        @pl.when(at_top)
        def _():
            fix_n(True)

    with jax.named_scope("end"):
        fold.wait_send()

        @pl.when(inner)
        def _():
            to_s.wait_send()

        to_e.wait_send()
        to_w.wait_send()

        @pl.when(relays)
        def _():
            onward.wait_send()


def solution(mesh):
    n_lon, n_lat = mesh.shape["lon"], mesh.shape["lat"]

    def local(tracers, kmt):
        nt, levels, rows, lanes = tracers.shape
        tiles = nt * levels
        per = (lanes - 2) // (nt + 2)
        regs = (levels + per - 1) // per
        pieces = 5 if nt % 5 == 0 else 1
        assert levels == rows and per > 0

        def vmem(*shape):
            return pltpu.VMEM(shape, jnp.float32)

        out = pl.pallas_call(
            functools.partial(kernel, (nt, levels, rows, lanes, n_lon, n_lat, pieces)),
            out_shape=pltpu.VMEM((tiles * rows, lanes), jnp.float32),
            in_specs=[pl.BlockSpec(memory_space=pltpu.HBM), pl.BlockSpec(memory_space=pltpu.HBM)],
            out_specs=pl.BlockSpec(memory_space=pltpu.VMEM),
            scratch_shapes=[
                vmem(tiles + 1, rows, lanes),
                pltpu.VMEM((rows, lanes), jnp.int32),
                vmem(15 * levels * rows, lanes),
            ]
            + [vmem(regs * rows, lanes)] * 7
            + [vmem(tiles + rows, lanes)] * 2
            + [
                pltpu.SemaphoreType.DMA((pieces + 1,)),
                pltpu.SemaphoreType.DMA((5,)),
                pltpu.SemaphoreType.DMA((5,)),
            ],
            compiler_params=pltpu.CompilerParams(collective_id=0, has_side_effects=True),
        )(tracers.reshape(tiles, rows, lanes), kmt)
        return out.reshape(nt, levels, rows, lanes)

    return jax.shard_map(
        local,
        mesh=mesh,
        in_specs=(P(None, None, "lat", "lon"), P("lat", "lon")),
        out_specs=P(None, None, "lat", "lon"),
        check_vma=False,
    )
```

```python
import functools

import jax
import jax.numpy as jnp
from jax import lax
from jax.experimental import pallas as pl
from jax.experimental.pallas import tpu as pltpu
from jax.sharding import PartitionSpec as P

THERMAL = 0.2
HALINE = 0.8
REDI = 0.1
SKEW = 0.05
SLOPE_MAX = 0.6
SLOPE_WIDTH = 0.2

MESH = pl.DeviceIdType.MESH
TOGETHER = 2
C, E, W, N, S = range(5)


def taper(slope):
    return slope * 0.5 * (1.0 + jnp.tanh((SLOPE_MAX - jnp.abs(slope)) / SLOPE_WIDTH))


def column(rho, wet, up, dn):
    hi = wet * dn(wet)
    strat = (dn(rho) - rho) * hi
    return rho, wet, hi, up(hi), 0.5 * (strat + up(strat))


def line(c, p, m, up, dn):
    c_rho, c_wet, c_hi, c_lo, c_cell = c
    p_rho, p_wet, p_hi, p_lo, p_cell = p
    m_rho, m_wet, m_hi, m_lo, m_cell = m
    mp, mm = c_wet * p_wet, c_wet * m_wet
    sp = taper((p_rho - c_rho) * mp / jnp.maximum(0.5 * (p_cell + c_cell), 1.0))
    sm = taper((c_rho - m_rho) * mm / jnp.maximum(0.5 * (m_cell + c_cell), 1.0))
    cx = 0.5 * (sp + sm)
    sw = 0.5 * (cx + dn(cx))
    fh = ((REDI + SKEW) * 0.25) * sw * c_hi
    zh = REDI * (sw * sw) * c_hi
    fl, zl = up(fh), up(zh)
    pp = ((REDI - SKEW) * 0.25) * sp * mp
    pm = -((REDI - SKEW) * 0.25) * sm * mm
    own_p, own_m = mp * (fh - fl), mm * (fl - fh)
    mph, mmh = dn(mp) * fh, dn(mm) * fh
    mpl, mml = up(mp) * fl, up(mm) * fl
    q = pp + pm
    return (
        (mpl - mml - q * c_lo + zl,
         q * (c_lo - c_hi) - REDI * (mp + mm) - (own_p + own_m) - (zh + zl),
         mmh - mph + q * c_hi + zh),
        (-pp * p_lo - mpl, REDI * mp + pp * (p_lo - p_hi) + own_p, pp * p_hi + mph),
        (mml - pm * m_lo, REDI * mm + pm * (m_lo - m_hi) + own_m, pm * m_hi - mmh),
    )


def total(terms):
    result = terms[0]
    for term in terms[1:]:
        result = result + term
    return result


def kernel(
    sizes, x_ref, kmt_ref, out_ref, add_ref,
    xv, kmt_int, coef, wcol, ecol, inner_w, inner_e, west, east, relay, from_n, from_s,
    load_sem, send_sem, recv_sem,
):
    tracers, levels, rows, lanes, n_lon, n_lat, pieces = sizes
    lon, lat = lax.axis_index("lon"), lax.axis_index("lat")
    at_top = lat == n_lat - 1
    below_top = jnp.logical_not(at_top)
    inner = lat > 0
    at_bottom = jnp.logical_not(inner)
    even_lat = jnp.logical_and(inner, jnp.logical_and(lat % 2 == 0, below_top))
    odd_lat = jnp.logical_and(lat > 1, lat % 2 == 1)
    relayed = jnp.logical_and(lon == 0, even_lat)
    relays = jnp.logical_and(lon == 0, odd_lat)
    far = jnp.logical_and(lon == n_lon - 1, even_lat)
    direct, near = jnp.logical_not(relayed), jnp.logical_not(far)
    early = jnp.logical_and(lon == 0, direct)
    late = jnp.logical_not(early)
    late_top, late_below = jnp.logical_and(late, at_top), jnp.logical_and(late, below_top)
    e_dev = (lax.rem(lon + 1, n_lon), lat)
    w_dev = (lax.rem(lon + n_lon - 1, n_lon), lat)
    n_dev, s_dev = (lon, lat + 1), (lon, lat - 1)
    lat_up, lat_down = lax.rem(lat + 1, n_lat), lax.rem(lat + n_lat - 1, n_lat)
    fold_dev = (n_lon - 1 - lon, lat)
    tiles = tracers * levels
    plane = levels * rows
    group = tracers // pieces
    piece = group * levels
    slot = tracers + 2
    per = (lanes - 2) // slot
    regs = (levels + per - 1) // per

    barrier = pltpu.get_barrier_semaphore()

    def greet(dev):
        pl.semaphore_signal(barrier, inc=1, device_id=dev, device_id_type=MESH)

    with jax.named_scope("greet"):
        greet(w_dev)

        @pl.when(near)
        def _():
            greet(e_dev)

        @pl.when(far)
        def _():
            greet((0, lat_up))

        @pl.when(at_top)
        def _():
            greet(fold_dev)

        @pl.when(below_top)
        def _():
            greet(n_dev)

        @pl.when(inner)
        def _():
            greet(s_dev)

    load_kmt = pltpu.make_async_copy(kmt_ref, kmt_int, load_sem.at[pieces])
    load_kmt.start()
    loads = []
    for i in range(pieces):
        span = pl.ds(i * piece, piece)
        copy = pltpu.make_async_copy(x_ref.at[span], xv.at[span], load_sem.at[i])
        copy.start()
        loads.append(copy)
    flat = xv.reshape((tiles + 1) * rows, lanes)

    lane = lax.broadcasted_iota(jnp.int32, (rows, lanes), 1)
    row = lax.broadcasted_iota(jnp.int32, (rows, lanes), 0)

    def pick(value, index):
        return jnp.take_along_axis(value, index, axis=1)

    def send(src, dst, s, r, dev):
        return pltpu.make_async_remote_copy(
            src_ref=src, dst_ref=dst, send_sem=send_sem.at[s], recv_sem=recv_sem.at[r],
            device_id=dev, device_id_type=MESH,
        )

    def rows_of(r, span, dst, s, dev):
        return send(xv.at[span, r, :], dst.at[span], s, s, dev)

    every = pl.ds(0, tiles + 1)
    fold = rows_of(rows - 1, every, from_n, 0, fold_dev)
    to_n = send(xv.at[every, rows - 1, :], from_s.at[every], 0, 1, n_dev)
    to_s = send(xv.at[every, 0, :], from_n.at[every], 1, 0, s_dev)
    cuts = [i * piece for i in range(pieces)] + [tiles + 1]
    folds = [
        rows_of(rows - 1, pl.ds(cuts[i], cuts[i + 1] - cuts[i]), from_n, 0, fold_dev) for i in range(pieces)
    ]
    to_e = send(ecol, west, 2, 2, e_dev)
    to_w = send(wcol, east, 3, 3, w_dev)
    to_relay = send(wcol, relay, 3, 4, (lon, lat_up))
    onward = send(relay, east, 4, 3, (n_lon - 1, lat_down))

    def tile(t, k):
        return flat[pl.ds(t * plane + k * rows, rows), :]

    def density(k):
        return HALINE * tile(1, k) - THERMAL * tile(0, k)

    starts = {0: 1}
    while max(starts.values()) < pieces:
        last = max(starts.values())
        starts[last] = min(last + 2, pieces)

    def gather_columns(e_ref, w_ref, e_off, w_off, before=None):
        zeros = jnp.zeros((rows, lanes), jnp.float32)
        es, ws = [zeros] * regs, [zeros] * regs

        def place(value, at, reg):
            value = pltpu.roll(value, at + 1, 1)
            es[reg] = jnp.where(lane == (at + e_off) % lanes, value, es[reg])
            ws[reg] = jnp.where(lane == (at + w_off) % lanes, value, ws[reg])

        for i in range(pieces):
            if before is not None and i in starts:
                for n in range(i, starts[i]):
                    before(n)
            if i == 0:
                place(kmt_own, per * slot, 0)
                for k in range(levels):
                    place(density(k), k % per * slot + tracers, k // per)
            for t in range(i * group, (i + 1) * group):
                for k in range(levels):
                    place(tile(t, k), k % per * slot + t, k // per)
        for j in range(regs):
            e_ref[pl.ds(j * rows, rows), :] = es[j]
            w_ref[pl.ds(j * rows, rows), :] = ws[j]

    def enter():
        @pl.when(at_bottom)
        def _():
            pl.semaphore_wait(barrier, 3)

        @pl.when(jnp.logical_and(inner, jnp.logical_not(jnp.logical_or(relayed, relays))))
        def _():
            pl.semaphore_wait(barrier, 4)

        @pl.when(relayed)
        def _():
            pl.semaphore_wait(barrier, 3)

        @pl.when(relays)
        def _():
            pl.semaphore_wait(barrier, 5)

    def send_inner_rows():
        @pl.when(below_top)
        def _():
            to_n.start()

        @pl.when(inner)
        def _():
            to_s.start()

    held = max(pieces - 2, 1)

    def before(i):
        with jax.named_scope(f"load{i}"):
            loads[i].wait()
        if i == 0:

            @pl.when(late_top)
            def _():
                enter()

        if i < held:

            @pl.when(late_top)
            def _():
                folds[i].start()

        if i == pieces - 1:

            @pl.when(late_below)
            def _():
                with jax.named_scope("barrier"):
                    enter()

            @pl.when(late)
            def _():
                send_inner_rows()

    with jax.named_scope("loadk"):
        load_kmt.wait()
    kmt_own = kmt_int[...].astype(jnp.float32)
    xv[tiles, :, :] = kmt_own
    gather_columns(ecol, wcol, 0, 1, before)
    with jax.named_scope("send"):

        @pl.when(late)
        def _():
            to_e.start()

        @pl.when(jnp.logical_and(late, direct))
        def _():
            to_w.start()

        @pl.when(relayed)
        def _():
            to_relay.start()

        @pl.when(late_top)
        def _():
            for i in range(held, pieces):
                folds[i].start()

    with jax.named_scope("inner"):
        gather_columns(inner_e, inner_w, -1, 2)

        @pl.when(at_bottom)
        def _():
            for t in range(tracers + 1):
                from_s[pl.ds(t * levels, levels), :] = jnp.zeros((levels, lanes), jnp.float32)

    def put(d, dk, k, value):
        coef[pl.ds(((d * 3 + dk) * levels + k) * rows, rows), :] = value

    def piece_of(d, dk, k):
        return coef[pl.ds(((d * 3 + dk) * levels + k) * rows, rows), :]

    with jax.named_scope("coefs"):
        none = jnp.zeros((1, rows, lanes), jnp.float32)

        def up3(v):
            return jnp.concatenate([none, v[:-1]], axis=0)

        def dn3(v):
            return jnp.concatenate([v[1:], none], axis=0)

        def shifted(v, by, axis):
            return jnp.stack([pltpu.roll(v[k], by, axis) for k in range(levels)])

        own_rho = jnp.stack([density(k) for k in range(levels)])
        own_wet = jnp.stack([(kmt_own > float(k)).astype(jnp.float32) for k in range(levels)])
        c3 = column(own_rho, own_wet, up3, dn3)

        def moved(by, axis):
            return tuple(shifted(v, by, axis) for v in c3)

        mid_lane = jnp.logical_and(lane > 0, lane < lanes - 1)
        xc, xe, xw = line(c3, moved(lanes - 1, 1), moved(1, 1), up3, dn3)
        for dk in range(3):
            for k in range(levels):
                put(E, dk, k, jnp.where(mid_lane, xe[dk][k], 0.0))
                put(W, dk, k, jnp.where(mid_lane, xw[dk][k], 0.0))
                put(C, dk, k, jnp.where(mid_lane, xc[dk][k], 0.0))
        mid_row = jnp.logical_and(row > 0, row < rows - 1)
        yc, yn, ys = line(c3, moved(rows - 1, 0), moved(1, 0), up3, dn3)
        for dk in range(3):
            for k in range(levels):
                put(N, dk, k, jnp.where(mid_row, yn[dk][k], 0.0))
                put(S, dk, k, jnp.where(mid_row, ys[dk][k], 0.0))
                both = piece_of(C, dk, k) + jnp.where(mid_row, yc[dk][k], 0.0)
                put(C, dk, k, both + 1.0 if dk == 1 else both)

    with jax.named_scope("main"):

        @pl.loop(0, tracers // TOGETHER)
        def _(i):
            fields = []
            for u in range(TOGETHER):
                base = pl.multiple_of((i * TOGETHER + u) * plane, rows)
                field = []
                for k in range(levels):
                    own = flat[pl.ds(base + k * rows, rows), :]
                    field.append((
                        own, pltpu.roll(own, lanes - 1, 1), pltpu.roll(own, 1, 1),
                        pltpu.roll(own, rows - 1, 0), pltpu.roll(own, 1, 0),
                    ))
                fields.append(field)
            for k in range(levels):
                sums = [None] * TOGETHER
                for d in range(5):
                    for dk in range(3):
                        if not 0 <= k + dk - 1 < levels:
                            continue
                        c = piece_of(d, dk, k)
                        for u in range(TOGETHER):
                            term = c * fields[u][k + dk - 1][d]
                            sums[u] = term if sums[u] is None else sums[u] + term
                for u in range(TOGETHER):
                    base = pl.multiple_of((i * TOGETHER + u) * plane, rows)
                    out_ref[pl.ds(base + k * rows, rows), :] = sums[u]

    @pl.when(early)
    def _():
        with jax.named_scope("barrier"):
            enter()
        to_e.start()
        to_w.start()
        send_inner_rows()

        @pl.when(at_top)
        def _():
            fold.start()

    @pl.when(relays)
    def _():
        to_relay.wait_recv()
        onward.start()

    level = lax.broadcasted_iota(jnp.int32, (levels, lanes), 0)
    level_f = level.astype(jnp.float32)

    def up_s(v):
        return jnp.where(level == 0, 0.0, pltpu.roll(v, 1, 0))

    def dn_s(v):
        return jnp.where(level == levels - 1, 0.0, pltpu.roll(v, levels - 1, 0))

    def at_row(t, r):
        return flat[pl.ds(t * plane + r, levels, stride=rows), :]

    def row_column(t0, t1, kmt):
        wet = (jnp.broadcast_to(kmt, (levels, lanes)) > level_f).astype(jnp.float32)
        return column(HALINE * t1 - THERMAL * t0, wet, up_s, dn_s)

    def own_row(r):
        return row_column(at_row(0, r), at_row(1, r), kmt_own[r : r + 1, :])

    def fix_rows(source, r, r_in, north, turn):
        def halo(t):
            h = source[pl.ds(t * levels, levels), :]
            return pick(h, lanes - 1 - lane) if turn else h

        k = halo(tracers)[:1, :]
        out_c, in_c = row_column(halo(0), halo(1), k), own_row(r_in)
        p, m = (out_c, in_c) if north else (in_c, out_c)
        cc, cp, cm = line(own_row(r), p, m, up_s, dn_s)
        c_out, c_in = (cp, cm) if north else (cm, cp)
        table = (cc, c_out, c_in)
        lo = [pltpu.roll(c[0], levels - 1, 0) for c in table]
        mid = [c[1] for c in table]
        hi = [pltpu.roll(c[2], 1, 0) for c in table]

        batch = tracers // 2 if turn else group

        @pl.loop(0, tracers // batch)
        def _(i):
            for u in range(batch):
                t = i * batch + u
                values = (at_row(t, r), halo(t), at_row(t, r_in))
                above = total([c * v for c, v in zip(lo, values)])
                same = total([c * v for c, v in zip(mid, values)])
                below = total([c * v for c, v in zip(hi, values)])
                place = pl.ds(t * plane + r, levels, stride=rows)
                out_ref[place, :] = (
                    out_ref[place, :] + same + pltpu.roll(above, 1, 0) + pltpu.roll(below, levels - 1, 0)
                )

    def fix_n(turn):
        fold.wait_recv()
        fix_rows(from_n, rows - 1, rows - 2, True, turn)

    with jax.named_scope("fixs"):

        @pl.when(inner)
        def _():
            to_n.wait_recv()

        fix_rows(from_s, 0, 1, False, False)

    with jax.named_scope("fixn"):

        @pl.when(below_top)
        def _():
            fix_n(False)

    west_side = lane % 2 == 0
    spot = jnp.minimum((lane + 1) // 2 % (lanes // 2), tracers - 1)

    def both(w_ref, e_ref, w_off, e_off, at, k):
        base, span = k % per * slot, pl.ds(k // per * rows, rows)
        w_at = (base + at + w_off + lanes) % lanes
        e_at = (base + at + e_off + lanes) % lanes
        return jnp.where(west_side, pick(w_ref[span, :], w_at), pick(e_ref[span, :], e_at))

    def edge(w_ref, e_ref, w_off, e_off):
        args = (w_ref, e_ref, w_off, e_off)
        fixed = jnp.full((rows, lanes), tracers, jnp.int32)
        values = jnp.stack([both(*args, spot, k) for k in range(levels)])
        rho = jnp.stack([both(*args, fixed, k) for k in range(levels)])
        kmt = both(*args, jnp.full((rows, lanes), per * slot, jnp.int32), 0)
        wet = jnp.stack([(kmt > float(k)).astype(jnp.float32) for k in range(levels)])
        return values, column(rho, wet, up3, dn3)

    with jax.named_scope("fixc0"):
        own, own_c = edge(wcol, ecol, 1, 0)
        ins, ins_c = edge(inner_w, inner_e, 2, -1)
    with jax.named_scope("waitc"):
        to_e.wait_recv()
        to_w.wait_recv()
    with jax.named_scope("fixc1"):
        outs, outs_c = edge(west, east, 0, 1)
        table = line(own_c, outs_c, ins_c, up3, dn3)
        values = (own, outs, ins)
        above = total([c[0] * up3(v) for c, v in zip(table, values)])
        same = total([c[1] * v for c, v in zip(table, values)])
        below = total([c[2] * dn3(v) for c, v in zip(table, values)])
        for k in range(levels):
            add_ref[pl.ds(k * rows, rows), :] = same[k] + above[k] + below[k]

    with jax.named_scope("fixtop"):

        @pl.when(at_top)
        def _():
            fix_n(True)

    with jax.named_scope("end"):
        fold.wait_send()

        @pl.when(inner)
        def _():
            to_s.wait_send()

        to_e.wait_send()
        to_w.wait_send()

        @pl.when(relays)
        def _():
            onward.wait_send()


def finish(sizes, part_ref, add_ref, out_ref, stage, sem):
    tracers, levels, rows, lanes, pieces = sizes
    plane = levels * rows
    group = tracers // pieces
    lane = lax.broadcasted_iota(jnp.int32, (rows, lanes), 1)
    ends = jnp.logical_or(lane == 0, lane == lanes - 1)
    add = [add_ref[pl.ds(k * rows, rows), :] for k in range(levels)]
    copies = []
    for i in range(pieces):
        with jax.named_scope(f"insert{i}"):
            for t in range(i * group, (i + 1) * group):
                for k in range(levels):
                    term = pltpu.roll(add[k], (lanes - 2 * t) % lanes, 1)
                    place = pl.ds(t * plane + k * rows, rows)
                    stage[place, :] = part_ref[place, :] + jnp.where(ends, term, 0.0)
            span = pl.ds(i * group * plane, group * plane)
            copy = pltpu.make_async_copy(stage.at[span], out_ref.at[span], sem.at[i])
            copy.start()
            copies.append(copy)
    with jax.named_scope("written"):
        for copy in copies:
            copy.wait()


def solution(mesh):
    n_lon, n_lat = mesh.shape["lon"], mesh.shape["lat"]

    def local(tracers, kmt):
        nt, levels, rows, lanes = tracers.shape
        tiles = nt * levels
        per = (lanes - 2) // (nt + 2)
        regs = (levels + per - 1) // per
        pieces = 5 if nt % 5 == 0 else 1
        assert levels == rows and per > 0

        def vmem(*shape):
            return pltpu.VMEM(shape, jnp.float32)

        part, add = pl.pallas_call(
            functools.partial(kernel, (nt, levels, rows, lanes, n_lon, n_lat, pieces)),
            out_shape=[vmem(tiles * rows, lanes), vmem(levels * rows, lanes)],
            in_specs=[pl.BlockSpec(memory_space=pltpu.HBM), pl.BlockSpec(memory_space=pltpu.HBM)],
            out_specs=[pl.BlockSpec(memory_space=pltpu.VMEM)] * 2,
            scratch_shapes=[
                vmem(tiles + 1, rows, lanes),
                pltpu.VMEM((rows, lanes), jnp.int32),
                vmem(15 * levels * rows, lanes),
            ]
            + [vmem(regs * rows, lanes)] * 7
            + [vmem(tiles + rows, lanes)] * 2
            + [
                pltpu.SemaphoreType.DMA((pieces + 1,)),
                pltpu.SemaphoreType.DMA((5,)),
                pltpu.SemaphoreType.DMA((5,)),
            ],
            compiler_params=pltpu.CompilerParams(collective_id=0, has_side_effects=True),
        )(tracers.reshape(tiles, rows, lanes), kmt)
        part, add = (pltpu.with_memory_space_constraint(v, pltpu.VMEM) for v in (part, add))
        out = pl.pallas_call(
            functools.partial(finish, (nt, levels, rows, lanes, pieces)),
            out_shape=jax.ShapeDtypeStruct((tiles * rows, lanes), jnp.float32),
            in_specs=[pl.BlockSpec(memory_space=pltpu.VMEM)] * 2,
            out_specs=pl.BlockSpec(memory_space=pltpu.HBM),
            scratch_shapes=[vmem(tiles * rows, lanes), pltpu.SemaphoreType.DMA((pieces,))],
        )(part, add)
        return out.reshape(nt, levels, rows, lanes)

    return jax.shard_map(
        local,
        mesh=mesh,
        in_specs=(P(None, None, "lat", "lon"), P("lat", "lon")),
        out_specs=P(None, None, "lat", "lon"),
        check_vma=False,
    )
```

```python
import functools

import jax
import jax.numpy as jnp
from jax import lax
from jax.experimental import pallas as pl
from jax.experimental.pallas import tpu as pltpu
from jax.sharding import PartitionSpec as P

THERMAL = 0.2
HALINE = 0.8
REDI = 0.1
SKEW = 0.05
SLOPE_MAX = 0.6
SLOPE_WIDTH = 0.2

MESH = pl.DeviceIdType.MESH
TOGETHER = 2
STORE = 2
C, E, W, N, S = range(5)


def taper(slope):
    return slope * 0.5 * (1.0 + jnp.tanh((SLOPE_MAX - jnp.abs(slope)) / SLOPE_WIDTH))


def column(rho, wet, up, dn):
    hi = wet * dn(wet)
    strat = (dn(rho) - rho) * hi
    return rho, wet, hi, up(hi), 0.5 * (strat + up(strat))


def line(c, p, m, up, dn):
    c_rho, c_wet, c_hi, c_lo, c_cell = c
    p_rho, p_wet, p_hi, p_lo, p_cell = p
    m_rho, m_wet, m_hi, m_lo, m_cell = m
    mp, mm = c_wet * p_wet, c_wet * m_wet
    sp = taper((p_rho - c_rho) * mp / jnp.maximum(0.5 * (p_cell + c_cell), 1.0))
    sm = taper((c_rho - m_rho) * mm / jnp.maximum(0.5 * (m_cell + c_cell), 1.0))
    cx = 0.5 * (sp + sm)
    sw = 0.5 * (cx + dn(cx))
    fh = ((REDI + SKEW) * 0.25) * sw * c_hi
    zh = REDI * (sw * sw) * c_hi
    fl, zl = up(fh), up(zh)
    pp = ((REDI - SKEW) * 0.25) * sp * mp
    pm = -((REDI - SKEW) * 0.25) * sm * mm
    own_p, own_m = mp * (fh - fl), mm * (fl - fh)
    mph, mmh = dn(mp) * fh, dn(mm) * fh
    mpl, mml = up(mp) * fl, up(mm) * fl
    q = pp + pm
    return (
        (mpl - mml - q * c_lo + zl,
         q * (c_lo - c_hi) - REDI * (mp + mm) - (own_p + own_m) - (zh + zl),
         mmh - mph + q * c_hi + zh),
        (-pp * p_lo - mpl, REDI * mp + pp * (p_lo - p_hi) + own_p, pp * p_hi + mph),
        (mml - pm * m_lo, REDI * mm + pm * (m_lo - m_hi) + own_m, pm * m_hi - mmh),
    )


def total(terms):
    result = terms[0]
    for term in terms[1:]:
        result = result + term
    return result


def kernel(sizes, x_ref, kmt_ref, out_ref, add_ref, *scratch):
    pl.run_scoped(
        functools.partial(body, sizes, x_ref, kmt_ref, out_ref, add_ref, *scratch),
        pltpu.SemaphoreType.DMA((len(sizes[-1]) + 1,)),
        pltpu.SemaphoreType.DMA((5,)),
    )


def body(
    sizes, x_ref, kmt_ref, out_ref, add_ref,
    xv, kmt_int, coef, wcol, ecol, inner_w, inner_e, west, east, relay, from_n, from_s,
    recv_sem, load_sem, send_sem,
):
    tracers, levels, rows, lanes, n_lon, n_lat, groups = sizes
    lon, lat = lax.axis_index("lon"), lax.axis_index("lat")
    at_top = lat == n_lat - 1
    below_top = jnp.logical_not(at_top)
    inner = lat > 0
    at_bottom = jnp.logical_not(inner)
    even_lat = jnp.logical_and(inner, jnp.logical_and(lat % 2 == 0, below_top))
    odd_lat = jnp.logical_and(lat > 1, lat % 2 == 1)
    relayed = jnp.logical_and(lon == 0, even_lat)
    relays = jnp.logical_and(lon == 0, odd_lat)
    far = jnp.logical_and(lon == n_lon - 1, even_lat)
    direct, near = jnp.logical_not(relayed), jnp.logical_not(far)
    early = jnp.logical_and(lon == 0, direct)
    late = jnp.logical_not(early)
    late_top, late_below = jnp.logical_and(late, at_top), jnp.logical_and(late, below_top)
    e_dev = (lax.rem(lon + 1, n_lon), lat)
    w_dev = (lax.rem(lon + n_lon - 1, n_lon), lat)
    n_dev, s_dev = (lon, lat + 1), (lon, lat - 1)
    lat_up, lat_down = lax.rem(lat + 1, n_lat), lax.rem(lat + n_lat - 1, n_lat)
    fold_dev = (n_lon - 1 - lon, lat)
    tiles = tracers * levels
    plane = levels * rows
    lead = levels
    ends = [sum(groups[:i]) for i in range(len(groups) + 1)]
    slot = tracers + 2
    per = (lanes - 2) // slot
    regs = (levels + per - 1) // per

    barrier = pltpu.get_barrier_semaphore()

    def greet(dev):
        pl.semaphore_signal(barrier, inc=1, device_id=dev, device_id_type=MESH)

    with jax.named_scope("greet"):
        greet(w_dev)

        @pl.when(near)
        def _():
            greet(e_dev)

        @pl.when(far)
        def _():
            greet((0, lat_up))

        @pl.when(at_top)
        def _():
            greet(fold_dev)

        @pl.when(below_top)
        def _():
            greet(n_dev)

        @pl.when(inner)
        def _():
            greet(s_dev)

    load_kmt = pltpu.make_async_copy(kmt_ref, kmt_int, load_sem.at[len(groups)])
    load_kmt.start()

    def load(first, count, i):
        return pltpu.make_async_copy(
            x_ref.at[pl.ds(first, count)], xv.at[pl.ds(lead + first, count)], load_sem.at[i]
        )

    for i in range(len(groups)):
        for t in range(ends[i], ends[i + 1]):
            load(t * levels, levels, i).start()
    loads = [load(ends[i] * levels, groups[i] * levels, i) for i in range(len(groups))]
    flat = xv.reshape((lead + tiles) * rows, lanes)

    lane = lax.broadcasted_iota(jnp.int32, (rows, lanes), 1)
    row = lax.broadcasted_iota(jnp.int32, (rows, lanes), 0)

    def pick(value, index):
        return jnp.take_along_axis(value, index, axis=1)

    def send(src, dst, s, r, dev):
        return pltpu.make_async_remote_copy(
            src_ref=src, dst_ref=dst, send_sem=send_sem.at[s], recv_sem=recv_sem.at[r],
            device_id=dev, device_id_type=MESH,
        )

    def rows_of(r, span, dst, s, into, dev):
        return send(xv.at[span, r, :], dst.at[span], s, into, dev)

    cut = lead + ends[-2] * levels
    starts = [lead - 1] + [lead + e * levels for e in ends[1:]]
    spans = [pl.ds(a, b - a) for a, b in zip(starts, starts[1:])]
    every = pl.ds(lead - 1, tiles + 1)
    halves = [(pl.ds(lead - 1, cut - lead + 1), 0), (spans[-1], 5)]
    fold = rows_of(rows - 1, every, from_n, 0, 0, fold_dev)
    folds = [
        rows_of(rows - 1, span, from_n, 0, 5 if i == len(spans) - 1 else 0, fold_dev)
        for i, span in enumerate(spans)
    ]
    to_n = rows_of(rows - 1, every, from_s, 0, 1, n_dev)
    to_s = rows_of(0, every, from_n, 1, 0, s_dev)
    to_ss = [rows_of(0, span, from_n, 1, r, s_dev) for span, r in halves]
    to_e = send(ecol, west, 2, 2, e_dev)
    to_w = send(wcol, east, 3, 3, w_dev)
    to_relay = send(wcol, relay, 3, 4, (lon, lat_up))
    onward = send(relay, east, 4, 3, (n_lon - 1, lat_down))

    def tile(t, k):
        return flat[pl.ds(lead * rows + t * plane + k * rows, rows), :]

    def density(k):
        return HALINE * tile(1, k) - THERMAL * tile(0, k)

    def gather_columns(e_ref, w_ref, e_off, w_off, before=None):
        zeros = jnp.zeros((rows, lanes), jnp.float32)
        es, ws = [zeros] * regs, [zeros] * regs

        def place(value, at, reg):
            value = pltpu.roll(value, at + 1, 1)
            es[reg] = jnp.where(lane == (at + e_off) % lanes, value, es[reg])
            ws[reg] = jnp.where(lane == (at + w_off) % lanes, value, ws[reg])

        for i in range(len(groups)):
            if before is not None:
                before(i)
            if i == 0:
                place(kmt_own, per * slot, 0)
                for k in range(levels):
                    place(density(k), k % per * slot + tracers, k // per)
            for t in range(ends[i], ends[i + 1]):
                for k in range(levels):
                    place(tile(t, k), k % per * slot + t, k // per)
        for j in range(regs):
            e_ref[pl.ds(j * rows, rows), :] = es[j]
            w_ref[pl.ds(j * rows, rows), :] = ws[j]

    def enter():
        @pl.when(at_bottom)
        def _():
            pl.semaphore_wait(barrier, 3)

        @pl.when(jnp.logical_and(inner, jnp.logical_not(jnp.logical_or(relayed, relays))))
        def _():
            pl.semaphore_wait(barrier, 4)

        @pl.when(relayed)
        def _():
            pl.semaphore_wait(barrier, 3)

        @pl.when(relays)
        def _():
            pl.semaphore_wait(barrier, 5)

    def send_inner_rows():
        @pl.when(below_top)
        def _():
            to_n.start()

        @pl.when(inner)
        def _():
            for copy in to_ss:
                copy.start()

    def before(i):
        with jax.named_scope(f"load{i}"):
            loads[i].wait()
        if i == 0:

            @pl.when(late_top)
            def _():
                enter()

        if i < len(groups) - 1:

            @pl.when(late_top)
            def _():
                folds[i].start()

        else:

            @pl.when(late_below)
            def _():
                with jax.named_scope("barrier"):
                    enter()

    with jax.named_scope("loadk"):
        load_kmt.wait()
    kmt_own = kmt_int[...].astype(jnp.float32)
    xv[lead - 1, :, :] = kmt_own
    gather_columns(ecol, wcol, 0, 1, before)
    with jax.named_scope("send"):

        @pl.when(late)
        def _():
            to_e.start()

        @pl.when(jnp.logical_and(late, direct))
        def _():
            to_w.start()

        @pl.when(relayed)
        def _():
            to_relay.start()

        @pl.when(late_top)
        def _():
            folds[-1].start()

        @pl.when(late)
        def _():
            send_inner_rows()

    with jax.named_scope("inner"):
        gather_columns(inner_e, inner_w, -1, 2)

        @pl.when(at_bottom)
        def _():
            for t in range(tracers + 1):
                from_s[pl.ds(t * levels, levels), :] = jnp.zeros((levels, lanes), jnp.float32)

    def put(d, dk, k, value):
        coef[pl.ds(((d * 3 + dk) * levels + k) * rows, rows), :] = value

    def piece_of(d, dk, k):
        return coef[pl.ds(((d * 3 + dk) * levels + k) * rows, rows), :]

    with jax.named_scope("coefs"):
        none = jnp.zeros((1, rows, lanes), jnp.float32)

        def up3(v):
            return jnp.concatenate([none, v[:-1]], axis=0)

        def dn3(v):
            return jnp.concatenate([v[1:], none], axis=0)

        def shifted(v, by, axis):
            return jnp.stack([pltpu.roll(v[k], by, axis) for k in range(levels)])

        own_rho = jnp.stack([density(k) for k in range(levels)])
        own_wet = jnp.stack([(kmt_own > float(k)).astype(jnp.float32) for k in range(levels)])
        c3 = column(own_rho, own_wet, up3, dn3)

        def moved(by, axis):
            return tuple(shifted(v, by, axis) for v in c3)

        mid_lane = jnp.logical_and(lane > 0, lane < lanes - 1)
        xc, xe, xw = line(c3, moved(lanes - 1, 1), moved(1, 1), up3, dn3)
        for dk in range(3):
            for k in range(levels):
                put(E, dk, k, jnp.where(mid_lane, xe[dk][k], 0.0))
                put(W, dk, k, jnp.where(mid_lane, xw[dk][k], 0.0))
                put(C, dk, k, jnp.where(mid_lane, xc[dk][k], 0.0))
        mid_row = jnp.logical_and(row > 0, row < rows - 1)
        yc, yn, ys = line(c3, moved(rows - 1, 0), moved(1, 0), up3, dn3)
        for dk in range(3):
            for k in range(levels):
                put(N, dk, k, jnp.where(mid_row, yn[dk][k], 0.0))
                put(S, dk, k, jnp.where(mid_row, ys[dk][k], 0.0))
                both = piece_of(C, dk, k) + jnp.where(mid_row, yc[dk][k], 0.0)
                put(C, dk, k, both + 1.0 if dk == 1 else both)

    with jax.named_scope("main"):

        @pl.loop(0, tracers // TOGETHER)
        def _(i):
            fields = []
            for u in range(TOGETHER):
                base = pl.multiple_of(lead * rows + (i * TOGETHER + u) * plane, rows)
                field = []
                for k in range(levels):
                    own = flat[pl.ds(base + k * rows, rows), :]
                    field.append((
                        own, pltpu.roll(own, lanes - 1, 1), pltpu.roll(own, 1, 1),
                        pltpu.roll(own, rows - 1, 0), pltpu.roll(own, 1, 0),
                    ))
                fields.append(field)
            for k in range(levels):
                sums = [None] * TOGETHER
                for d in range(5):
                    for dk in range(3):
                        if not 0 <= k + dk - 1 < levels:
                            continue
                        c = piece_of(d, dk, k)
                        for u in range(TOGETHER):
                            term = c * fields[u][k + dk - 1][d]
                            sums[u] = term if sums[u] is None else sums[u] + term
                for u in range(TOGETHER):
                    base = pl.multiple_of((i * TOGETHER + u) * plane, rows)
                    out_ref[pl.ds(base + k * rows, rows), :] = sums[u]

    @pl.when(early)
    def _():
        with jax.named_scope("barrier"):
            enter()
        to_e.start()
        to_w.start()
        send_inner_rows()

        @pl.when(at_top)
        def _():
            for copy in folds:
                copy.start()

    @pl.when(relays)
    def _():
        to_relay.wait_recv()
        onward.start()

    level = lax.broadcasted_iota(jnp.int32, (levels, lanes), 0)
    level_f = level.astype(jnp.float32)

    def up_s(v):
        return jnp.where(level == 0, 0.0, pltpu.roll(v, 1, 0))

    def dn_s(v):
        return jnp.where(level == levels - 1, 0.0, pltpu.roll(v, levels - 1, 0))

    def at_row(t, r):
        return flat[pl.ds(lead * rows + t * plane + r, levels, stride=rows), :]

    def row_column(t0, t1, kmt):
        wet = (jnp.broadcast_to(kmt, (levels, lanes)) > level_f).astype(jnp.float32)
        return column(HALINE * t1 - THERMAL * t0, wet, up_s, dn_s)

    def own_row(r):
        return row_column(at_row(0, r), at_row(1, r), kmt_own[r : r + 1, :])

    def fix_rows(source, r, r_in, north, turn, parts):
        def halo(t):
            h = source[pl.ds(lead + t * levels, levels), :]
            return pick(h, lanes - 1 - lane) if turn else h

        first, last, wait = parts[0]
        wait()
        k = jnp.broadcast_to(source[pl.ds(lead - 1, 1), :], (rows, lanes))
        k = (pick(k, lanes - 1 - lane) if turn else k)[:1, :]
        out_c, in_c = row_column(halo(0), halo(1), k), own_row(r_in)
        p, m = (out_c, in_c) if north else (in_c, out_c)
        cc, cp, cm = line(own_row(r), p, m, up_s, dn_s)
        c_out, c_in = (cp, cm) if north else (cm, cp)
        table = (cc, c_out, c_in)
        lo = [pltpu.roll(c[0], levels - 1, 0) for c in table]
        mid = [c[1] for c in table]
        hi = [pltpu.roll(c[2], 1, 0) for c in table]
        for n, (first, last, wait) in enumerate(parts):
            if n:
                wait()
            count = last - first
            batch = next(b for b in (16, 12, 8, 4, 2, 1) if count % b == 0 and (turn or b <= 8))

            @pl.loop(0, count // batch)
            def _(i, first=first, batch=batch):
                for u in range(batch):
                    t = first + i * batch + u
                    values = (at_row(t, r), halo(t), at_row(t, r_in))
                    above = total([c * v for c, v in zip(lo, values)])
                    same = total([c * v for c, v in zip(mid, values)])
                    below = total([c * v for c, v in zip(hi, values)])
                    place = pl.ds(t * plane + r, levels, stride=rows)
                    out_ref[place, :] = (
                        out_ref[place, :] + same + pltpu.roll(above, 1, 0) + pltpu.roll(below, levels - 1, 0)
                    )

    def fix_n(turn):
        parts = [(0, ends[-2], to_ss[0].wait_recv), (ends[-2], tracers, to_ss[1].wait_recv)]
        fix_rows(from_n, rows - 1, rows - 2, True, turn, parts)

    with jax.named_scope("fixs"):

        @pl.when(inner)
        def _():
            to_n.wait_recv()

        fix_rows(from_s, 0, 1, False, False, [(0, tracers, lambda: None)])

    with jax.named_scope("fixn"):

        @pl.when(below_top)
        def _():
            fix_n(False)

    west_side = lane % 2 == 0
    spot = jnp.minimum((lane + 1) // 2 % (lanes // 2), tracers - 1)

    def both(w_ref, e_ref, w_off, e_off, at, k):
        base, span = k % per * slot, pl.ds(k // per * rows, rows)
        w_at = (base + at + w_off + lanes) % lanes
        e_at = (base + at + e_off + lanes) % lanes
        return jnp.where(west_side, pick(w_ref[span, :], w_at), pick(e_ref[span, :], e_at))

    def edge(w_ref, e_ref, w_off, e_off):
        args = (w_ref, e_ref, w_off, e_off)
        fixed = jnp.full((rows, lanes), tracers, jnp.int32)
        values = jnp.stack([both(*args, spot, k) for k in range(levels)])
        rho = jnp.stack([both(*args, fixed, k) for k in range(levels)])
        kmt = both(*args, jnp.full((rows, lanes), per * slot, jnp.int32), 0)
        wet = jnp.stack([(kmt > float(k)).astype(jnp.float32) for k in range(levels)])
        return values, column(rho, wet, up3, dn3)

    with jax.named_scope("fixc0"):
        own, own_c = edge(wcol, ecol, 1, 0)
        ins, ins_c = edge(inner_w, inner_e, 2, -1)
    with jax.named_scope("waitc"):
        to_e.wait_recv()
        to_w.wait_recv()
    with jax.named_scope("fixc1"):
        outs, outs_c = edge(west, east, 0, 1)
        table = line(own_c, outs_c, ins_c, up3, dn3)
        values = (own, outs, ins)
        above = total([c[0] * up3(v) for c, v in zip(table, values)])
        same = total([c[1] * v for c, v in zip(table, values)])
        below = total([c[2] * dn3(v) for c, v in zip(table, values)])
        for k in range(levels):
            add_ref[pl.ds(k * rows, rows), :] = same[k] + above[k] + below[k]

    with jax.named_scope("fixtop"):

        @pl.when(at_top)
        def _():
            fix_n(True)

    with jax.named_scope("end"):
        fold.wait_send()

        @pl.when(inner)
        def _():
            to_s.wait_send()

        to_e.wait_send()
        to_w.wait_send()

        @pl.when(relays)
        def _():
            onward.wait_send()


def finish(sizes, part_ref, add_ref, out_ref, stage, sem):
    tracers, levels, rows, lanes = sizes
    plane = levels * rows
    lane = lax.broadcasted_iota(jnp.int32, (rows, lanes), 1)
    sides = jnp.logical_or(lane == 0, lane == lanes - 1)
    add = [add_ref[pl.ds(k * rows, rows), :] for k in range(levels)]
    with jax.named_scope("insert"):
        for t in range(tracers):
            for k in range(levels):
                term = pltpu.roll(add[k], (lanes - 2 * t) % lanes, 1)
                place = pl.ds(t * plane + k * rows, rows)
                stage[place, :] = part_ref[place, :] + jnp.where(sides, term, 0.0)
            if t % STORE == 0 or t == tracers - 1:
                first = 0 if t == 0 else (t - 1) // STORE * STORE + 1
                span = pl.ds(first * plane, (t + 1 - first) * plane)
                pltpu.make_async_copy(stage.at[span], out_ref.at[span], sem).start()
    with jax.named_scope("written"):
        pltpu.make_async_copy(stage, out_ref, sem).wait()


def solution(mesh):
    n_lon, n_lat = mesh.shape["lon"], mesh.shape["lat"]

    def local(tracers, kmt):
        nt, levels, rows, lanes = tracers.shape
        tiles = nt * levels
        per = (lanes - 2) // (nt + 2)
        regs = (levels + per - 1) // per
        groups = (nt // 5, 2 * nt // 5, nt - nt // 5 - 2 * nt // 5)
        assert levels == rows and per > 0

        def vmem(*shape):
            return pltpu.VMEM(shape, jnp.float32)

        part, add = pl.pallas_call(
            functools.partial(kernel, (nt, levels, rows, lanes, n_lon, n_lat, groups)),
            out_shape=[vmem(tiles * rows, lanes), vmem(levels * rows, lanes)],
            in_specs=[pl.BlockSpec(memory_space=pltpu.HBM), pl.BlockSpec(memory_space=pltpu.HBM)],
            out_specs=[pl.BlockSpec(memory_space=pltpu.VMEM)] * 2,
            scratch_shapes=[
                vmem(tiles + levels, rows, lanes),
                pltpu.VMEM((rows, lanes), jnp.int32),
                vmem(15 * levels * rows, lanes),
            ]
            + [vmem(regs * rows, lanes)] * 7
            + [vmem(tiles + rows, lanes)] * 2
            + [
                pltpu.SemaphoreType.DMA((6,)),
            ],
            compiler_params=pltpu.CompilerParams(collective_id=0, has_side_effects=True),
        )(tracers.reshape(tiles, rows, lanes), kmt)
        part, add = (pltpu.with_memory_space_constraint(v, pltpu.VMEM) for v in (part, add))
        out = pl.pallas_call(
            functools.partial(finish, (nt, levels, rows, lanes)),
            out_shape=jax.ShapeDtypeStruct((tiles * rows, lanes), jnp.float32),
            in_specs=[pl.BlockSpec(memory_space=pltpu.VMEM)] * 2,
            out_specs=pl.BlockSpec(memory_space=pltpu.HBM),
            scratch_shapes=[vmem(tiles * rows, lanes), pltpu.SemaphoreType.DMA],
        )(part, add)
        return out.reshape(nt, levels, rows, lanes)

    return jax.shard_map(
        local,
        mesh=mesh,
        in_specs=(P(None, None, "lat", "lon"), P("lat", "lon")),
        out_specs=P(None, None, "lat", "lon"),
        check_vma=False,
    )
```

```python
import functools

import jax
import jax.numpy as jnp
from jax import lax
from jax.experimental import pallas as pl
from jax.experimental.pallas import tpu as pltpu
from jax.sharding import PartitionSpec as P

THERMAL = 0.2
HALINE = 0.8
REDI = 0.1
SKEW = 0.05
SLOPE_MAX = 0.6
SLOPE_WIDTH = 0.2

MESH = pl.DeviceIdType.MESH
TOGETHER = 2
STORE = 2
C, E, W, N, S = range(5)


def taper(slope):
    return slope * 0.5 * (1.0 + jnp.tanh((SLOPE_MAX - jnp.abs(slope)) / SLOPE_WIDTH))


def column(rho, wet, up, dn):
    hi = wet * dn(wet)
    strat = (dn(rho) - rho) * hi
    return rho, wet, hi, up(hi), 0.5 * (strat + up(strat))


def line(c, p, m, up, dn):
    c_rho, c_wet, c_hi, c_lo, c_cell = c
    p_rho, p_wet, p_hi, p_lo, p_cell = p
    m_rho, m_wet, m_hi, m_lo, m_cell = m
    mp, mm = c_wet * p_wet, c_wet * m_wet
    sp = taper((p_rho - c_rho) * mp / jnp.maximum(0.5 * (p_cell + c_cell), 1.0))
    sm = taper((c_rho - m_rho) * mm / jnp.maximum(0.5 * (m_cell + c_cell), 1.0))
    cx = 0.5 * (sp + sm)
    sw = 0.5 * (cx + dn(cx))
    fh = ((REDI + SKEW) * 0.25) * sw * c_hi
    zh = REDI * (sw * sw) * c_hi
    fl, zl = up(fh), up(zh)
    pp = ((REDI - SKEW) * 0.25) * sp * mp
    pm = -((REDI - SKEW) * 0.25) * sm * mm
    own_p, own_m = mp * (fh - fl), mm * (fl - fh)
    mph, mmh = dn(mp) * fh, dn(mm) * fh
    mpl, mml = up(mp) * fl, up(mm) * fl
    q = pp + pm
    return (
        (mpl - mml - q * c_lo + zl,
         q * (c_lo - c_hi) - REDI * (mp + mm) - (own_p + own_m) - (zh + zl),
         mmh - mph + q * c_hi + zh),
        (-pp * p_lo - mpl, REDI * mp + pp * (p_lo - p_hi) + own_p, pp * p_hi + mph),
        (mml - pm * m_lo, REDI * mm + pm * (m_lo - m_hi) + own_m, pm * m_hi - mmh),
    )


def total(terms):
    result = terms[0]
    for term in terms[1:]:
        result = result + term
    return result


def kernel(sizes, x_ref, kmt_ref, out_ref, add_ref, *scratch):
    pl.run_scoped(
        functools.partial(body, sizes, x_ref, kmt_ref, out_ref, add_ref, *scratch),
        pltpu.SemaphoreType.DMA((len(sizes[-1]) + 1,)),
        pltpu.SemaphoreType.DMA((5,)),
    )


def body(
    sizes, x_ref, kmt_ref, out_ref, add_ref,
    xv, kmt_int, coef, wcol, ecol, inner_w, inner_e, west, east, relay, from_n, from_s,
    recv_sem, load_sem, send_sem,
):
    tracers, levels, rows, lanes, n_lon, n_lat, groups = sizes
    lon, lat = lax.axis_index("lon"), lax.axis_index("lat")
    at_top = lat == n_lat - 1
    below_top = jnp.logical_not(at_top)
    inner = lat > 0
    at_bottom = jnp.logical_not(inner)
    even_lat = jnp.logical_and(inner, jnp.logical_and(lat % 2 == 0, below_top))
    odd_lat = jnp.logical_and(lat > 1, lat % 2 == 1)
    relayed = jnp.logical_and(lon == 0, even_lat)
    relays = jnp.logical_and(lon == 0, odd_lat)
    far = jnp.logical_and(lon == n_lon - 1, even_lat)
    direct, near = jnp.logical_not(relayed), jnp.logical_not(far)
    early = jnp.logical_and(lon == 0, direct)
    late = jnp.logical_not(early)
    late_top, late_below = jnp.logical_and(late, at_top), jnp.logical_and(late, below_top)
    e_dev = (lax.rem(lon + 1, n_lon), lat)
    w_dev = (lax.rem(lon + n_lon - 1, n_lon), lat)
    n_dev, s_dev = (lon, lat + 1), (lon, lat - 1)
    lat_up, lat_down = lax.rem(lat + 1, n_lat), lax.rem(lat + n_lat - 1, n_lat)
    fold_dev = (n_lon - 1 - lon, lat)
    tiles = tracers * levels
    plane = levels * rows
    lead = levels
    ends = [sum(groups[:i]) for i in range(len(groups) + 1)]
    split = ends[-2]
    slots = (split + 2, tracers - split)
    pers = tuple((lanes - 2) // slot for slot in slots)
    shares = tuple((levels + per - 1) // per for per in pers)
    kmt_at = pers[0] * slots[0]

    load_kmt = pltpu.make_async_copy(kmt_ref, kmt_int, load_sem.at[len(groups)])
    load_kmt.start()

    def load(first, count, i):
        return pltpu.make_async_copy(
            x_ref.at[pl.ds(first, count)], xv.at[pl.ds(lead + first, count)], load_sem.at[i]
        )

    for i in range(len(groups)):
        for t in range(ends[i], ends[i + 1]):
            load(t * levels, levels, i).start()
    loads = [load(ends[i] * levels, groups[i] * levels, i) for i in range(len(groups))]
    flat = xv.reshape((lead + tiles) * rows, lanes)

    barrier = pltpu.get_barrier_semaphore()

    def greet(dev):
        pl.semaphore_signal(barrier, inc=1, device_id=dev, device_id_type=MESH)

    with jax.named_scope("greet"):
        greet(w_dev)

        @pl.when(near)
        def _():
            greet(e_dev)

        @pl.when(far)
        def _():
            greet((0, lat_up))

        @pl.when(at_top)
        def _():
            greet(fold_dev)

        @pl.when(below_top)
        def _():
            greet(n_dev)

        @pl.when(inner)
        def _():
            greet(s_dev)

    lane = lax.broadcasted_iota(jnp.int32, (rows, lanes), 1)
    row = lax.broadcasted_iota(jnp.int32, (rows, lanes), 0)

    def pick(value, index):
        return jnp.take_along_axis(value, index, axis=1)

    def send(src, dst, s, r, dev):
        return pltpu.make_async_remote_copy(
            src_ref=src, dst_ref=dst, send_sem=send_sem.at[s], recv_sem=recv_sem.at[r],
            device_id=dev, device_id_type=MESH,
        )

    def rows_of(r, span, dst, s, into, dev):
        return send(xv.at[span, r, :], dst.at[span], s, into, dev)

    cut = lead + ends[-2] * levels
    starts = [lead - 1] + [lead + e * levels for e in ends[1:]]
    spans = [pl.ds(a, b - a) for a, b in zip(starts, starts[1:])]
    every = pl.ds(lead - 1, tiles + 1)
    halves = [(pl.ds(lead - 1, cut - lead + 1), 0), (spans[-1], 5)]
    fold = rows_of(rows - 1, every, from_n, 0, 0, fold_dev)
    folds = [
        rows_of(rows - 1, span, from_n, 0, 5 if i == len(spans) - 1 else 0, fold_dev)
        for i, span in enumerate(spans)
    ]
    to_n = rows_of(rows - 1, every, from_s, 0, 1, n_dev)
    to_s = rows_of(0, every, from_n, 1, 0, s_dev)
    to_ss = [rows_of(0, span, from_n, 1, r, s_dev) for span, r in halves]
    cols = (pl.ds(0, shares[0] * rows), pl.ds(shares[0] * rows, shares[1] * rows))
    far_dev = (n_lon - 1, lat_down)
    to_e = [send(ecol.at[c], west.at[c], 2, (2, 6)[i], e_dev) for i, c in enumerate(cols)]
    to_w = [send(wcol.at[c], east.at[c], 3, (3, 7)[i], w_dev) for i, c in enumerate(cols)]
    onward = [send(relay.at[c], east.at[c], 4, (3, 7)[i], far_dev) for i, c in enumerate(cols)]
    to_relay = send(wcol, relay, 3, 4, (lon, lat_up))
    all_e, all_w = send(ecol, west, 2, 2, e_dev), send(wcol, east, 3, 3, w_dev)
    all_onward = send(relay, east, 4, 3, far_dev)

    def tile(t, k):
        return flat[pl.ds(lead * rows + t * plane + k * rows, rows), :]

    def density(k):
        return HALINE * tile(1, k) - THERMAL * tile(0, k)

    def where_is(t, k):
        n, u = (0, t) if t < split else (1, t - split)
        return k % pers[n] * slots[n] + u, n * shares[0] + k // pers[n]

    def gather_columns(e_ref, w_ref, e_off, w_off, before=None, after=None):
        zeros = jnp.zeros((rows, lanes), jnp.float32)
        es, ws = [zeros] * sum(shares), [zeros] * sum(shares)

        def place(value, at, reg):
            value = pltpu.roll(value, at + 1, 1)
            es[reg] = jnp.where(lane == (at + e_off) % lanes, value, es[reg])
            ws[reg] = jnp.where(lane == (at + w_off) % lanes, value, ws[reg])

        for i in range(len(groups)):
            if before is not None:
                before(i)
            if i == 0:
                place(kmt_own, kmt_at, 0)
                for k in range(levels):
                    at, reg = where_is(0, k)
                    place(density(k), at + split, reg)
            for t in range(ends[i], ends[i + 1]):
                for k in range(levels):
                    place(tile(t, k), *where_is(t, k))
            if ends[i + 1] in (split, tracers):
                n = 0 if ends[i + 1] == split else 1
                for j in range(n * shares[0], n * shares[0] + shares[n]):
                    e_ref[pl.ds(j * rows, rows), :] = es[j]
                    w_ref[pl.ds(j * rows, rows), :] = ws[j]
                if after is not None:
                    after(n)

    def enter():
        @pl.when(at_bottom)
        def _():
            pl.semaphore_wait(barrier, 3)

        @pl.when(jnp.logical_and(inner, jnp.logical_not(jnp.logical_or(relayed, relays))))
        def _():
            pl.semaphore_wait(barrier, 4)

        @pl.when(relayed)
        def _():
            pl.semaphore_wait(barrier, 3)

        @pl.when(relays)
        def _():
            pl.semaphore_wait(barrier, 5)

    def send_inner_rows():
        @pl.when(below_top)
        def _():
            to_n.start()

        @pl.when(inner)
        def _():
            for copy in to_ss:
                copy.start()

    def before(i):
        with jax.named_scope(f"load{i}"):
            loads[i].wait()
        if i == 0:

            @pl.when(late_top)
            def _():
                enter()

        if i < len(groups) - 1:

            @pl.when(late_top)
            def _():
                folds[i].start()

    def after(n):
        if n == 0:

            @pl.when(late_below)
            def _():
                with jax.named_scope("barrier"):
                    enter()

        @pl.when(late)
        def _():
            to_e[n].start()

        @pl.when(jnp.logical_and(late, direct))
        def _():
            to_w[n].start()

    with jax.named_scope("loadk"):
        load_kmt.wait()
    kmt_own = kmt_int[...].astype(jnp.float32)
    xv[lead - 1, :, :] = kmt_own
    gather_columns(ecol, wcol, 0, 1, before, after)
    with jax.named_scope("send"):

        @pl.when(relayed)
        def _():
            to_relay.start()

        @pl.when(late_top)
        def _():
            folds[-1].start()

        @pl.when(late)
        def _():
            send_inner_rows()

    with jax.named_scope("inner"):
        gather_columns(inner_e, inner_w, -1, 2)

        @pl.when(at_bottom)
        def _():
            for t in range(tracers + 1):
                from_s[pl.ds(t * levels, levels), :] = jnp.zeros((levels, lanes), jnp.float32)

    def put(d, dk, k, value):
        coef[pl.ds(((d * 3 + dk) * levels + k) * rows, rows), :] = value

    def piece_of(d, dk, k):
        return coef[pl.ds(((d * 3 + dk) * levels + k) * rows, rows), :]

    with jax.named_scope("coefs"):
        none = jnp.zeros((1, rows, lanes), jnp.float32)

        def up3(v):
            return jnp.concatenate([none, v[:-1]], axis=0)

        def dn3(v):
            return jnp.concatenate([v[1:], none], axis=0)

        def shifted(v, by, axis):
            return jnp.stack([pltpu.roll(v[k], by, axis) for k in range(levels)])

        own_rho = jnp.stack([density(k) for k in range(levels)])
        own_wet = jnp.stack([(kmt_own > float(k)).astype(jnp.float32) for k in range(levels)])
        c3 = column(own_rho, own_wet, up3, dn3)

        def moved(by, axis):
            return tuple(shifted(v, by, axis) for v in c3)

        mid_lane = jnp.logical_and(lane > 0, lane < lanes - 1)
        xc, xe, xw = line(c3, moved(lanes - 1, 1), moved(1, 1), up3, dn3)
        for dk in range(3):
            for k in range(levels):
                put(E, dk, k, jnp.where(mid_lane, xe[dk][k], 0.0))
                put(W, dk, k, jnp.where(mid_lane, xw[dk][k], 0.0))
                put(C, dk, k, jnp.where(mid_lane, xc[dk][k], 0.0))
        mid_row = jnp.logical_and(row > 0, row < rows - 1)
        yc, yn, ys = line(c3, moved(rows - 1, 0), moved(1, 0), up3, dn3)
        for dk in range(3):
            for k in range(levels):
                put(N, dk, k, jnp.where(mid_row, yn[dk][k], 0.0))
                put(S, dk, k, jnp.where(mid_row, ys[dk][k], 0.0))
                both = piece_of(C, dk, k) + jnp.where(mid_row, yc[dk][k], 0.0)
                put(C, dk, k, both + 1.0 if dk == 1 else both)

    with jax.named_scope("main"):

        @pl.loop(0, tracers // TOGETHER)
        def _(i):
            fields = []
            for u in range(TOGETHER):
                base = pl.multiple_of(lead * rows + (i * TOGETHER + u) * plane, rows)
                field = []
                for k in range(levels):
                    own = flat[pl.ds(base + k * rows, rows), :]
                    field.append((
                        own, pltpu.roll(own, lanes - 1, 1), pltpu.roll(own, 1, 1),
                        pltpu.roll(own, rows - 1, 0), pltpu.roll(own, 1, 0),
                    ))
                fields.append(field)
            for k in range(levels):
                sums = [None] * TOGETHER
                for d in range(5):
                    for dk in range(3):
                        if not 0 <= k + dk - 1 < levels:
                            continue
                        c = piece_of(d, dk, k)
                        for u in range(TOGETHER):
                            term = c * fields[u][k + dk - 1][d]
                            sums[u] = term if sums[u] is None else sums[u] + term
                for u in range(TOGETHER):
                    base = pl.multiple_of((i * TOGETHER + u) * plane, rows)
                    out_ref[pl.ds(base + k * rows, rows), :] = sums[u]

    @pl.when(early)
    def _():
        with jax.named_scope("barrier"):
            enter()
        for copy in to_e + to_w:
            copy.start()
        send_inner_rows()

        @pl.when(at_top)
        def _():
            for copy in folds:
                copy.start()

    @pl.when(relays)
    def _():
        to_relay.wait_recv()
        for copy in onward:
            copy.start()

    level = lax.broadcasted_iota(jnp.int32, (levels, lanes), 0)
    level_f = level.astype(jnp.float32)

    def up_s(v):
        return jnp.where(level == 0, 0.0, pltpu.roll(v, 1, 0))

    def dn_s(v):
        return jnp.where(level == levels - 1, 0.0, pltpu.roll(v, levels - 1, 0))

    def at_row(t, r):
        return flat[pl.ds(lead * rows + t * plane + r, levels, stride=rows), :]

    def row_column(t0, t1, kmt):
        wet = (jnp.broadcast_to(kmt, (levels, lanes)) > level_f).astype(jnp.float32)
        return column(HALINE * t1 - THERMAL * t0, wet, up_s, dn_s)

    def own_row(r):
        return row_column(at_row(0, r), at_row(1, r), kmt_own[r : r + 1, :])

    def fix_rows(source, r, r_in, north, turn, parts):
        def halo(t):
            h = source[pl.ds(lead + t * levels, levels), :]
            return pick(h, lanes - 1 - lane) if turn else h

        first, last, wait = parts[0]
        wait()
        k = jnp.broadcast_to(source[pl.ds(lead - 1, 1), :], (rows, lanes))
        k = (pick(k, lanes - 1 - lane) if turn else k)[:1, :]
        out_c, in_c = row_column(halo(0), halo(1), k), own_row(r_in)
        p, m = (out_c, in_c) if north else (in_c, out_c)
        cc, cp, cm = line(own_row(r), p, m, up_s, dn_s)
        c_out, c_in = (cp, cm) if north else (cm, cp)
        table = (cc, c_out, c_in)
        lo = [pltpu.roll(c[0], levels - 1, 0) for c in table]
        mid = [c[1] for c in table]
        hi = [pltpu.roll(c[2], 1, 0) for c in table]
        for n, (first, last, wait) in enumerate(parts):
            if n:
                wait()
            count = last - first
            batch = next(b for b in (16, 12, 8, 4, 2, 1) if count % b == 0 and (turn or b <= 8))

            @pl.loop(0, count // batch)
            def _(i, first=first, batch=batch):
                for u in range(batch):
                    t = first + i * batch + u
                    values = (at_row(t, r), halo(t), at_row(t, r_in))
                    above = total([c * v for c, v in zip(lo, values)])
                    same = total([c * v for c, v in zip(mid, values)])
                    below = total([c * v for c, v in zip(hi, values)])
                    place = pl.ds(t * plane + r, levels, stride=rows)
                    out_ref[place, :] = (
                        out_ref[place, :] + same + pltpu.roll(above, 1, 0) + pltpu.roll(below, levels - 1, 0)
                    )

    def fix_n(turn):
        parts = [(0, ends[-2], to_ss[0].wait_recv), (ends[-2], tracers, to_ss[1].wait_recv)]
        fix_rows(from_n, rows - 1, rows - 2, True, turn, parts)

    with jax.named_scope("fixs"):

        @pl.when(inner)
        def _():
            to_n.wait_recv()

        fix_rows(from_s, 0, 1, False, False, [(0, tracers, lambda: None)])

    with jax.named_scope("fixn"):

        @pl.when(below_top)
        def _():
            fix_n(False)

    west_side = lane % 2 == 0
    spot = jnp.minimum((lane + 1) // 2 % (lanes // 2), tracers - 1)
    low = spot < split
    spots = (jnp.minimum(spot, split - 1), jnp.maximum(spot - split, 0))

    def both(refs, offs, at, reg):
        span = pl.ds(reg * rows, rows)
        picked = [pick(ref[span, :], (at + off + lanes) % lanes) for ref, off in zip(refs, offs)]
        return jnp.where(west_side, *picked)

    def values_of(refs, offs, n):
        return jnp.stack([both(refs, offs, k % pers[n] * slots[n] + spots[n], n * shares[0] + k // pers[n])
                          for k in range(levels)])

    def column_of(refs, offs):
        fixed = jnp.zeros((rows, lanes), jnp.int32)
        rho = jnp.stack([both(refs, offs, fixed + (where_is(0, k)[0] + split), where_is(0, k)[1])
                         for k in range(levels)])
        kmt = both(refs, offs, fixed + kmt_at, 0)
        wet = jnp.stack([(kmt > float(k)).astype(jnp.float32) for k in range(levels)])
        return column(rho, wet, up3, dn3)

    def joined(first, second):
        return jnp.stack([jnp.where(low, first[k], second[k]) for k in range(levels)])

    def applied(c, v):
        return c[1] * v + c[0] * up3(v) + c[2] * dn3(v)

    with jax.named_scope("fixc0"):
        own_at, ins_at, outs_at = ((wcol, ecol), (1, 0)), ((inner_w, inner_e), (2, -1)), ((west, east), (0, 1))
        own_c, ins_c = column_of(*own_at), column_of(*ins_at)
        own, ins = (joined(values_of(*at, 0), values_of(*at, 1)) for at in (own_at, ins_at))
    with jax.named_scope("waitc"):
        to_e[0].wait_recv()
        to_w[0].wait_recv()
    with jax.named_scope("fixc1"):
        own_t, outs_t, ins_t = line(own_c, column_of(*outs_at), ins_c, up3, dn3)
        some = applied(own_t, own) + applied(ins_t, ins)
        outs_0 = values_of(*outs_at, 0)
    with jax.named_scope("waitc2"):
        to_e[1].wait_recv()
        to_w[1].wait_recv()
    with jax.named_scope("fixc2"):
        add = some + applied(outs_t, joined(outs_0, values_of(*outs_at, 1)))
        for k in range(levels):
            add_ref[pl.ds(k * rows, rows), :] = add[k]

    with jax.named_scope("fixtop"):

        @pl.when(at_top)
        def _():
            fix_n(True)

    with jax.named_scope("end"):
        fold.wait_send()

        @pl.when(inner)
        def _():
            to_s.wait_send()

        all_e.wait_send()
        all_w.wait_send()

        @pl.when(relays)
        def _():
            all_onward.wait_send()


def finish(sizes, part_ref, add_ref, out_ref, stage, sem):
    tracers, levels, rows, lanes = sizes
    plane = levels * rows
    lane = lax.broadcasted_iota(jnp.int32, (rows, lanes), 1)
    sides = jnp.logical_or(lane == 0, lane == lanes - 1)
    add = [add_ref[pl.ds(k * rows, rows), :] for k in range(levels)]
    with jax.named_scope("insert"):
        for t in range(tracers):
            for k in range(levels):
                term = pltpu.roll(add[k], (lanes - 2 * t) % lanes, 1)
                place = pl.ds(t * plane + k * rows, rows)
                stage[place, :] = part_ref[place, :] + jnp.where(sides, term, 0.0)
            if t % STORE == 0 or t == tracers - 1:
                first = 0 if t == 0 else (t - 1) // STORE * STORE + 1
                span = pl.ds(first * plane, (t + 1 - first) * plane)
                pltpu.make_async_copy(stage.at[span], out_ref.at[span], sem).start()
    with jax.named_scope("written"):
        pltpu.make_async_copy(stage, out_ref, sem).wait()


def solution(mesh):
    n_lon, n_lat = mesh.shape["lon"], mesh.shape["lat"]

    def local(tracers, kmt):
        nt, levels, rows, lanes = tracers.shape
        tiles = nt * levels
        cuts = (0, nt // 10, 3 * nt // 10, 6 * nt // 10, nt)
        groups = tuple(b - a for a, b in zip(cuts, cuts[1:]))
        slots = (cuts[-2] + 2, groups[-1])
        regs = sum(-(-levels // ((lanes - 2) // slot)) for slot in slots)
        assert levels == rows and groups[0] > 1

        def vmem(*shape):
            return pltpu.VMEM(shape, jnp.float32)

        part, add = pl.pallas_call(
            functools.partial(kernel, (nt, levels, rows, lanes, n_lon, n_lat, groups)),
            out_shape=[vmem(tiles * rows, lanes), vmem(levels * rows, lanes)],
            in_specs=[pl.BlockSpec(memory_space=pltpu.HBM), pl.BlockSpec(memory_space=pltpu.HBM)],
            out_specs=[pl.BlockSpec(memory_space=pltpu.VMEM)] * 2,
            scratch_shapes=[
                vmem(tiles + levels, rows, lanes),
                pltpu.VMEM((rows, lanes), jnp.int32),
                vmem(15 * levels * rows, lanes),
            ]
            + [vmem(regs * rows, lanes)] * 7
            + [vmem(tiles + rows, lanes)] * 2
            + [
                pltpu.SemaphoreType.DMA((8,)),
            ],
            compiler_params=pltpu.CompilerParams(collective_id=0, has_side_effects=True),
        )(tracers.reshape(tiles, rows, lanes), kmt)
        part, add = (pltpu.with_memory_space_constraint(v, pltpu.VMEM) for v in (part, add))
        out = pl.pallas_call(
            functools.partial(finish, (nt, levels, rows, lanes)),
            out_shape=jax.ShapeDtypeStruct((tiles * rows, lanes), jnp.float32),
            in_specs=[pl.BlockSpec(memory_space=pltpu.VMEM)] * 2,
            out_specs=pl.BlockSpec(memory_space=pltpu.HBM),
            scratch_shapes=[vmem(tiles * rows, lanes), pltpu.SemaphoreType.DMA],
        )(part, add)
        return out.reshape(nt, levels, rows, lanes)

    return jax.shard_map(
        local,
        mesh=mesh,
        in_specs=(P(None, None, "lat", "lon"), P("lat", "lon")),
        out_specs=P(None, None, "lat", "lon"),
        check_vma=False,
    )
```

```python
import functools

import jax
import jax.numpy as jnp
from jax import lax
from jax.experimental import pallas as pl
from jax.experimental.pallas import tpu as pltpu
from jax.sharding import PartitionSpec as P

THERMAL = 0.2
HALINE = 0.8
REDI = 0.1
SKEW = 0.05
SLOPE_MAX = 0.6
SLOPE_WIDTH = 0.2

MESH = pl.DeviceIdType.MESH
TOGETHER = 2
STORE = 2
EARLY = 2
C, E, W, N, S = range(5)


def taper(slope):
    return slope * 0.5 * (1.0 + jnp.tanh((SLOPE_MAX - jnp.abs(slope)) / SLOPE_WIDTH))


def column(rho, wet, up, dn):
    hi = wet * dn(wet)
    strat = (dn(rho) - rho) * hi
    return rho, wet, hi, up(hi), 0.5 * (strat + up(strat))


def line(c, p, m, up, dn):
    c_rho, c_wet, c_hi, c_lo, c_cell = c
    p_rho, p_wet, p_hi, p_lo, p_cell = p
    m_rho, m_wet, m_hi, m_lo, m_cell = m
    mp, mm = c_wet * p_wet, c_wet * m_wet
    sp = taper((p_rho - c_rho) * mp / jnp.maximum(0.5 * (p_cell + c_cell), 1.0))
    sm = taper((c_rho - m_rho) * mm / jnp.maximum(0.5 * (m_cell + c_cell), 1.0))
    cx = 0.5 * (sp + sm)
    sw = 0.5 * (cx + dn(cx))
    fh = ((REDI + SKEW) * 0.25) * sw * c_hi
    zh = REDI * (sw * sw) * c_hi
    fl, zl = up(fh), up(zh)
    pp = ((REDI - SKEW) * 0.25) * sp * mp
    pm = -((REDI - SKEW) * 0.25) * sm * mm
    own_p, own_m = mp * (fh - fl), mm * (fl - fh)
    mph, mmh = dn(mp) * fh, dn(mm) * fh
    mpl, mml = up(mp) * fl, up(mm) * fl
    q = pp + pm
    return (
        (mpl - mml - q * c_lo + zl,
         q * (c_lo - c_hi) - REDI * (mp + mm) - (own_p + own_m) - (zh + zl),
         mmh - mph + q * c_hi + zh),
        (-pp * p_lo - mpl, REDI * mp + pp * (p_lo - p_hi) + own_p, pp * p_hi + mph),
        (mml - pm * m_lo, REDI * mm + pm * (m_lo - m_hi) + own_m, pm * m_hi - mmh),
    )


def total(terms):
    result = terms[0]
    for term in terms[1:]:
        result = result + term
    return result


def pick(value, index):
    return jnp.take_along_axis(value, index, axis=1)


def up3(v):
    return jnp.concatenate([jnp.zeros_like(v[:1]), v[:-1]], axis=0)


def dn3(v):
    return jnp.concatenate([v[1:], jnp.zeros_like(v[:1])], axis=0)


def applied(c, v):
    return c[1] * v + c[0] * up3(v) + c[2] * dn3(v)


def layout(tracers, split, levels, lanes):
    slots = (split + 2, tracers - split)
    pers = tuple((lanes - 2) // slot for slot in slots)
    return slots, pers, tuple((levels + per - 1) // per for per in pers)


def tracer_of(lane, lanes, tracers):
    return jnp.minimum((lane + 1) // 2 % (lanes // 2), tracers - 1)


def both(refs, offs, at, reg):
    rows, lanes = at.shape
    span = pl.ds(reg * rows, rows)
    west_side = lax.broadcasted_iota(jnp.int32, at.shape, 1) % 2 == 0
    picked = [pick(ref[span, :], (at + off + lanes) % lanes) for ref, off in zip(refs, offs)]
    return jnp.where(west_side, *picked)


def values_of(refs, offs, spot, per, slot, first, levels):
    return jnp.stack([both(refs, offs, k % per * slot + spot, first + k // per) for k in range(levels)])


def kernel(sizes, x_ref, kmt_ref, out_ref, add_ref, tab_ref, halo2, *scratch):
    pl.run_scoped(
        functools.partial(body, sizes, x_ref, kmt_ref, out_ref, add_ref, tab_ref, halo2, *scratch),
        pltpu.SemaphoreType.DMA((len(sizes[-1]) + 1,)),
        pltpu.SemaphoreType.DMA((5,)),
    )


def body(
    sizes, x_ref, kmt_ref, out_ref, add_ref, tab_ref, halo2,
    xv, kmt_int, coef, wcol, ecol, inner_w, inner_e, relay, halo1, from_n, from_s,
    recv_sem, load_sem, send_sem,
):
    tracers, levels, rows, lanes, n_lon, n_lat, groups = sizes
    lon, lat = lax.axis_index("lon"), lax.axis_index("lat")
    at_top = lat == n_lat - 1
    below_top = jnp.logical_not(at_top)
    inner = lat > 0
    at_bottom = jnp.logical_not(inner)
    even_lat = jnp.logical_and(inner, jnp.logical_and(lat % 2 == 0, below_top))
    odd_lat = jnp.logical_and(lat > 1, lat % 2 == 1)
    relayed = jnp.logical_and(lon == 0, even_lat)
    relays = jnp.logical_and(lon == 0, odd_lat)
    far = jnp.logical_and(lon == n_lon - 1, even_lat)
    direct, near = jnp.logical_not(relayed), jnp.logical_not(far)
    early = jnp.logical_and(lon == 0, direct)
    late = jnp.logical_not(early)
    late_top, late_below = jnp.logical_and(late, at_top), jnp.logical_and(late, below_top)
    e_dev = (lax.rem(lon + 1, n_lon), lat)
    w_dev = (lax.rem(lon + n_lon - 1, n_lon), lat)
    n_dev, s_dev = (lon, lat + 1), (lon, lat - 1)
    lat_up, lat_down = lax.rem(lat + 1, n_lat), lax.rem(lat + n_lat - 1, n_lat)
    fold_dev = (n_lon - 1 - lon, lat)
    tiles = tracers * levels
    plane = levels * rows
    lead = levels
    ends = [sum(groups[:i]) for i in range(len(groups) + 1)]
    split = ends[-2]
    slots, pers, shares = layout(tracers, split, levels, lanes)
    kmt_at = pers[0] * slots[0]

    load_kmt = pltpu.make_async_copy(kmt_ref, kmt_int, load_sem.at[len(groups)])
    load_kmt.start()

    def load(first, count, i):
        return pltpu.make_async_copy(
            x_ref.at[pl.ds(first, count)], xv.at[pl.ds(lead + first, count)], load_sem.at[i]
        )

    for i in range(len(groups)):
        for t in range(ends[i], ends[i + 1]):
            load(t * levels, levels, i).start()
    loads = [load(ends[i] * levels, groups[i] * levels, i) for i in range(len(groups))]
    flat = xv.reshape((lead + tiles) * rows, lanes)

    barrier = pltpu.get_barrier_semaphore()

    def greet(dev):
        pl.semaphore_signal(barrier, inc=1, device_id=dev, device_id_type=MESH)

    with jax.named_scope("greet"):
        greet(w_dev)

        @pl.when(near)
        def _():
            greet(e_dev)

        @pl.when(far)
        def _():
            greet((0, lat_up))

        @pl.when(at_top)
        def _():
            greet(fold_dev)

        @pl.when(below_top)
        def _():
            greet(n_dev)

        @pl.when(inner)
        def _():
            greet(s_dev)

    lane = lax.broadcasted_iota(jnp.int32, (rows, lanes), 1)
    row = lax.broadcasted_iota(jnp.int32, (rows, lanes), 0)

    def send(src, dst, s, r, dev):
        return pltpu.make_async_remote_copy(
            src_ref=src, dst_ref=dst, send_sem=send_sem.at[s], recv_sem=recv_sem.at[r],
            device_id=dev, device_id_type=MESH,
        )

    def rows_of(r, span, dst, s, into, dev):
        return send(xv.at[span, r, :], dst.at[span], s, into, dev)

    cut = lead + ends[-2] * levels
    starts = [lead - 1] + [lead + e * levels for e in ends[1:]]
    spans = [pl.ds(a, b - a) for a, b in zip(starts, starts[1:])]
    every = pl.ds(lead - 1, tiles + 1)
    halves = [(pl.ds(lead - 1, cut - lead + 1), 0), (spans[-1], 5)]
    fold = rows_of(rows - 1, every, from_n, 0, 0, fold_dev)
    folds = [
        rows_of(rows - 1, span, from_n, 0, 5 if i == len(spans) - 1 else 0, fold_dev)
        for i, span in enumerate(spans)
    ]
    to_n = rows_of(rows - 1, every, from_s, 0, 1, n_dev)
    to_s = rows_of(0, every, from_n, 1, 0, s_dev)
    to_ss = [rows_of(0, span, from_n, 1, r, s_dev) for span, r in halves]
    cols = (pl.ds(0, shares[0] * rows), pl.ds(shares[0] * rows, shares[1] * rows))
    halos = (halo1, halo2)
    wests = [h.at[pl.ds(0, n * rows)] for h, n in zip(halos, shares)]
    easts = [h.at[pl.ds(n * rows, n * rows)] for h, n in zip(halos, shares)]
    far_dev = (n_lon - 1, lat_down)
    to_e = [send(ecol.at[c], wests[i], 2, 2 + i, e_dev) for i, c in enumerate(cols)]
    to_w = [send(wcol.at[c], easts[i], 3, 2 + i, w_dev) for i, c in enumerate(cols)]
    onward = [send(relay.at[c], easts[i], 4, 2 + i, far_dev) for i, c in enumerate(cols)]
    to_relay = send(wcol, relay, 3, 4, (lon, lat_up))
    got = [send(h, h, 2, 2 + i, e_dev) for i, h in enumerate(halos)]
    all_e, all_w, all_onward = (send(c, relay, s, 4, e_dev) for c, s in ((ecol, 2), (wcol, 3), (relay, 4)))

    def tile(t, k):
        return flat[pl.ds(lead * rows + t * plane + k * rows, rows), :]

    def density(k):
        return HALINE * tile(1, k) - THERMAL * tile(0, k)

    def where_is(t, k):
        n, u = (0, t) if t < split else (1, t - split)
        return k % pers[n] * slots[n] + u, n * shares[0] + k // pers[n]

    def gather_columns(e_ref, w_ref, e_off, w_off, before=None, after=None):
        zeros = jnp.zeros((rows, lanes), jnp.float32)
        es, ws = [zeros] * sum(shares), [zeros] * sum(shares)

        def place(value, at, reg):
            value = pltpu.roll(value, at + 1, 1)
            es[reg] = jnp.where(lane == (at + e_off) % lanes, value, es[reg])
            ws[reg] = jnp.where(lane == (at + w_off) % lanes, value, ws[reg])

        for i in range(len(groups)):
            if before is not None:
                before(i)
            if i == 0:
                place(kmt_own, kmt_at, 0)
                for k in range(levels):
                    at, reg = where_is(0, k)
                    place(density(k), at + split, reg)
            for t in range(ends[i], ends[i + 1]):
                for k in range(levels):
                    place(tile(t, k), *where_is(t, k))
            if ends[i + 1] in (split, tracers):
                n = 0 if ends[i + 1] == split else 1
                for j in range(n * shares[0], n * shares[0] + shares[n]):
                    e_ref[pl.ds(j * rows, rows), :] = es[j]
                    w_ref[pl.ds(j * rows, rows), :] = ws[j]
                if after is not None:
                    after(n)

    def enter():
        @pl.when(at_bottom)
        def _():
            pl.semaphore_wait(barrier, 3)

        @pl.when(jnp.logical_and(inner, jnp.logical_not(jnp.logical_or(relayed, relays))))
        def _():
            pl.semaphore_wait(barrier, 4)

        @pl.when(relayed)
        def _():
            pl.semaphore_wait(barrier, 3)

        @pl.when(relays)
        def _():
            pl.semaphore_wait(barrier, 5)

    def send_inner_rows():
        @pl.when(below_top)
        def _():
            to_n.start()

        @pl.when(inner)
        def _():
            for copy in to_ss:
                copy.start()

    def before(i):
        with jax.named_scope(f"load{i}"):
            loads[i].wait()
        if i == 0:

            @pl.when(late_top)
            def _():
                enter()

        if i < len(groups) - 1:

            @pl.when(late_top)
            def _():
                folds[i].start()

    def after(n):
        if n == 0:

            @pl.when(late_below)
            def _():
                with jax.named_scope("barrier"):
                    enter()

        @pl.when(late)
        def _():
            to_e[n].start()

        @pl.when(jnp.logical_and(late, direct))
        def _():
            to_w[n].start()

    with jax.named_scope("loadk"):
        load_kmt.wait()
    kmt_own = kmt_int[...].astype(jnp.float32)
    xv[lead - 1, :, :] = kmt_own
    gather_columns(ecol, wcol, 0, 1, before, after)
    with jax.named_scope("send"):

        @pl.when(relayed)
        def _():
            to_relay.start()

        @pl.when(late_top)
        def _():
            folds[-1].start()

        @pl.when(late)
        def _():
            send_inner_rows()

    with jax.named_scope("inner"):
        gather_columns(inner_e, inner_w, -1, 2)

        @pl.when(at_bottom)
        def _():
            for t in range(tracers + 1):
                from_s[pl.ds(t * levels, levels), :] = jnp.zeros((levels, lanes), jnp.float32)

    def put(d, dk, k, value):
        coef[pl.ds(((d * 3 + dk) * levels + k) * rows, rows), :] = value

    def piece_of(d, dk, k):
        return coef[pl.ds(((d * 3 + dk) * levels + k) * rows, rows), :]

    with jax.named_scope("coefs"):
        def shifted(v, by, axis):
            return jnp.stack([pltpu.roll(v[k], by, axis) for k in range(levels)])

        own_rho = jnp.stack([density(k) for k in range(levels)])
        own_wet = jnp.stack([(kmt_own > float(k)).astype(jnp.float32) for k in range(levels)])
        c3 = column(own_rho, own_wet, up3, dn3)

        def moved(by, axis):
            return tuple(shifted(v, by, axis) for v in c3)

        mid_lane = jnp.logical_and(lane > 0, lane < lanes - 1)
        xc, xe, xw = line(c3, moved(lanes - 1, 1), moved(1, 1), up3, dn3)
        for dk in range(3):
            for k in range(levels):
                put(E, dk, k, jnp.where(mid_lane, xe[dk][k], 0.0))
                put(W, dk, k, jnp.where(mid_lane, xw[dk][k], 0.0))
                put(C, dk, k, jnp.where(mid_lane, xc[dk][k], 0.0))
        mid_row = jnp.logical_and(row > 0, row < rows - 1)
        yc, yn, ys = line(c3, moved(rows - 1, 0), moved(1, 0), up3, dn3)
        for dk in range(3):
            for k in range(levels):
                put(N, dk, k, jnp.where(mid_row, yn[dk][k], 0.0))
                put(S, dk, k, jnp.where(mid_row, ys[dk][k], 0.0))
                core = piece_of(C, dk, k) + jnp.where(mid_row, yc[dk][k], 0.0)
                put(C, dk, k, core + 1.0 if dk == 1 else core)

    with jax.named_scope("main"):

        @pl.loop(0, tracers // TOGETHER)
        def _(i):
            fields = []
            for u in range(TOGETHER):
                base = pl.multiple_of(lead * rows + (i * TOGETHER + u) * plane, rows)
                field = []
                for k in range(levels):
                    own = flat[pl.ds(base + k * rows, rows), :]
                    field.append((
                        own, pltpu.roll(own, lanes - 1, 1), pltpu.roll(own, 1, 1),
                        pltpu.roll(own, rows - 1, 0), pltpu.roll(own, 1, 0),
                    ))
                fields.append(field)
            for k in range(levels):
                sums = [None] * TOGETHER
                for d in range(5):
                    for dk in range(3):
                        if not 0 <= k + dk - 1 < levels:
                            continue
                        c = piece_of(d, dk, k)
                        for u in range(TOGETHER):
                            term = c * fields[u][k + dk - 1][d]
                            sums[u] = term if sums[u] is None else sums[u] + term
                for u in range(TOGETHER):
                    base = pl.multiple_of((i * TOGETHER + u) * plane, rows)
                    out_ref[pl.ds(base + k * rows, rows), :] = sums[u]

    @pl.when(early)
    def _():
        with jax.named_scope("barrier"):
            enter()
        for copy in to_e + to_w:
            copy.start()
        send_inner_rows()

        @pl.when(at_top)
        def _():
            for copy in folds:
                copy.start()

    @pl.when(relays)
    def _():
        to_relay.wait_recv()
        for copy in onward:
            copy.start()

    level = lax.broadcasted_iota(jnp.int32, (levels, lanes), 0)
    level_f = level.astype(jnp.float32)

    def up_s(v):
        return jnp.where(level == 0, 0.0, pltpu.roll(v, 1, 0))

    def dn_s(v):
        return jnp.where(level == levels - 1, 0.0, pltpu.roll(v, levels - 1, 0))

    def at_row(t, r):
        return flat[pl.ds(lead * rows + t * plane + r, levels, stride=rows), :]

    def row_column(t0, t1, kmt):
        wet = (jnp.broadcast_to(kmt, (levels, lanes)) > level_f).astype(jnp.float32)
        return column(HALINE * t1 - THERMAL * t0, wet, up_s, dn_s)

    def own_row(r):
        return row_column(at_row(0, r), at_row(1, r), kmt_own[r : r + 1, :])

    def fix_rows(source, r, r_in, north, turn, parts):
        def halo(t):
            h = source[pl.ds(lead + t * levels, levels), :]
            return pick(h, lanes - 1 - lane) if turn else h

        first, last, wait = parts[0]
        wait()
        k = jnp.broadcast_to(source[pl.ds(lead - 1, 1), :], (rows, lanes))
        k = (pick(k, lanes - 1 - lane) if turn else k)[:1, :]
        out_c, in_c = row_column(halo(0), halo(1), k), own_row(r_in)
        p, m = (out_c, in_c) if north else (in_c, out_c)
        cc, cp, cm = line(own_row(r), p, m, up_s, dn_s)
        c_out, c_in = (cp, cm) if north else (cm, cp)
        table = (cc, c_out, c_in)
        lo = [pltpu.roll(c[0], levels - 1, 0) for c in table]
        mid = [c[1] for c in table]
        hi = [pltpu.roll(c[2], 1, 0) for c in table]
        for n, (first, last, wait) in enumerate(parts):
            if n:
                wait()
            count = last - first
            batch = next(b for b in (16, 12, 8, 4, 2, 1) if count % b == 0 and (turn or b <= 8))

            @pl.loop(0, count // batch)
            def _(i, first=first, batch=batch):
                for u in range(batch):
                    t = first + i * batch + u
                    values = (at_row(t, r), halo(t), at_row(t, r_in))
                    above = total([c * v for c, v in zip(lo, values)])
                    same = total([c * v for c, v in zip(mid, values)])
                    below = total([c * v for c, v in zip(hi, values)])
                    place = pl.ds(t * plane + r, levels, stride=rows)
                    out_ref[place, :] = (
                        out_ref[place, :] + same + pltpu.roll(above, 1, 0) + pltpu.roll(below, levels - 1, 0)
                    )

    def fix_n(turn):
        parts = [(0, ends[-2], to_ss[0].wait_recv), (ends[-2], tracers, to_ss[1].wait_recv)]
        fix_rows(from_n, rows - 1, rows - 2, True, turn, parts)

    with jax.named_scope("fixs"):

        @pl.when(inner)
        def _():
            to_n.wait_recv()

        fix_rows(from_s, 0, 1, False, False, [(0, tracers, lambda: None)])

    with jax.named_scope("fixn"):

        @pl.when(below_top)
        def _():
            fix_n(False)

    spot = tracer_of(lane, lanes, tracers)
    low = spot < split
    spots = (jnp.minimum(spot, split - 1), jnp.maximum(spot - split, 0))

    def part_of(refs, offs, n):
        return values_of(refs, offs, spots[n], pers[n], slots[n], n * shares[0], levels)

    def column_of(refs, offs):
        fixed = jnp.zeros((rows, lanes), jnp.int32)
        rho = jnp.stack([both(refs, offs, fixed + (where_is(0, k)[0] + split), where_is(0, k)[1])
                         for k in range(levels)])
        kmt = both(refs, offs, fixed + kmt_at, 0)
        wet = jnp.stack([(kmt > float(k)).astype(jnp.float32) for k in range(levels)])
        return column(rho, wet, up3, dn3)

    def joined(first, second):
        return jnp.stack([jnp.where(low, first[k], second[k]) for k in range(levels)])

    with jax.named_scope("fixc0"):
        own_at, ins_at, outs_at = ((wcol, ecol), (1, 0)), ((inner_w, inner_e), (2, -1)), ((wests[0], easts[0]), (0, 1))
        own_c, ins_c = column_of(*own_at), column_of(*ins_at)
        own, ins = (joined(part_of(*at, 0), part_of(*at, 1)) for at in (own_at, ins_at))
    with jax.named_scope("waitc"):
        got[0].wait_recv()
    with jax.named_scope("fixc1"):
        own_t, outs_t, ins_t = line(own_c, column_of(*outs_at), ins_c, up3, dn3)
        some = applied(own_t, own) + applied(ins_t, ins)
        more = applied(outs_t, part_of(*outs_at, 0))
        for k in range(levels):
            add_ref[pl.ds(k * rows, rows), :] = some[k] + jnp.where(low, more[k], 0.0)
            for dk in range(3):
                tab_ref[pl.ds((dk * levels + k) * rows, rows), :] = outs_t[dk][k]

    with jax.named_scope("fixtop"):

        @pl.when(at_top)
        def _():
            fix_n(True)

    with jax.named_scope("waitc2"):
        got[1].wait_recv()

    with jax.named_scope("end"):
        fold.wait_send()

        @pl.when(inner)
        def _():
            to_s.wait_send()

        all_e.wait_send()
        all_w.wait_send()

        @pl.when(relays)
        def _():
            all_onward.wait_send()


def finish(sizes, part_ref, add_ref, tab_ref, halo_ref, out_ref, stage, sem):
    tracers, levels, rows, lanes, split = sizes
    plane = levels * rows
    slots, pers, shares = layout(tracers, split, levels, lanes)
    lane = lax.broadcasted_iota(jnp.int32, (rows, lanes), 1)
    sides = jnp.logical_or(lane == 0, lane == lanes - 1)
    spot = tracer_of(lane, lanes, tracers)
    add = jnp.stack([add_ref[pl.ds(k * rows, rows), :] for k in range(levels)])

    def rest():
        refs = [halo_ref.at[pl.ds(i * shares[1] * rows, shares[1] * rows)] for i in range(2)]
        values = values_of(refs, (0, 1), jnp.maximum(spot - split, 0), pers[1], slots[1], 0, levels)
        table = [
            jnp.stack([tab_ref[pl.ds((dk * levels + k) * rows, rows), :] for k in range(levels)]) for dk in range(3)
        ]
        return add + applied(table, values)

    with jax.named_scope("insert"):
        terms, full = add, None
        for t in range(tracers):
            if t == EARLY:
                full = rest()
            if t == split:
                terms = full
            for k in range(levels):
                term = pltpu.roll(terms[k], (lanes - 2 * t) % lanes, 1)
                place = pl.ds(t * plane + k * rows, rows)
                stage[place, :] = part_ref[place, :] + jnp.where(sides, term, 0.0)
            if t % STORE == 0 or t == tracers - 1:
                first = 0 if t == 0 else (t - 1) // STORE * STORE + 1
                span = pl.ds(first * plane, (t + 1 - first) * plane)
                pltpu.make_async_copy(stage.at[span], out_ref.at[span], sem).start()
    with jax.named_scope("written"):
        pltpu.make_async_copy(stage, out_ref, sem).wait()


def solution(mesh):
    n_lon, n_lat = mesh.shape["lon"], mesh.shape["lat"]

    def local(tracers, kmt):
        nt, levels, rows, lanes = tracers.shape
        tiles = nt * levels
        cuts = (0, nt // 10, 3 * nt // 10, 6 * nt // 10, nt)
        groups = tuple(b - a for a, b in zip(cuts, cuts[1:]))
        shares = layout(nt, cuts[-2], levels, lanes)[-1]
        regs = sum(shares)
        assert levels == rows and groups[0] > 1 and cuts[-2] > EARLY

        def vmem(*shape):
            return pltpu.VMEM(shape, jnp.float32)

        parts = pl.pallas_call(
            functools.partial(kernel, (nt, levels, rows, lanes, n_lon, n_lat, groups)),
            out_shape=[
                vmem(tiles * rows, lanes),
                vmem(levels * rows, lanes),
                vmem(3 * levels * rows, lanes),
                vmem(2 * shares[1] * rows, lanes),
            ],
            in_specs=[pl.BlockSpec(memory_space=pltpu.HBM), pl.BlockSpec(memory_space=pltpu.HBM)],
            out_specs=[pl.BlockSpec(memory_space=pltpu.VMEM)] * 4,
            scratch_shapes=[
                vmem(tiles + levels, rows, lanes),
                pltpu.VMEM((rows, lanes), jnp.int32),
                vmem(15 * levels * rows, lanes),
            ]
            + [vmem(regs * rows, lanes)] * 5
            + [vmem(2 * shares[0] * rows, lanes)]
            + [vmem(tiles + rows, lanes)] * 2
            + [
                pltpu.SemaphoreType.DMA((6,)),
            ],
            compiler_params=pltpu.CompilerParams(collective_id=0, has_side_effects=True),
        )(tracers.reshape(tiles, rows, lanes), kmt)
        parts = [pltpu.with_memory_space_constraint(v, pltpu.VMEM) for v in parts]
        out = pl.pallas_call(
            functools.partial(finish, (nt, levels, rows, lanes, cuts[-2])),
            out_shape=jax.ShapeDtypeStruct((tiles * rows, lanes), jnp.float32),
            in_specs=[pl.BlockSpec(memory_space=pltpu.VMEM)] * 4,
            out_specs=pl.BlockSpec(memory_space=pltpu.HBM),
            scratch_shapes=[vmem(tiles * rows, lanes), pltpu.SemaphoreType.DMA],
        )(*parts)
        return out.reshape(nt, levels, rows, lanes)

    return jax.shard_map(
        local,
        mesh=mesh,
        in_specs=(P(None, None, "lat", "lon"), P("lat", "lon")),
        out_specs=P(None, None, "lat", "lon"),
        check_vma=False,
    )
```

```python
import functools

import jax
import jax.numpy as jnp
from jax import lax
from jax.experimental import pallas as pl
from jax.experimental.pallas import tpu as pltpu
from jax.sharding import PartitionSpec as P

THERMAL = 0.2
HALINE = 0.8
REDI = 0.1
SKEW = 0.05
SLOPE_MAX = 0.6
SLOPE_WIDTH = 0.2

MESH = pl.DeviceIdType.MESH
TOGETHER = 2
STORE = 2
EARLY = 2
C, E, W, N, S = range(5)


def taper(slope):
    return slope * 0.5 * (1.0 + jnp.tanh((SLOPE_MAX - jnp.abs(slope)) / SLOPE_WIDTH))


def column(rho, wet, up, dn):
    hi = wet * dn(wet)
    strat = (dn(rho) - rho) * hi
    return rho, wet, hi, up(hi), 0.5 * (strat + up(strat))


def line(c, p, m, up, dn):
    c_rho, c_wet, c_hi, c_lo, c_cell = c
    p_rho, p_wet, p_hi, p_lo, p_cell = p
    m_rho, m_wet, m_hi, m_lo, m_cell = m
    mp, mm = c_wet * p_wet, c_wet * m_wet
    sp = taper((p_rho - c_rho) * mp / jnp.maximum(0.5 * (p_cell + c_cell), 1.0))
    sm = taper((c_rho - m_rho) * mm / jnp.maximum(0.5 * (m_cell + c_cell), 1.0))
    cx = 0.5 * (sp + sm)
    sw = 0.5 * (cx + dn(cx))
    fh = ((REDI + SKEW) * 0.25) * sw * c_hi
    zh = REDI * (sw * sw) * c_hi
    fl, zl = up(fh), up(zh)
    pp = ((REDI - SKEW) * 0.25) * sp * mp
    pm = -((REDI - SKEW) * 0.25) * sm * mm
    own_p, own_m = mp * (fh - fl), mm * (fl - fh)
    mph, mmh = dn(mp) * fh, dn(mm) * fh
    mpl, mml = up(mp) * fl, up(mm) * fl
    q = pp + pm
    return (
        (mpl - mml - q * c_lo + zl,
         q * (c_lo - c_hi) - REDI * (mp + mm) - (own_p + own_m) - (zh + zl),
         mmh - mph + q * c_hi + zh),
        (-pp * p_lo - mpl, REDI * mp + pp * (p_lo - p_hi) + own_p, pp * p_hi + mph),
        (mml - pm * m_lo, REDI * mm + pm * (m_lo - m_hi) + own_m, pm * m_hi - mmh),
    )


def total(terms):
    result = terms[0]
    for term in terms[1:]:
        result = result + term
    return result


def pick(value, index):
    return jnp.take_along_axis(value, index, axis=1)


def up3(v):
    return jnp.concatenate([jnp.zeros_like(v[:1]), v[:-1]], axis=0)


def dn3(v):
    return jnp.concatenate([v[1:], jnp.zeros_like(v[:1])], axis=0)


def applied(c, v):
    return c[1] * v + c[0] * up3(v) + c[2] * dn3(v)


def layout(tracers, split, levels, lanes):
    slots = (split + 2, tracers - split)
    pers = tuple((lanes - 2) // slot for slot in slots)
    return slots, pers, tuple((levels + per - 1) // per for per in pers)


def tracer_of(lane, lanes, tracers):
    return jnp.minimum((lane + 1) // 2 % (lanes // 2), tracers - 1)


def both(refs, offs, at, reg):
    rows, lanes = at.shape
    span = pl.ds(reg * rows, rows)
    west_side = lax.broadcasted_iota(jnp.int32, at.shape, 1) % 2 == 0
    picked = [pick(ref[span, :], (at + off + lanes) % lanes) for ref, off in zip(refs, offs)]
    return jnp.where(west_side, *picked)


def values_of(refs, offs, spot, per, slot, first, levels):
    return jnp.stack([both(refs, offs, k % per * slot + spot, first + k // per) for k in range(levels)])


def kernel(sizes, x_ref, kmt_ref, out_ref, add_ref, tab_ref, halo2, *scratch):
    pl.run_scoped(
        functools.partial(body, sizes, x_ref, kmt_ref, out_ref, add_ref, tab_ref, halo2, *scratch),
        pltpu.SemaphoreType.DMA((len(sizes[-1]) + 1,)),
        pltpu.SemaphoreType.DMA((5,)),
    )


def body(
    sizes, x_ref, kmt_ref, out_ref, add_ref, tab_ref, halo2,
    xv, kmt_int, coef, wcol, ecol, inner_w, inner_e, relay, halo1, from_n, from_s,
    recv_sem, load_sem, send_sem,
):
    tracers, levels, rows, lanes, n_lon, n_lat, groups = sizes
    lon, lat = lax.axis_index("lon"), lax.axis_index("lat")
    at_top = lat == n_lat - 1
    below_top = jnp.logical_not(at_top)
    inner = lat > 0
    at_bottom = jnp.logical_not(inner)
    even_lat = jnp.logical_and(inner, jnp.logical_and(lat % 2 == 0, below_top))
    odd_lat = jnp.logical_and(lat > 1, lat % 2 == 1)
    relayed = jnp.logical_and(lon == 0, even_lat)
    relays = jnp.logical_and(lon == 0, odd_lat)
    far = jnp.logical_and(lon == n_lon - 1, even_lat)
    direct, near = jnp.logical_not(relayed), jnp.logical_not(far)
    early = jnp.logical_and(lon == 0, direct)
    late = jnp.logical_not(early)
    late_top, late_below = jnp.logical_and(late, at_top), jnp.logical_and(late, below_top)
    e_dev = (lax.rem(lon + 1, n_lon), lat)
    w_dev = (lax.rem(lon + n_lon - 1, n_lon), lat)
    n_dev, s_dev = (lon, lat + 1), (lon, lat - 1)
    lat_up, lat_down = lax.rem(lat + 1, n_lat), lax.rem(lat + n_lat - 1, n_lat)
    fold_dev = (n_lon - 1 - lon, lat)
    tiles = tracers * levels
    plane = levels * rows
    lead = levels
    ends = [sum(groups[:i]) for i in range(len(groups) + 1)]
    split = ends[-2]
    slots, pers, shares = layout(tracers, split, levels, lanes)
    kmt_at = pers[0] * slots[0]

    load_kmt = pltpu.make_async_copy(kmt_ref, kmt_int, load_sem.at[len(groups)])
    load_kmt.start()

    def load(first, count, i):
        return pltpu.make_async_copy(
            x_ref.at[pl.ds(first, count)], xv.at[pl.ds(lead + first, count)], load_sem.at[i]
        )

    for i in range(len(groups)):
        for t in range(ends[i], ends[i + 1]):
            load(t * levels, levels, i).start()
    loads = [load(ends[i] * levels, groups[i] * levels, i) for i in range(len(groups))]
    flat = xv.reshape((lead + tiles) * rows, lanes)

    barrier = pltpu.get_barrier_semaphore()

    def greet(dev):
        pl.semaphore_signal(barrier, inc=1, device_id=dev, device_id_type=MESH)

    with jax.named_scope("greet"):
        greet(w_dev)

        @pl.when(near)
        def _():
            greet(e_dev)

        @pl.when(far)
        def _():
            greet((0, lat_up))

        @pl.when(at_top)
        def _():
            greet(fold_dev)

        @pl.when(below_top)
        def _():
            greet(n_dev)

        @pl.when(inner)
        def _():
            greet(s_dev)

    lane = lax.broadcasted_iota(jnp.int32, (rows, lanes), 1)
    row = lax.broadcasted_iota(jnp.int32, (rows, lanes), 0)

    def send(src, dst, s, r, dev):
        return pltpu.make_async_remote_copy(
            src_ref=src, dst_ref=dst, send_sem=send_sem.at[s], recv_sem=recv_sem.at[r],
            device_id=dev, device_id_type=MESH,
        )

    def rows_of(r, span, dst, s, into, dev):
        return send(xv.at[span, r, :], dst.at[span], s, into, dev)

    cut = lead + ends[-2] * levels
    starts = [lead - 1] + [lead + e * levels for e in ends[1:]]
    spans = [pl.ds(a, b - a) for a, b in zip(starts, starts[1:])]
    every = pl.ds(lead - 1, tiles + 1)
    halves = [(pl.ds(lead - 1, cut - lead + 1), 0), (spans[-1], 5)]
    fold = rows_of(rows - 1, every, from_n, 0, 0, fold_dev)
    folds = [
        rows_of(rows - 1, span, from_n, 0, 5 if i == len(spans) - 1 else 0, fold_dev)
        for i, span in enumerate(spans)
    ]
    to_n = rows_of(rows - 1, every, from_s, 0, 1, n_dev)
    to_s = rows_of(0, every, from_n, 1, 0, s_dev)
    to_ss = [rows_of(0, span, from_n, 1, r, s_dev) for span, r in halves]
    cols = (pl.ds(0, shares[0] * rows), pl.ds(shares[0] * rows, shares[1] * rows))
    halos = (halo1, halo2)
    wests = [h.at[pl.ds(0, n * rows)] for h, n in zip(halos, shares)]
    easts = [h.at[pl.ds(n * rows, n * rows)] for h, n in zip(halos, shares)]
    far_dev = (n_lon - 1, lat_down)
    to_e = [send(ecol.at[c], wests[i], 2, 2 + i, e_dev) for i, c in enumerate(cols)]
    to_w = [send(wcol.at[c], easts[i], 3, 2 + i, w_dev) for i, c in enumerate(cols)]
    onward = [send(relay.at[c], easts[i], 4, 2 + i, far_dev) for i, c in enumerate(cols)]
    to_relay = send(wcol, relay, 3, 4, (lon, lat_up))
    got = [send(h, h, 2, 2 + i, e_dev) for i, h in enumerate(halos)]
    all_e, all_w, all_onward = (send(c, relay, s, 4, e_dev) for c, s in ((ecol, 2), (wcol, 3), (relay, 4)))

    def tile(t, k):
        return flat[pl.ds(lead * rows + t * plane + k * rows, rows), :]

    def density(k):
        return HALINE * tile(1, k) - THERMAL * tile(0, k)

    def where_is(t, k):
        n, u = (0, t) if t < split else (1, t - split)
        return k % pers[n] * slots[n] + u, n * shares[0] + k // pers[n]

    def gather_columns(e_ref, w_ref, e_off, w_off, before=None, after=None):
        zeros = jnp.zeros((rows, lanes), jnp.float32)
        es, ws = [zeros] * sum(shares), [zeros] * sum(shares)

        def place(value, at, reg):
            value = pltpu.roll(value, at + 1, 1)
            es[reg] = jnp.where(lane == (at + e_off) % lanes, value, es[reg])
            ws[reg] = jnp.where(lane == (at + w_off) % lanes, value, ws[reg])

        for i in range(len(groups)):
            if before is not None:
                before(i)
            if i == 0:
                place(kmt_own, kmt_at, 0)
                for k in range(levels):
                    at, reg = where_is(0, k)
                    place(density(k), at + split, reg)
            for t in range(ends[i], ends[i + 1]):
                for k in range(levels):
                    place(tile(t, k), *where_is(t, k))
            if ends[i + 1] in (split, tracers):
                n = 0 if ends[i + 1] == split else 1
                for j in range(n * shares[0], n * shares[0] + shares[n]):
                    e_ref[pl.ds(j * rows, rows), :] = es[j]
                    w_ref[pl.ds(j * rows, rows), :] = ws[j]
                if after is not None:
                    after(n)

    def enter():
        @pl.when(at_bottom)
        def _():
            pl.semaphore_wait(barrier, 3)

        @pl.when(jnp.logical_and(inner, jnp.logical_not(jnp.logical_or(relayed, relays))))
        def _():
            pl.semaphore_wait(barrier, 4)

        @pl.when(relayed)
        def _():
            pl.semaphore_wait(barrier, 3)

        @pl.when(relays)
        def _():
            pl.semaphore_wait(barrier, 5)

    def send_inner_rows():
        @pl.when(below_top)
        def _():
            to_n.start()

        @pl.when(inner)
        def _():
            for copy in to_ss:
                copy.start()

    def before(i):
        with jax.named_scope(f"load{i}"):
            loads[i].wait()
        if i == 0:

            @pl.when(late_top)
            def _():
                enter()

        if i < len(groups) - 1:

            @pl.when(late_top)
            def _():
                folds[i].start()

    def after(n):
        if n == 0:

            @pl.when(late_below)
            def _():
                with jax.named_scope("barrier"):
                    enter()

        @pl.when(late)
        def _():
            to_e[n].start()

        @pl.when(jnp.logical_and(late, direct))
        def _():
            to_w[n].start()

    with jax.named_scope("loadk"):
        load_kmt.wait()
    kmt_own = kmt_int[...].astype(jnp.float32)
    xv[lead - 1, :, :] = kmt_own
    gather_columns(ecol, wcol, 0, 1, before, after)
    with jax.named_scope("send"):

        @pl.when(relayed)
        def _():
            to_relay.start()

        @pl.when(late_top)
        def _():
            folds[-1].start()

        @pl.when(late)
        def _():
            send_inner_rows()

    with jax.named_scope("inner"):
        gather_columns(inner_e, inner_w, -1, 2)

        @pl.when(at_bottom)
        def _():
            for t in range(tracers + 1):
                from_s[pl.ds(t * levels, levels), :] = jnp.zeros((levels, lanes), jnp.float32)

    def put(d, dk, k, value):
        coef[pl.ds(((d * 3 + dk) * levels + k) * rows, rows), :] = value

    def piece_of(d, dk, k):
        return coef[pl.ds(((d * 3 + dk) * levels + k) * rows, rows), :]

    with jax.named_scope("coefs"):
        def shifted(v, by, axis):
            return jnp.stack([pltpu.roll(v[k], by, axis) for k in range(levels)])

        own_rho = jnp.stack([density(k) for k in range(levels)])
        own_wet = jnp.stack([(kmt_own > float(k)).astype(jnp.float32) for k in range(levels)])
        c3 = column(own_rho, own_wet, up3, dn3)

        def moved(by, axis):
            return tuple(shifted(v, by, axis) for v in c3)

        mid_lane = jnp.logical_and(lane > 0, lane < lanes - 1)
        xc, xe, xw = line(c3, moved(lanes - 1, 1), moved(1, 1), up3, dn3)
        for dk in range(3):
            for k in range(levels):
                put(E, dk, k, jnp.where(mid_lane, xe[dk][k], 0.0))
                put(W, dk, k, jnp.where(mid_lane, xw[dk][k], 0.0))
                put(C, dk, k, jnp.where(mid_lane, xc[dk][k], 0.0))
        mid_row = jnp.logical_and(row > 0, row < rows - 1)
        yc, yn, ys = line(c3, moved(rows - 1, 0), moved(1, 0), up3, dn3)
        for dk in range(3):
            for k in range(levels):
                put(N, dk, k, jnp.where(mid_row, yn[dk][k], 0.0))
                put(S, dk, k, jnp.where(mid_row, ys[dk][k], 0.0))
                core = piece_of(C, dk, k) + jnp.where(mid_row, yc[dk][k], 0.0)
                put(C, dk, k, core + 1.0 if dk == 1 else core)

    with jax.named_scope("main"):

        @pl.loop(0, tracers // TOGETHER)
        def _(i):
            fields = []
            for u in range(TOGETHER):
                base = pl.multiple_of(lead * rows + (i * TOGETHER + u) * plane, rows)
                field = []
                for k in range(levels):
                    own = flat[pl.ds(base + k * rows, rows), :]
                    field.append((
                        own, pltpu.roll(own, lanes - 1, 1), pltpu.roll(own, 1, 1),
                        pltpu.roll(own, rows - 1, 0), pltpu.roll(own, 1, 0),
                    ))
                fields.append(field)
            for k in range(levels):
                sums = [None] * TOGETHER
                for d in range(5):
                    for dk in range(3):
                        if not 0 <= k + dk - 1 < levels:
                            continue
                        c = piece_of(d, dk, k)
                        for u in range(TOGETHER):
                            term = c * fields[u][k + dk - 1][d]
                            sums[u] = term if sums[u] is None else sums[u] + term
                for u in range(TOGETHER):
                    base = pl.multiple_of((i * TOGETHER + u) * plane, rows)
                    out_ref[pl.ds(base + k * rows, rows), :] = sums[u]

    @pl.when(early)
    def _():
        with jax.named_scope("barrier"):
            enter()
        for copy in to_e + to_w:
            copy.start()
        send_inner_rows()

        @pl.when(at_top)
        def _():
            for copy in folds:
                copy.start()

    @pl.when(relays)
    def _():
        to_relay.wait_recv()
        for copy in onward:
            copy.start()

    level = lax.broadcasted_iota(jnp.int32, (levels, lanes), 0)
    level_f = level.astype(jnp.float32)

    def up_s(v):
        return jnp.where(level == 0, 0.0, pltpu.roll(v, 1, 0))

    def dn_s(v):
        return jnp.where(level == levels - 1, 0.0, pltpu.roll(v, levels - 1, 0))

    def at_row(t, r):
        return flat[pl.ds(lead * rows + t * plane + r, levels, stride=rows), :]

    def row_column(t0, t1, kmt):
        wet = (jnp.broadcast_to(kmt, (levels, lanes)) > level_f).astype(jnp.float32)
        return column(HALINE * t1 - THERMAL * t0, wet, up_s, dn_s)

    def own_row(r):
        return row_column(at_row(0, r), at_row(1, r), kmt_own[r : r + 1, :])

    def fix_rows(source, r, r_in, north, turn, parts):
        def halo(t):
            h = source[pl.ds(lead + t * levels, levels), :]
            return pick(h, lanes - 1 - lane) if turn else h

        first, last, wait = parts[0]
        wait()
        k = jnp.broadcast_to(source[pl.ds(lead - 1, 1), :], (rows, lanes))
        k = (pick(k, lanes - 1 - lane) if turn else k)[:1, :]
        out_c, in_c = row_column(halo(0), halo(1), k), own_row(r_in)
        p, m = (out_c, in_c) if north else (in_c, out_c)
        cc, cp, cm = line(own_row(r), p, m, up_s, dn_s)
        c_out, c_in = (cp, cm) if north else (cm, cp)
        table = (cc, c_out, c_in)
        lo = [pltpu.roll(c[0], levels - 1, 0) for c in table]
        mid = [c[1] for c in table]
        hi = [pltpu.roll(c[2], 1, 0) for c in table]
        for n, (first, last, wait) in enumerate(parts):
            if n:
                wait()
            count = last - first
            batch = count if turn else next(b for b in (8, 5, 4, 3, 2, 1) if count % b == 0)

            @pl.loop(0, count // batch)
            def _(i, first=first, batch=batch):
                for u in range(batch):
                    t = first + i * batch + u
                    values = (at_row(t, r), halo(t), at_row(t, r_in))
                    above = total([c * v for c, v in zip(lo, values)])
                    same = total([c * v for c, v in zip(mid, values)])
                    below = total([c * v for c, v in zip(hi, values)])
                    place = pl.ds(t * plane + r, levels, stride=rows)
                    out_ref[place, :] = (
                        out_ref[place, :] + same + pltpu.roll(above, 1, 0) + pltpu.roll(below, levels - 1, 0)
                    )

    def fix_n(turn):
        parts = [(0, ends[-2], to_ss[0].wait_recv), (ends[-2], tracers, to_ss[1].wait_recv)]
        fix_rows(from_n, rows - 1, rows - 2, True, turn, parts)

    with jax.named_scope("fixs"):

        @pl.when(inner)
        def _():
            to_n.wait_recv()

        fix_rows(from_s, 0, 1, False, False, [(0, tracers, lambda: None)])

    with jax.named_scope("fixn"):

        @pl.when(below_top)
        def _():
            fix_n(False)

    spot = tracer_of(lane, lanes, tracers)
    low = spot < split
    spots = (jnp.minimum(spot, split - 1), jnp.maximum(spot - split, 0))

    def part_of(refs, offs, n):
        return values_of(refs, offs, spots[n], pers[n], slots[n], n * shares[0], levels)

    def column_of(refs, offs):
        fixed = jnp.zeros((rows, lanes), jnp.int32)
        rho = jnp.stack([both(refs, offs, fixed + (where_is(0, k)[0] + split), where_is(0, k)[1])
                         for k in range(levels)])
        kmt = both(refs, offs, fixed + kmt_at, 0)
        wet = jnp.stack([(kmt > float(k)).astype(jnp.float32) for k in range(levels)])
        return column(rho, wet, up3, dn3)

    def joined(first, second):
        return jnp.stack([jnp.where(low, first[k], second[k]) for k in range(levels)])

    with jax.named_scope("fixc0"):
        own_at, ins_at, outs_at = ((wcol, ecol), (1, 0)), ((inner_w, inner_e), (2, -1)), ((wests[0], easts[0]), (0, 1))
        own_c, ins_c = column_of(*own_at), column_of(*ins_at)
        own, ins = (joined(part_of(*at, 0), part_of(*at, 1)) for at in (own_at, ins_at))
    with jax.named_scope("waitc"):
        got[0].wait_recv()
    with jax.named_scope("fixc1"):
        own_t, outs_t, ins_t = line(own_c, column_of(*outs_at), ins_c, up3, dn3)
        some = applied(own_t, own) + applied(ins_t, ins)
        more = applied(outs_t, part_of(*outs_at, 0))
        for k in range(levels):
            add_ref[pl.ds(k * rows, rows), :] = some[k] + jnp.where(low, more[k], 0.0)
            for dk in range(3):
                tab_ref[pl.ds((dk * levels + k) * rows, rows), :] = outs_t[dk][k]

    with jax.named_scope("fixtop"):

        @pl.when(at_top)
        def _():
            fix_n(True)

    with jax.named_scope("waitc2"):
        got[1].wait_recv()

    with jax.named_scope("end"):
        fold.wait_send()

        @pl.when(inner)
        def _():
            to_s.wait_send()

        all_e.wait_send()
        all_w.wait_send()

        @pl.when(relays)
        def _():
            all_onward.wait_send()


def finish(sizes, part_ref, add_ref, tab_ref, halo_ref, out_ref, stage, sem):
    tracers, levels, rows, lanes, split = sizes
    plane = levels * rows
    slots, pers, shares = layout(tracers, split, levels, lanes)
    lane = lax.broadcasted_iota(jnp.int32, (rows, lanes), 1)
    sides = jnp.logical_or(lane == 0, lane == lanes - 1)
    spot = tracer_of(lane, lanes, tracers)
    add = jnp.stack([add_ref[pl.ds(k * rows, rows), :] for k in range(levels)])

    def rest():
        refs = [halo_ref.at[pl.ds(i * shares[1] * rows, shares[1] * rows)] for i in range(2)]
        values = values_of(refs, (0, 1), jnp.maximum(spot - split, 0), pers[1], slots[1], 0, levels)
        table = [
            jnp.stack([tab_ref[pl.ds((dk * levels + k) * rows, rows), :] for k in range(levels)]) for dk in range(3)
        ]
        return add + applied(table, values)

    with jax.named_scope("insert"):
        terms, full = add, None
        for t in range(tracers):
            if t == EARLY:
                full = rest()
            if t == split:
                terms = full
            for k in range(levels):
                term = pltpu.roll(terms[k], (lanes - 2 * t) % lanes, 1)
                place = pl.ds(t * plane + k * rows, rows)
                stage[place, :] = part_ref[place, :] + jnp.where(sides, term, 0.0)
            if t % STORE == 0 or t == tracers - 1:
                first = 0 if t == 0 else (t - 1) // STORE * STORE + 1
                span = pl.ds(first * plane, (t + 1 - first) * plane)
                pltpu.make_async_copy(stage.at[span], out_ref.at[span], sem).start()
    with jax.named_scope("written"):
        pltpu.make_async_copy(stage, out_ref, sem).wait()


def solution(mesh):
    n_lon, n_lat = mesh.shape["lon"], mesh.shape["lat"]

    def local(tracers, kmt):
        nt, levels, rows, lanes = tracers.shape
        tiles = nt * levels
        split = max(nt - (lanes - 2) // levels, nt // 2)
        cuts = (0, split // 6, split // 2, split, nt)
        groups = tuple(b - a for a, b in zip(cuts, cuts[1:]))
        shares = layout(nt, split, levels, lanes)[-1]
        regs = sum(shares)
        assert levels == rows and groups[0] > 1 and split > EARLY

        def vmem(*shape):
            return pltpu.VMEM(shape, jnp.float32)

        parts = pl.pallas_call(
            functools.partial(kernel, (nt, levels, rows, lanes, n_lon, n_lat, groups)),
            out_shape=[
                vmem(tiles * rows, lanes),
                vmem(levels * rows, lanes),
                vmem(3 * levels * rows, lanes),
                vmem(2 * shares[1] * rows, lanes),
            ],
            in_specs=[pl.BlockSpec(memory_space=pltpu.HBM), pl.BlockSpec(memory_space=pltpu.HBM)],
            out_specs=[pl.BlockSpec(memory_space=pltpu.VMEM)] * 4,
            scratch_shapes=[
                vmem(tiles + levels, rows, lanes),
                pltpu.VMEM((rows, lanes), jnp.int32),
                vmem(15 * levels * rows, lanes),
            ]
            + [vmem(regs * rows, lanes)] * 5
            + [vmem(2 * shares[0] * rows, lanes)]
            + [vmem(tiles + rows, lanes)] * 2
            + [
                pltpu.SemaphoreType.DMA((6,)),
            ],
            compiler_params=pltpu.CompilerParams(collective_id=0, has_side_effects=True),
        )(tracers.reshape(tiles, rows, lanes), kmt)
        parts = [pltpu.with_memory_space_constraint(v, pltpu.VMEM) for v in parts]
        out = pl.pallas_call(
            functools.partial(finish, (nt, levels, rows, lanes, split)),
            out_shape=jax.ShapeDtypeStruct((tiles * rows, lanes), jnp.float32),
            in_specs=[pl.BlockSpec(memory_space=pltpu.VMEM)] * 4,
            out_specs=pl.BlockSpec(memory_space=pltpu.HBM),
            scratch_shapes=[vmem(tiles * rows, lanes), pltpu.SemaphoreType.DMA],
        )(*parts)
        return out.reshape(nt, levels, rows, lanes)

    return jax.shard_map(
        local,
        mesh=mesh,
        in_specs=(P(None, None, "lat", "lon"), P("lat", "lon")),
        out_specs=P(None, None, "lat", "lon"),
        check_vma=False,
    )
```

```python
import functools

import jax
import jax.numpy as jnp
from jax import lax
from jax.experimental import pallas as pl
from jax.experimental.pallas import tpu as pltpu
from jax.sharding import PartitionSpec as P

THERMAL = 0.2
HALINE = 0.8
REDI = 0.1
SKEW = 0.05
SLOPE_MAX = 0.6
SLOPE_WIDTH = 0.2

MESH = pl.DeviceIdType.MESH
TOGETHER = 2
STORE = 2
C, E, W, N, S = range(5)


def taper(slope):
    return slope * 0.5 * (1.0 + jnp.tanh((SLOPE_MAX - jnp.abs(slope)) / SLOPE_WIDTH))


def column(rho, wet, up, dn):
    hi = wet * dn(wet)
    strat = (dn(rho) - rho) * hi
    return rho, wet, hi, up(hi), 0.5 * (strat + up(strat))


def line(c, p, m, up, dn):
    c_rho, c_wet, c_hi, c_lo, c_cell = c
    p_rho, p_wet, p_hi, p_lo, p_cell = p
    m_rho, m_wet, m_hi, m_lo, m_cell = m
    mp, mm = c_wet * p_wet, c_wet * m_wet
    sp = taper((p_rho - c_rho) * mp / jnp.maximum(0.5 * (p_cell + c_cell), 1.0))
    sm = taper((c_rho - m_rho) * mm / jnp.maximum(0.5 * (m_cell + c_cell), 1.0))
    cx = 0.5 * (sp + sm)
    sw = 0.5 * (cx + dn(cx))
    fh = ((REDI + SKEW) * 0.25) * sw * c_hi
    zh = REDI * (sw * sw) * c_hi
    fl, zl = up(fh), up(zh)
    pp = ((REDI - SKEW) * 0.25) * sp * mp
    pm = -((REDI - SKEW) * 0.25) * sm * mm
    own_p, own_m = mp * (fh - fl), mm * (fl - fh)
    mph, mmh = dn(mp) * fh, dn(mm) * fh
    mpl, mml = up(mp) * fl, up(mm) * fl
    q = pp + pm
    return (
        (mpl - mml - q * c_lo + zl,
         q * (c_lo - c_hi) - REDI * (mp + mm) - (own_p + own_m) - (zh + zl),
         mmh - mph + q * c_hi + zh),
        (-pp * p_lo - mpl, REDI * mp + pp * (p_lo - p_hi) + own_p, pp * p_hi + mph),
        (mml - pm * m_lo, REDI * mm + pm * (m_lo - m_hi) + own_m, pm * m_hi - mmh),
    )


def total(terms):
    result = terms[0]
    for term in terms[1:]:
        result = result + term
    return result


def pick(value, index):
    return jnp.take_along_axis(value, index, axis=1)


def up3(v):
    return jnp.concatenate([jnp.zeros_like(v[:1]), v[:-1]], axis=0)


def dn3(v):
    return jnp.concatenate([v[1:], jnp.zeros_like(v[:1])], axis=0)


def applied(c, v):
    return c[1] * v + c[0] * up3(v) + c[2] * dn3(v)


def layout(splits, levels, lanes):
    slots = tuple(b - a + (2 if a == 0 else 0) for a, b in zip(splits, splits[1:]))
    pers = tuple((lanes - 2) // slot for slot in slots)
    return slots, pers, tuple((levels + per - 1) // per for per in pers)


def tracer_of(lane, lanes, tracers):
    return jnp.minimum(lax.shift_right_logical(lane + 1, 1) & (lanes // 2 - 1), tracers - 1)


def both(refs, offs, at, reg):
    rows, lanes = at.shape
    span = pl.ds(reg * rows, rows)
    west_side = lax.broadcasted_iota(jnp.int32, at.shape, 1) & 1 == 0
    wraps = any(off not in (0, 1) for off in offs)
    index = [at + off & (lanes - 1) if wraps else at + off for off in offs]
    picked = [pick(ref[span, :], i) for ref, i in zip(refs, index)]
    return jnp.where(west_side, *picked)


def values_of(refs, offs, spot, per, slot, first, levels):
    return jnp.stack([both(refs, offs, k % per * slot + spot, first + k // per) for k in range(levels)])


def insert_tiles(which, terms, src, dst):
    levels, rows, lanes = terms.shape
    lane = lax.broadcasted_iota(jnp.int32, (rows, lanes), 1)
    sides = jnp.logical_or(lane == 0, lane == lanes - 1)
    for t in which:
        for k in range(levels):
            term = pltpu.roll(terms[k], (lanes - 2 * t) % lanes, 1)
            place = pl.ds((t * levels + k) * rows, rows)
            dst[place, :] = src[place, :] + jnp.where(sides, term, 0.0)


def kernel(sizes, x_ref, kmt_ref, out_ref, add_ref, tab_ref, halo2, *scratch):
    pl.run_scoped(
        functools.partial(body, sizes, x_ref, kmt_ref, out_ref, add_ref, tab_ref, halo2, *scratch),
        pltpu.SemaphoreType.DMA((len(sizes[-1]) + 1,)),
        pltpu.SemaphoreType.DMA((5,)),
    )


def body(
    sizes, x_ref, kmt_ref, out_ref, add_ref, tab_ref, halo2,
    xv, kmt_int, coef, wcol, ecol, inner_w, inner_e, relay, halo1, from_n, from_s,
    recv_sem, load_sem, send_sem,
):
    tracers, levels, rows, lanes, n_lon, n_lat, groups = sizes
    lon, lat = lax.axis_index("lon"), lax.axis_index("lat")
    at_top = lat == n_lat - 1
    below_top = jnp.logical_not(at_top)
    inner = lat > 0
    at_bottom = jnp.logical_not(inner)
    even_lat = jnp.logical_and(inner, jnp.logical_and(lat % 2 == 0, below_top))
    odd_lat = jnp.logical_and(lat > 1, lat % 2 == 1)
    relayed = jnp.logical_and(lon == 0, even_lat)
    relays = jnp.logical_and(lon == 0, odd_lat)
    far = jnp.logical_and(lon == n_lon - 1, even_lat)
    direct, near = jnp.logical_not(relayed), jnp.logical_not(far)
    early = jnp.logical_and(lon == 0, direct)
    late = jnp.logical_not(early)
    late_top, late_below = jnp.logical_and(late, at_top), jnp.logical_and(late, below_top)
    urgent = jnp.logical_and(jnp.logical_and(late_below, lon == n_lon - 1), lat % 2 == 0)
    patient = jnp.logical_and(late_below, jnp.logical_not(urgent))
    e_dev = (lax.rem(lon + 1, n_lon), lat)
    w_dev = (lax.rem(lon + n_lon - 1, n_lon), lat)
    n_dev, s_dev = (lon, lat + 1), (lon, lat - 1)
    lat_up, lat_down = lax.rem(lat + 1, n_lat), lax.rem(lat + n_lat - 1, n_lat)
    fold_dev = (n_lon - 1 - lon, lat)
    tiles = tracers * levels
    plane = levels * rows
    lead = levels
    ends = [sum(groups[:i]) for i in range(len(groups) + 1)]
    splits = (0, *ends[2:])
    split = splits[1]
    slots, pers, shares = layout(splits, levels, lanes)
    firsts = [sum(shares[:n]) for n in range(3)]
    kmt_at = pers[0] * slots[0]

    load_kmt = pltpu.make_async_copy(kmt_ref, kmt_int, load_sem.at[len(groups)])
    load_kmt.start()

    def load(first, count, i):
        return pltpu.make_async_copy(
            x_ref.at[pl.ds(first, count)], xv.at[pl.ds(lead + first, count)], load_sem.at[i]
        )

    for i in range(len(groups)):
        for t in range(ends[i], ends[i + 1]):
            load(t * levels, levels, i).start()
    loads = [load(ends[i] * levels, groups[i] * levels, i) for i in range(len(groups))]
    flat = xv.reshape((lead + tiles) * rows, lanes)

    barrier = pltpu.get_barrier_semaphore()

    def greet(dev):
        pl.semaphore_signal(barrier, inc=1, device_id=dev, device_id_type=MESH)

    with jax.named_scope("greet"):
        greet(w_dev)

        @pl.when(near)
        def _():
            greet(e_dev)

        @pl.when(far)
        def _():
            greet((0, lat_up))

        @pl.when(at_top)
        def _():
            greet(fold_dev)

        @pl.when(below_top)
        def _():
            greet(n_dev)

        @pl.when(inner)
        def _():
            greet(s_dev)

    lane = lax.broadcasted_iota(jnp.int32, (rows, lanes), 1)
    row = lax.broadcasted_iota(jnp.int32, (rows, lanes), 0)

    def send(src, dst, s, r, dev):
        return pltpu.make_async_remote_copy(
            src_ref=src, dst_ref=dst, send_sem=send_sem.at[s], recv_sem=recv_sem.at[r],
            device_id=dev, device_id_type=MESH,
        )

    def rows_of(r, span, dst, s, into, dev):
        return send(xv.at[span, r, :], dst.at[span], s, into, dev)

    cut = lead + ends[-2] * levels
    starts = [lead - 1] + [lead + e * levels for e in ends[1:]]
    spans = [pl.ds(a, b - a) for a, b in zip(starts, starts[1:])]
    every = pl.ds(lead - 1, tiles + 1)
    halves = [(pl.ds(lead - 1, cut - lead + 1), 0), (spans[-1], 5)]
    fold = rows_of(rows - 1, every, from_n, 0, 0, fold_dev)
    folds = [
        rows_of(rows - 1, span, from_n, 0, 5 if i == len(spans) - 1 else 0, fold_dev)
        for i, span in enumerate(spans)
    ]
    to_n = rows_of(rows - 1, every, from_s, 0, 1, n_dev)
    to_s = rows_of(0, every, from_n, 1, 0, s_dev)
    to_ss = [rows_of(0, span, from_n, 1, r, s_dev) for span, r in halves]
    cols = [pl.ds(f * rows, n * rows) for f, n in zip(firsts, shares)]
    tail = sum(shares[1:]) * rows
    homes = [(halo1, 0, shares[0] * rows), (halo2, 0, tail), (halo2, shares[1] * rows, tail)]
    wests = [h.at[pl.ds(a, n * rows)] for (h, a, _), n in zip(homes, shares)]
    easts = [h.at[pl.ds(a + half, n * rows)] for (h, a, half), n in zip(homes, shares)]
    arrive = (2, 3, 3)
    far_dev = (n_lon - 1, lat_down)
    to_e = [send(ecol.at[c], wests[i], 2, arrive[i], e_dev) for i, c in enumerate(cols)]
    to_w = [send(wcol.at[c], easts[i], 3, arrive[i], w_dev) for i, c in enumerate(cols)]
    onward = [send(relay.at[c], easts[i], 4, arrive[i], far_dev) for i, c in enumerate(cols)]
    to_relay = send(wcol, relay, 3, 4, (lon, lat_up))
    got = [send(h, h, 2, r, e_dev) for h, r in ((halo1, 2), (halo2, 3))]
    all_e, all_w, all_onward = (send(c, relay, s, 4, e_dev) for c, s in ((ecol, 2), (wcol, 3), (relay, 4)))

    def tile(t, k):
        return flat[pl.ds(lead * rows + t * plane + k * rows, rows), :]

    def density(k):
        return HALINE * tile(1, k) - THERMAL * tile(0, k)

    def where_is(t, k):
        n = sum(t >= s for s in splits[1:])
        return k % pers[n] * slots[n] + t - splits[n], firsts[n] + k // pers[n]

    def gather_columns(e_ref, w_ref, e_off, w_off, before=None, after=None):
        zeros = jnp.zeros((rows, lanes), jnp.float32)
        es, ws = [zeros] * sum(shares), [zeros] * sum(shares)

        def place(value, at, reg):
            value = pltpu.roll(value, at + 1, 1)
            es[reg] = jnp.where(lane == (at + e_off) % lanes, value, es[reg])
            ws[reg] = jnp.where(lane == (at + w_off) % lanes, value, ws[reg])

        for i in range(len(groups)):
            if before is not None:
                before(i)
            if i == 0:
                place(kmt_own, kmt_at, 0)
                for k in range(levels):
                    at, reg = where_is(0, k)
                    place(density(k), at + split, reg)
            for t in range(ends[i], ends[i + 1]):
                for k in range(levels):
                    place(tile(t, k), *where_is(t, k))
            if ends[i + 1] in splits:
                n = splits.index(ends[i + 1]) - 1
                for j in range(firsts[n], firsts[n] + shares[n]):
                    e_ref[pl.ds(j * rows, rows), :] = es[j]
                    w_ref[pl.ds(j * rows, rows), :] = ws[j]
                if after is not None:
                    after(n)

    def enter():
        @pl.when(at_bottom)
        def _():
            pl.semaphore_wait(barrier, 3)

        @pl.when(jnp.logical_and(inner, jnp.logical_not(jnp.logical_or(relayed, relays))))
        def _():
            pl.semaphore_wait(barrier, 4)

        @pl.when(relayed)
        def _():
            pl.semaphore_wait(barrier, 3)

        @pl.when(relays)
        def _():
            pl.semaphore_wait(barrier, 5)

    def send_inner_rows():
        @pl.when(below_top)
        def _():
            to_n.start()

        @pl.when(inner)
        def _():
            for copy in to_ss:
                copy.start()

    def before(i):
        with jax.named_scope(f"load{i}"):
            loads[i].wait()
        if i == 0:

            @pl.when(late_top)
            def _():
                enter()

        if i < len(groups) - 1:

            @pl.when(late_top)
            def _():
                folds[i].start()

    def send_part(n, who):
        @pl.when(who)
        def _():
            to_e[n].start()

        @pl.when(jnp.logical_and(who, direct))
        def _():
            to_w[n].start()

    def after(n):
        if n < 2:

            @pl.when(patient if n else urgent)
            def _():
                with jax.named_scope("barrier"):
                    enter()

        if n == 1:
            send_part(0, patient)
        send_part(n, late if n else jnp.logical_and(late, jnp.logical_not(patient)))

    with jax.named_scope("loadk"):
        load_kmt.wait()
    kmt_own = kmt_int[...].astype(jnp.float32)
    xv[lead - 1, :, :] = kmt_own
    gather_columns(ecol, wcol, 0, 1, before, after)
    with jax.named_scope("send"):

        @pl.when(relayed)
        def _():
            to_relay.start()

        @pl.when(late_top)
        def _():
            folds[-1].start()

        @pl.when(late)
        def _():
            send_inner_rows()

    with jax.named_scope("inner"):
        gather_columns(inner_e, inner_w, -1, 2)

        @pl.when(at_bottom)
        def _():
            for t in range(tracers + 1):
                from_s[pl.ds(t * levels, levels), :] = jnp.zeros((levels, lanes), jnp.float32)

    def put(d, dk, k, value):
        coef[pl.ds(((d * 3 + dk) * levels + k) * rows, rows), :] = value

    def piece_of(d, dk, k):
        return coef[pl.ds(((d * 3 + dk) * levels + k) * rows, rows), :]

    with jax.named_scope("coefs"):
        def shifted(v, by, axis):
            return jnp.stack([pltpu.roll(v[k], by, axis) for k in range(levels)])

        own_rho = jnp.stack([density(k) for k in range(levels)])
        own_wet = jnp.stack([(kmt_own > float(k)).astype(jnp.float32) for k in range(levels)])
        c3 = column(own_rho, own_wet, up3, dn3)

        def moved(by, axis):
            return tuple(shifted(v, by, axis) for v in c3)

        mid_lane = jnp.logical_and(lane > 0, lane < lanes - 1)
        xc, xe, xw = line(c3, moved(lanes - 1, 1), moved(1, 1), up3, dn3)
        for dk in range(3):
            for k in range(levels):
                put(E, dk, k, jnp.where(mid_lane, xe[dk][k], 0.0))
                put(W, dk, k, jnp.where(mid_lane, xw[dk][k], 0.0))
                put(C, dk, k, jnp.where(mid_lane, xc[dk][k], 0.0))
        mid_row = jnp.logical_and(row > 0, row < rows - 1)
        yc, yn, ys = line(c3, moved(rows - 1, 0), moved(1, 0), up3, dn3)
        for dk in range(3):
            for k in range(levels):
                put(N, dk, k, jnp.where(mid_row, yn[dk][k], 0.0))
                put(S, dk, k, jnp.where(mid_row, ys[dk][k], 0.0))
                core = piece_of(C, dk, k) + jnp.where(mid_row, yc[dk][k], 0.0)
                put(C, dk, k, core + 1.0 if dk == 1 else core)

    with jax.named_scope("main"):

        @pl.loop(0, tracers // TOGETHER)
        def _(i):
            fields = []
            for u in range(TOGETHER):
                base = pl.multiple_of(lead * rows + (i * TOGETHER + u) * plane, rows)
                field = []
                for k in range(levels):
                    own = flat[pl.ds(base + k * rows, rows), :]
                    field.append((
                        own, pltpu.roll(own, lanes - 1, 1), pltpu.roll(own, 1, 1),
                        pltpu.roll(own, rows - 1, 0), pltpu.roll(own, 1, 0),
                    ))
                fields.append(field)
            for k in range(levels):
                sums = [None] * TOGETHER
                for d in range(5):
                    for dk in range(3):
                        if not 0 <= k + dk - 1 < levels:
                            continue
                        c = piece_of(d, dk, k)
                        for u in range(TOGETHER):
                            term = c * fields[u][k + dk - 1][d]
                            sums[u] = term if sums[u] is None else sums[u] + term
                for u in range(TOGETHER):
                    base = pl.multiple_of((i * TOGETHER + u) * plane, rows)
                    out_ref[pl.ds(base + k * rows, rows), :] = sums[u]

    @pl.when(early)
    def _():
        with jax.named_scope("barrier"):
            enter()
        for copy in to_e + to_w:
            copy.start()
        send_inner_rows()

        @pl.when(at_top)
        def _():
            for copy in folds:
                copy.start()

    @pl.when(relays)
    def _():
        to_relay.wait_recv()
        for copy in onward:
            copy.start()

    level = lax.broadcasted_iota(jnp.int32, (levels, lanes), 0)
    level_f = level.astype(jnp.float32)

    def up_s(v):
        return jnp.where(level == 0, 0.0, pltpu.roll(v, 1, 0))

    def dn_s(v):
        return jnp.where(level == levels - 1, 0.0, pltpu.roll(v, levels - 1, 0))

    def at_row(t, r):
        return flat[pl.ds(lead * rows + t * plane + r, levels, stride=rows), :]

    def row_column(t0, t1, kmt):
        wet = (jnp.broadcast_to(kmt, (levels, lanes)) > level_f).astype(jnp.float32)
        return column(HALINE * t1 - THERMAL * t0, wet, up_s, dn_s)

    def own_row(r):
        return row_column(at_row(0, r), at_row(1, r), kmt_own[r : r + 1, :])

    def fix_rows(source, r, r_in, north, turn, parts):
        def halo(t):
            h = source[pl.ds(lead + t * levels, levels), :]
            return pick(h, lanes - 1 - lane) if turn else h

        first, last, wait = parts[0]
        wait()
        k = jnp.broadcast_to(source[pl.ds(lead - 1, 1), :], (rows, lanes))
        k = (pick(k, lanes - 1 - lane) if turn else k)[:1, :]
        out_c, in_c = row_column(halo(0), halo(1), k), own_row(r_in)
        p, m = (out_c, in_c) if north else (in_c, out_c)
        cc, cp, cm = line(own_row(r), p, m, up_s, dn_s)
        c_out, c_in = (cp, cm) if north else (cm, cp)
        table = (cc, c_out, c_in)
        lo = [pltpu.roll(c[0], levels - 1, 0) for c in table]
        mid = [c[1] for c in table]
        hi = [pltpu.roll(c[2], 1, 0) for c in table]
        for n, (first, last, wait) in enumerate(parts):
            if n:
                wait()
            count = last - first
            batch = count if turn else next(b for b in (8, 5, 4, 3, 2, 1) if count % b == 0)

            @pl.loop(0, count // batch)
            def _(i, first=first, batch=batch):
                for u in range(batch):
                    t = first + i * batch + u
                    values = (at_row(t, r), halo(t), at_row(t, r_in))
                    above = total([c * v for c, v in zip(lo, values)])
                    same = total([c * v for c, v in zip(mid, values)])
                    below = total([c * v for c, v in zip(hi, values)])
                    place = pl.ds(t * plane + r, levels, stride=rows)
                    out_ref[place, :] = (
                        out_ref[place, :] + same + pltpu.roll(above, 1, 0) + pltpu.roll(below, levels - 1, 0)
                    )

    def fix_n(turn):
        parts = [(0, ends[-2], to_ss[0].wait_recv), (ends[-2], tracers, to_ss[1].wait_recv)]
        fix_rows(from_n, rows - 1, rows - 2, True, turn, parts)

    with jax.named_scope("fixs"):

        @pl.when(inner)
        def _():
            to_n.wait_recv()

        fix_rows(from_s, 0, 1, False, False, [(0, tracers, lambda: None)])

    with jax.named_scope("fixn"):

        @pl.when(below_top)
        def _():
            fix_n(False)

    spot = tracer_of(lane, lanes, tracers)

    def part_of(refs, offs, n):
        at = jnp.clip(spot - splits[n], 0, splits[n + 1] - splits[n] - 1)
        return values_of(refs, offs, at, pers[n], slots[n], firsts[n], levels)

    def column_of(refs, offs):
        fixed = jnp.zeros((rows, lanes), jnp.int32)
        rho = jnp.stack([both(refs, offs, fixed + (where_is(0, k)[0] + split), where_is(0, k)[1])
                         for k in range(levels)])
        kmt = both(refs, offs, fixed + kmt_at, 0)
        wet = jnp.stack([(kmt > float(k)).astype(jnp.float32) for k in range(levels)])
        return column(rho, wet, up3, dn3)

    def joined(*args):
        a, b, c = (part_of(*args, n) for n in range(3))
        return jnp.stack([
            jnp.where(spot < splits[1], a[k], jnp.where(spot < splits[2], b[k], c[k])) for k in range(levels)
        ])

    with jax.named_scope("fixc0"):
        own_at, ins_at, outs_at = ((wcol, ecol), (1, 0)), ((inner_w, inner_e), (2, -1)), ((wests[0], easts[0]), (0, 1))
        own_c, ins_c = column_of(*own_at), column_of(*ins_at)
        own, ins = joined(*own_at), joined(*ins_at)
    with jax.named_scope("waitc"):
        got[0].wait_recv()
    with jax.named_scope("fixc1"):
        own_t, outs_t, ins_t = line(own_c, column_of(*outs_at), ins_c, up3, dn3)
        some = applied(own_t, own) + applied(ins_t, ins)
        full = some + applied(outs_t, part_of(*outs_at, 0))
        for k in range(levels):
            add_ref[pl.ds(k * rows, rows), :] = some[k]
            for dk in range(3):
                tab_ref[pl.ds((dk * levels + k) * rows, rows), :] = outs_t[dk][k]
        insert_tiles(range(split), full, out_ref, out_ref)

    with jax.named_scope("fixtop"):

        @pl.when(at_top)
        def _():
            fix_n(True)

    with jax.named_scope("waitc2"):
        got[1].wait_recv()

    with jax.named_scope("end"):
        fold.wait_send()

        @pl.when(inner)
        def _():
            to_s.wait_send()

        all_e.wait_send()
        all_w.wait_send()

        @pl.when(relays)
        def _():
            all_onward.wait_send()


def finish(sizes, part_ref, add_ref, tab_ref, halo_ref, out_ref, stage, sem):
    tracers, levels, rows, lanes, splits = sizes
    plane = levels * rows
    slots, pers, shares = layout(splits, levels, lanes)
    lane = lax.broadcasted_iota(jnp.int32, (rows, lanes), 1)
    spot = tracer_of(lane, lanes, tracers)
    half = sum(shares[1:]) * rows

    def write(ref, first, count):
        span = pl.ds(pl.multiple_of(first * plane, plane), count * plane)
        pltpu.make_async_copy(ref.at[span], out_ref.at[span], sem).start()

    def terms_of(n):
        refs = [halo_ref.at[pl.ds(i * half, half)] for i in range(2)]
        at = jnp.clip(spot - splits[n], 0, splits[n + 1] - splits[n] - 1)
        values = values_of(refs, (0, 1), at, pers[n], slots[n], (n - 1) * shares[1], levels)
        table = [
            jnp.stack([tab_ref[pl.ds((dk * levels + k) * rows, rows), :] for k in range(levels)]) for dk in range(3)
        ]
        return jnp.stack([add_ref[pl.ds(k * rows, rows), :] for k in range(levels)]) + applied(table, values)

    with jax.named_scope("insert"):
        ready = splits[1] // 2

        @pl.loop(0, 2)
        def _(i):
            write(part_ref, i * ready, ready)

        terms = [terms_of(1), None]
        for n in (1, 2):
            for t in range(splits[n], splits[n + 1], STORE):
                last = min(t + STORE, splits[n + 1])
                insert_tiles(range(t, last), terms[n - 1], part_ref, stage)
                write(stage, t, last - t)
                if terms[1] is None:
                    terms[1] = terms_of(2)
    with jax.named_scope("written"):
        pltpu.make_async_copy(stage, out_ref, sem).wait()


def solution(mesh):
    n_lon, n_lat = mesh.shape["lon"], mesh.shape["lat"]

    def local(tracers, kmt):
        nt, levels, rows, lanes = tracers.shape
        tiles = nt * levels
        most = (lanes - 2) // levels
        split = max(nt - most, nt // 2)
        cuts = (0, split // 6, min(split // 2, max(most - 2, 2)), split, nt)
        splits = (0, *cuts[2:])
        groups = tuple(b - a for a, b in zip(cuts, cuts[1:]))
        shares = layout(splits, levels, lanes)[-1]
        regs = sum(shares)
        assert levels == rows and groups[0] > 1 and cuts[2] % 2 == 0 and lanes & (lanes - 1) == 0

        def vmem(*shape):
            return pltpu.VMEM(shape, jnp.float32)

        parts = pl.pallas_call(
            functools.partial(kernel, (nt, levels, rows, lanes, n_lon, n_lat, groups)),
            out_shape=[
                vmem(tiles * rows, lanes),
                vmem(levels * rows, lanes),
                vmem(3 * levels * rows, lanes),
                vmem(2 * sum(shares[1:]) * rows, lanes),
            ],
            in_specs=[pl.BlockSpec(memory_space=pltpu.HBM), pl.BlockSpec(memory_space=pltpu.HBM)],
            out_specs=[pl.BlockSpec(memory_space=pltpu.VMEM)] * 4,
            scratch_shapes=[
                vmem(tiles + levels, rows, lanes),
                pltpu.VMEM((rows, lanes), jnp.int32),
                vmem(15 * levels * rows, lanes),
            ]
            + [vmem(regs * rows, lanes)] * 5
            + [vmem(2 * shares[0] * rows, lanes)]
            + [vmem(tiles + rows, lanes)] * 2
            + [
                pltpu.SemaphoreType.DMA((6,)),
            ],
            compiler_params=pltpu.CompilerParams(collective_id=0, has_side_effects=True),
        )(tracers.reshape(tiles, rows, lanes), kmt)
        parts = [pltpu.with_memory_space_constraint(v, pltpu.VMEM) for v in parts]
        out = pl.pallas_call(
            functools.partial(finish, (nt, levels, rows, lanes, splits)),
            out_shape=jax.ShapeDtypeStruct((tiles * rows, lanes), jnp.float32),
            in_specs=[pl.BlockSpec(memory_space=pltpu.VMEM)] * 4,
            out_specs=pl.BlockSpec(memory_space=pltpu.HBM),
            scratch_shapes=[vmem(tiles * rows, lanes), pltpu.SemaphoreType.DMA],
        )(*parts)
        return out.reshape(nt, levels, rows, lanes)

    return jax.shard_map(
        local,
        mesh=mesh,
        in_specs=(P(None, None, "lat", "lon"), P("lat", "lon")),
        out_specs=P(None, None, "lat", "lon"),
        check_vma=False,
    )
```

```python
import functools

import jax
import jax.numpy as jnp
from jax import lax
from jax.experimental import pallas as pl
from jax.experimental.pallas import tpu as pltpu
from jax.sharding import PartitionSpec as P

THERMAL = 0.2
HALINE = 0.8
REDI = 0.1
SKEW = 0.05
SLOPE_MAX = 0.6
SLOPE_WIDTH = 0.2

MESH = pl.DeviceIdType.MESH
TOGETHER = 2
STORE = 2
C, E, W, N, S = range(5)


def taper(slope):
    return slope * 0.5 * (1.0 + jnp.tanh((SLOPE_MAX - jnp.abs(slope)) / SLOPE_WIDTH))


def column(rho, wet, up, dn):
    hi = wet * dn(wet)
    strat = (dn(rho) - rho) * hi
    return rho, wet, hi, up(hi), 0.5 * (strat + up(strat))


def line(c, p, m, up, dn):
    c_rho, c_wet, c_hi, c_lo, c_cell = c
    p_rho, p_wet, p_hi, p_lo, p_cell = p
    m_rho, m_wet, m_hi, m_lo, m_cell = m
    mp, mm = c_wet * p_wet, c_wet * m_wet
    sp = taper((p_rho - c_rho) * mp / jnp.maximum(0.5 * (p_cell + c_cell), 1.0))
    sm = taper((c_rho - m_rho) * mm / jnp.maximum(0.5 * (m_cell + c_cell), 1.0))
    cx = 0.5 * (sp + sm)
    sw = 0.5 * (cx + dn(cx))
    fh = ((REDI + SKEW) * 0.25) * sw * c_hi
    zh = REDI * (sw * sw) * c_hi
    fl, zl = up(fh), up(zh)
    pp = ((REDI - SKEW) * 0.25) * sp * mp
    pm = -((REDI - SKEW) * 0.25) * sm * mm
    own_p, own_m = mp * (fh - fl), mm * (fl - fh)
    mph, mmh = dn(mp) * fh, dn(mm) * fh
    mpl, mml = up(mp) * fl, up(mm) * fl
    q = pp + pm
    return (
        (mpl - mml - q * c_lo + zl,
         q * (c_lo - c_hi) - REDI * (mp + mm) - (own_p + own_m) - (zh + zl),
         mmh - mph + q * c_hi + zh),
        (-pp * p_lo - mpl, REDI * mp + pp * (p_lo - p_hi) + own_p, pp * p_hi + mph),
        (mml - pm * m_lo, REDI * mm + pm * (m_lo - m_hi) + own_m, pm * m_hi - mmh),
    )


def total(terms):
    result = terms[0]
    for term in terms[1:]:
        result = result + term
    return result


def pick(value, index):
    return jnp.take_along_axis(value, index, axis=1)


def up3(v):
    return jnp.concatenate([jnp.zeros_like(v[:1]), v[:-1]], axis=0)


def dn3(v):
    return jnp.concatenate([v[1:], jnp.zeros_like(v[:1])], axis=0)


def applied(c, v):
    return c[1] * v + c[0] * up3(v) + c[2] * dn3(v)


def layout(splits, levels, lanes):
    slots = tuple(b - a + (2 if a == 0 else 0) for a, b in zip(splits, splits[1:]))
    pers = tuple((lanes - 2) // slot for slot in slots)
    return slots, pers, tuple((levels + per - 1) // per for per in pers)


def tracer_of(lane, lanes, tracers):
    return jnp.minimum(lax.shift_right_logical(lane + 1, 1) & (lanes // 2 - 1), tracers - 1)


def both(refs, offs, at, reg):
    rows, lanes = at.shape
    span = pl.ds(reg * rows, rows)
    west_side = lax.broadcasted_iota(jnp.int32, at.shape, 1) & 1 == 0
    wraps = any(off not in (0, 1) for off in offs)
    index = [at + off & (lanes - 1) if wraps else at + off for off in offs]
    picked = [pick(ref[span, :], i) for ref, i in zip(refs, index)]
    return jnp.where(west_side, *picked)


def values_of(refs, offs, spot, per, slot, first, levels):
    return jnp.stack([both(refs, offs, k % per * slot + spot, first + k // per) for k in range(levels)])


def insert_tiles(which, terms, src, dst):
    levels, rows, lanes = terms.shape
    lane = lax.broadcasted_iota(jnp.int32, (rows, lanes), 1)
    sides = jnp.logical_or(lane == 0, lane == lanes - 1)
    for t in which:
        for k in range(levels):
            term = pltpu.roll(terms[k], (lanes - 2 * t) % lanes, 1)
            place = pl.ds((t * levels + k) * rows, rows)
            dst[place, :] = src[place, :] + jnp.where(sides, term, 0.0)


def kernel(sizes, x_ref, kmt_ref, out_ref, add_ref, tab_ref, halo2, *scratch):
    pl.run_scoped(
        functools.partial(body, sizes, x_ref, kmt_ref, out_ref, add_ref, tab_ref, halo2, *scratch),
        pltpu.SemaphoreType.DMA((len(sizes[-1]) + 1,)),
        pltpu.SemaphoreType.DMA((5,)),
    )


def body(
    sizes, x_ref, kmt_ref, out_ref, add_ref, tab_ref, halo2,
    xv, kmt_int, coef, wcol, ecol, inner_w, inner_e, relay, halo0, halo1, from_n, from_s,
    recv_sem, load_sem, send_sem,
):
    tracers, levels, rows, lanes, n_lon, n_lat, groups = sizes
    lon, lat = lax.axis_index("lon"), lax.axis_index("lat")
    at_top = lat == n_lat - 1
    below_top = jnp.logical_not(at_top)
    inner = lat > 0
    at_bottom = jnp.logical_not(inner)
    even_lat = jnp.logical_and(inner, jnp.logical_and(lat % 2 == 0, below_top))
    odd_lat = jnp.logical_and(lat > 1, lat % 2 == 1)
    relayed = jnp.logical_and(lon == 0, even_lat)
    relays = jnp.logical_and(lon == 0, odd_lat)
    far = jnp.logical_and(lon == n_lon - 1, even_lat)
    direct, near = jnp.logical_not(relayed), jnp.logical_not(far)
    early = jnp.logical_and(lon == 0, direct)
    late = jnp.logical_not(early)
    late_top, late_below = jnp.logical_and(late, at_top), jnp.logical_and(late, below_top)
    urgent = jnp.logical_and(jnp.logical_and(late_below, lon == n_lon - 1), lat % 2 == 0)
    patient = jnp.logical_and(late_below, jnp.logical_not(urgent))
    e_dev = (lax.rem(lon + 1, n_lon), lat)
    w_dev = (lax.rem(lon + n_lon - 1, n_lon), lat)
    n_dev, s_dev = (lon, lat + 1), (lon, lat - 1)
    lat_up, lat_down = lax.rem(lat + 1, n_lat), lax.rem(lat + n_lat - 1, n_lat)
    fold_dev = (n_lon - 1 - lon, lat)
    tiles = tracers * levels
    plane = levels * rows
    lead = levels
    ends = [sum(groups[:i]) for i in range(len(groups) + 1)]
    splits = (0, *ends[2:])
    split = splits[1]
    slots, pers, shares = layout(splits, levels, lanes)
    firsts = [sum(shares[:n]) for n in range(3)]
    kmt_at = pers[0] * slots[0]

    load_kmt = pltpu.make_async_copy(kmt_ref, kmt_int, load_sem.at[len(groups)])
    load_kmt.start()

    def load(first, count, i):
        return pltpu.make_async_copy(
            x_ref.at[pl.ds(first, count)], xv.at[pl.ds(lead + first, count)], load_sem.at[i]
        )

    for i in range(len(groups)):
        for t in range(ends[i], ends[i + 1]):
            load(t * levels, levels, i).start()
    loads = [load(ends[i] * levels, groups[i] * levels, i) for i in range(len(groups))]
    flat = xv.reshape((lead + tiles) * rows, lanes)

    barrier = pltpu.get_barrier_semaphore()

    def greet(dev):
        pl.semaphore_signal(barrier, inc=1, device_id=dev, device_id_type=MESH)

    with jax.named_scope("greet"):
        greet(w_dev)

        @pl.when(near)
        def _():
            greet(e_dev)

        @pl.when(far)
        def _():
            greet((0, lat_up))

        @pl.when(at_top)
        def _():
            greet(fold_dev)

        @pl.when(below_top)
        def _():
            greet(n_dev)

        @pl.when(inner)
        def _():
            greet(s_dev)

    lane = lax.broadcasted_iota(jnp.int32, (rows, lanes), 1)
    row = lax.broadcasted_iota(jnp.int32, (rows, lanes), 0)

    def send(src, dst, s, r, dev):
        return pltpu.make_async_remote_copy(
            src_ref=src, dst_ref=dst, send_sem=send_sem.at[s], recv_sem=recv_sem.at[r],
            device_id=dev, device_id_type=MESH,
        )

    def rows_of(r, span, dst, s, into, dev):
        return send(xv.at[span, r, :], dst.at[span], s, into, dev)

    cut = lead + ends[-2] * levels
    starts = [lead - 1] + [lead + e * levels for e in ends[1:]]
    spans = [pl.ds(a, b - a) for a, b in zip(starts, starts[1:])]
    every = pl.ds(lead - 1, tiles + 1)
    halves = [(pl.ds(lead - 1, cut - lead + 1), 0), (spans[-1], 5)]
    fold = rows_of(rows - 1, every, from_n, 0, 0, fold_dev)
    folds = [
        rows_of(rows - 1, span, from_n, 0, 5 if i == len(spans) - 1 else 0, fold_dev)
        for i, span in enumerate(spans)
    ]
    to_n = rows_of(rows - 1, every, from_s, 0, 1, n_dev)
    to_s = rows_of(0, every, from_n, 1, 0, s_dev)
    to_ss = [rows_of(0, span, from_n, 1, r, s_dev) for span, r in halves]
    cols = [pl.ds(f * rows, n * rows) for f, n in zip(firsts, shares)]
    halos = (halo0, halo1, halo2)
    wests = [h.at[pl.ds(0, n * rows)] for h, n in zip(halos, shares)]
    easts = [h.at[pl.ds(n * rows, n * rows)] for h, n in zip(halos, shares)]
    arrive = (2, 3, 6)
    far_dev = (n_lon - 1, lat_down)
    to_e = [send(ecol.at[c], wests[i], 2, arrive[i], e_dev) for i, c in enumerate(cols)]
    to_w = [send(wcol.at[c], easts[i], 3, arrive[i], w_dev) for i, c in enumerate(cols)]
    onward = [send(relay.at[c], easts[i], 4, arrive[i], far_dev) for i, c in enumerate(cols)]
    to_relay = send(wcol, relay, 3, 4, (lon, lat_up))
    got = [send(h, h, 2, r, e_dev) for h, r in zip(halos, arrive)]
    all_e, all_w, all_onward = (send(c, relay, s, 4, e_dev) for c, s in ((ecol, 2), (wcol, 3), (relay, 4)))

    def tile(t, k):
        return flat[pl.ds(lead * rows + t * plane + k * rows, rows), :]

    def density(k):
        return HALINE * tile(1, k) - THERMAL * tile(0, k)

    def where_is(t, k):
        n = sum(t >= s for s in splits[1:])
        return k % pers[n] * slots[n] + t - splits[n], firsts[n] + k // pers[n]

    def gather_columns(e_ref, w_ref, e_off, w_off, before=None, after=None):
        zeros = jnp.zeros((rows, lanes), jnp.float32)
        es, ws = [zeros] * sum(shares), [zeros] * sum(shares)

        def place(value, at, reg):
            value = pltpu.roll(value, at + 1, 1)
            es[reg] = jnp.where(lane == (at + e_off) % lanes, value, es[reg])
            ws[reg] = jnp.where(lane == (at + w_off) % lanes, value, ws[reg])

        for i in range(len(groups)):
            if before is not None:
                before(i)
            if i == 0:
                place(kmt_own, kmt_at, 0)
                for k in range(levels):
                    at, reg = where_is(0, k)
                    place(density(k), at + split, reg)
            for t in range(ends[i], ends[i + 1]):
                for k in range(levels):
                    place(tile(t, k), *where_is(t, k))
            if ends[i + 1] in splits:
                n = splits.index(ends[i + 1]) - 1
                for j in range(firsts[n], firsts[n] + shares[n]):
                    e_ref[pl.ds(j * rows, rows), :] = es[j]
                    w_ref[pl.ds(j * rows, rows), :] = ws[j]
                if after is not None:
                    after(n)

    def enter():
        @pl.when(at_bottom)
        def _():
            pl.semaphore_wait(barrier, 3)

        @pl.when(jnp.logical_and(inner, jnp.logical_not(jnp.logical_or(relayed, relays))))
        def _():
            pl.semaphore_wait(barrier, 4)

        @pl.when(relayed)
        def _():
            pl.semaphore_wait(barrier, 3)

        @pl.when(relays)
        def _():
            pl.semaphore_wait(barrier, 5)

    def send_inner_rows():
        @pl.when(below_top)
        def _():
            to_n.start()

        @pl.when(inner)
        def _():
            for copy in to_ss:
                copy.start()

    def before(i):
        with jax.named_scope(f"load{i}"):
            loads[i].wait()
        if i == 0:

            @pl.when(late_top)
            def _():
                enter()

        if i < len(groups) - 1:

            @pl.when(late_top)
            def _():
                folds[i].start()

    def send_part(n, who):
        @pl.when(who)
        def _():
            to_e[n].start()

        @pl.when(jnp.logical_and(who, direct))
        def _():
            to_w[n].start()

    def after(n):
        if n < 2:

            @pl.when(patient if n else urgent)
            def _():
                with jax.named_scope("barrier"):
                    enter()

        if n == 1:
            send_part(0, patient)
        send_part(n, late if n else jnp.logical_and(late, jnp.logical_not(patient)))

    with jax.named_scope("loadk"):
        load_kmt.wait()
    kmt_own = kmt_int[...].astype(jnp.float32)
    xv[lead - 1, :, :] = kmt_own
    gather_columns(ecol, wcol, 0, 1, before, after)
    with jax.named_scope("send"):

        @pl.when(relayed)
        def _():
            to_relay.start()

        @pl.when(late_top)
        def _():
            folds[-1].start()

        @pl.when(late)
        def _():
            send_inner_rows()

    with jax.named_scope("inner"):
        gather_columns(inner_e, inner_w, -1, 2)

        @pl.when(at_bottom)
        def _():
            for t in range(tracers + 1):
                from_s[pl.ds(t * levels, levels), :] = jnp.zeros((levels, lanes), jnp.float32)

    def put(d, dk, k, value):
        coef[pl.ds(((d * 3 + dk) * levels + k) * rows, rows), :] = value

    def piece_of(d, dk, k):
        return coef[pl.ds(((d * 3 + dk) * levels + k) * rows, rows), :]

    with jax.named_scope("coefs"):
        def shifted(v, by, axis):
            return jnp.stack([pltpu.roll(v[k], by, axis) for k in range(levels)])

        own_rho = jnp.stack([density(k) for k in range(levels)])
        own_wet = jnp.stack([(kmt_own > float(k)).astype(jnp.float32) for k in range(levels)])
        c3 = column(own_rho, own_wet, up3, dn3)

        def moved(by, axis):
            return tuple(shifted(v, by, axis) for v in c3)

        mid_lane = jnp.logical_and(lane > 0, lane < lanes - 1)
        xc, xe, xw = line(c3, moved(lanes - 1, 1), moved(1, 1), up3, dn3)
        for dk in range(3):
            for k in range(levels):
                put(E, dk, k, jnp.where(mid_lane, xe[dk][k], 0.0))
                put(W, dk, k, jnp.where(mid_lane, xw[dk][k], 0.0))
                put(C, dk, k, jnp.where(mid_lane, xc[dk][k], 0.0))
        mid_row = jnp.logical_and(row > 0, row < rows - 1)
        yc, yn, ys = line(c3, moved(rows - 1, 0), moved(1, 0), up3, dn3)
        for dk in range(3):
            for k in range(levels):
                put(N, dk, k, jnp.where(mid_row, yn[dk][k], 0.0))
                put(S, dk, k, jnp.where(mid_row, ys[dk][k], 0.0))
                core = piece_of(C, dk, k) + jnp.where(mid_row, yc[dk][k], 0.0)
                put(C, dk, k, core + 1.0 if dk == 1 else core)

    with jax.named_scope("main"):

        @pl.loop(0, tracers // TOGETHER)
        def _(i):
            fields = []
            for u in range(TOGETHER):
                base = pl.multiple_of(lead * rows + (i * TOGETHER + u) * plane, rows)
                field = []
                for k in range(levels):
                    own = flat[pl.ds(base + k * rows, rows), :]
                    field.append((
                        own, pltpu.roll(own, lanes - 1, 1), pltpu.roll(own, 1, 1),
                        pltpu.roll(own, rows - 1, 0), pltpu.roll(own, 1, 0),
                    ))
                fields.append(field)
            for k in range(levels):
                sums = [None] * TOGETHER
                for d in range(5):
                    for dk in range(3):
                        if not 0 <= k + dk - 1 < levels:
                            continue
                        c = piece_of(d, dk, k)
                        for u in range(TOGETHER):
                            term = c * fields[u][k + dk - 1][d]
                            sums[u] = term if sums[u] is None else sums[u] + term
                for u in range(TOGETHER):
                    base = pl.multiple_of((i * TOGETHER + u) * plane, rows)
                    out_ref[pl.ds(base + k * rows, rows), :] = sums[u]

    @pl.when(early)
    def _():
        with jax.named_scope("barrier"):
            enter()
        for copy in to_e + to_w:
            copy.start()
        send_inner_rows()

        @pl.when(at_top)
        def _():
            for copy in folds:
                copy.start()

    @pl.when(relays)
    def _():
        to_relay.wait_recv()
        for copy in onward:
            copy.start()

    level = lax.broadcasted_iota(jnp.int32, (levels, lanes), 0)
    level_f = level.astype(jnp.float32)

    def up_s(v):
        return jnp.where(level == 0, 0.0, pltpu.roll(v, 1, 0))

    def dn_s(v):
        return jnp.where(level == levels - 1, 0.0, pltpu.roll(v, levels - 1, 0))

    def at_row(t, r):
        return flat[pl.ds(lead * rows + t * plane + r, levels, stride=rows), :]

    def row_column(t0, t1, kmt):
        wet = (jnp.broadcast_to(kmt, (levels, lanes)) > level_f).astype(jnp.float32)
        return column(HALINE * t1 - THERMAL * t0, wet, up_s, dn_s)

    def own_row(r):
        return row_column(at_row(0, r), at_row(1, r), kmt_own[r : r + 1, :])

    def fix_rows(source, r, r_in, north, turn, parts):
        def halo(t):
            h = source[pl.ds(lead + t * levels, levels), :]
            return pick(h, lanes - 1 - lane) if turn else h

        first, last, wait = parts[0]
        wait()
        k = jnp.broadcast_to(source[pl.ds(lead - 1, 1), :], (rows, lanes))
        k = (pick(k, lanes - 1 - lane) if turn else k)[:1, :]
        out_c, in_c = row_column(halo(0), halo(1), k), own_row(r_in)
        p, m = (out_c, in_c) if north else (in_c, out_c)
        cc, cp, cm = line(own_row(r), p, m, up_s, dn_s)
        c_out, c_in = (cp, cm) if north else (cm, cp)
        table = (cc, c_out, c_in)
        lo = [pltpu.roll(c[0], levels - 1, 0) for c in table]
        mid = [c[1] for c in table]
        hi = [pltpu.roll(c[2], 1, 0) for c in table]
        for n, (first, last, wait) in enumerate(parts):
            if n:
                wait()
            count = last - first
            batch = count if turn else next(b for b in (8, 5, 4, 3, 2, 1) if count % b == 0)

            @pl.loop(0, count // batch)
            def _(i, first=first, batch=batch):
                for u in range(batch):
                    t = first + i * batch + u
                    values = (at_row(t, r), halo(t), at_row(t, r_in))
                    above = total([c * v for c, v in zip(lo, values)])
                    same = total([c * v for c, v in zip(mid, values)])
                    below = total([c * v for c, v in zip(hi, values)])
                    place = pl.ds(t * plane + r, levels, stride=rows)
                    out_ref[place, :] = (
                        out_ref[place, :] + same + pltpu.roll(above, 1, 0) + pltpu.roll(below, levels - 1, 0)
                    )

    def fix_n(turn):
        parts = [(0, ends[-2], to_ss[0].wait_recv), (ends[-2], tracers, to_ss[1].wait_recv)]
        fix_rows(from_n, rows - 1, rows - 2, True, turn, parts)

    with jax.named_scope("fixs"):

        @pl.when(inner)
        def _():
            to_n.wait_recv()

        fix_rows(from_s, 0, 1, False, False, [(0, tracers, lambda: None)])

    with jax.named_scope("fixn"):

        @pl.when(below_top)
        def _():
            fix_n(False)

    spot = tracer_of(lane, lanes, tracers)

    def part_of(refs, offs, n, first=None):
        at = jnp.clip(spot - splits[n], 0, splits[n + 1] - splits[n] - 1)
        return values_of(refs, offs, at, pers[n], slots[n], firsts[n] if first is None else first, levels)

    def column_of(refs, offs):
        fixed = jnp.zeros((rows, lanes), jnp.int32)
        rho = jnp.stack([both(refs, offs, fixed + (where_is(0, k)[0] + split), where_is(0, k)[1])
                         for k in range(levels)])
        kmt = both(refs, offs, fixed + kmt_at, 0)
        wet = jnp.stack([(kmt > float(k)).astype(jnp.float32) for k in range(levels)])
        return column(rho, wet, up3, dn3)

    def joined(*args):
        a, b, c = (part_of(*args, n) for n in range(3))
        return jnp.stack([
            jnp.where(spot < splits[1], a[k], jnp.where(spot < splits[2], b[k], c[k])) for k in range(levels)
        ])

    with jax.named_scope("fixc0"):
        own_at, ins_at, outs_at = ((wcol, ecol), (1, 0)), ((inner_w, inner_e), (2, -1)), ((wests[0], easts[0]), (0, 1))
        own_c, ins_c = column_of(*own_at), column_of(*ins_at)
        own, ins = joined(*own_at), joined(*ins_at)
    with jax.named_scope("waitc"):
        got[0].wait_recv()
    with jax.named_scope("fixc1"):
        own_t, outs_t, ins_t = line(own_c, column_of(*outs_at), ins_c, up3, dn3)
        some = applied(own_t, own) + applied(ins_t, ins)
        full = some + applied(outs_t, part_of(*outs_at, 0))
    with jax.named_scope("waitc1"):
        got[1].wait_recv()
    with jax.named_scope("insert0"):
        more = some + applied(outs_t, part_of((wests[1], easts[1]), (0, 1), 1, 0))
        insert_tiles(range(split), full, out_ref, out_ref)
        for k in range(levels):
            add_ref[pl.ds(k * rows, rows), :] = more[k]
            add_ref[pl.ds((levels + k) * rows, rows), :] = some[k]
            for dk in range(3):
                tab_ref[pl.ds((dk * levels + k) * rows, rows), :] = outs_t[dk][k]

    with jax.named_scope("fixtop"):

        @pl.when(at_top)
        def _():
            fix_n(True)

    with jax.named_scope("end"):
        fold.wait_send()

        @pl.when(inner)
        def _():
            to_s.wait_send()

        all_e.wait_send()
        all_w.wait_send()

        @pl.when(relays)
        def _():
            all_onward.wait_send()

    with jax.named_scope("waitc2"):
        got[2].wait_recv()


def finish(sizes, part_ref, add_ref, tab_ref, halo_ref, out_ref, stage, sem):
    tracers, levels, rows, lanes, splits = sizes
    plane = levels * rows
    slots, pers, shares = layout(splits, levels, lanes)
    lane = lax.broadcasted_iota(jnp.int32, (rows, lanes), 1)
    spot = tracer_of(lane, lanes, tracers)
    half = shares[2] * rows

    def write(ref, first, count):
        span = pl.ds(pl.multiple_of(first * plane, plane), count * plane)
        pltpu.make_async_copy(ref.at[span], out_ref.at[span], sem).start()

    def eight(ref, n):
        return jnp.stack([ref[pl.ds((n * levels + k) * rows, rows), :] for k in range(levels)])

    def last_terms():
        refs = [halo_ref.at[pl.ds(i * half, half)] for i in range(2)]
        at = jnp.clip(spot - splits[2], 0, splits[3] - splits[2] - 1)
        values = values_of(refs, (0, 1), at, pers[2], slots[2], 0, levels)
        return eight(add_ref, 1) + applied([eight(tab_ref, dk) for dk in range(3)], values)

    with jax.named_scope("insert"):
        ready = splits[1] // 2

        @pl.loop(0, 2)
        def _(i):
            write(part_ref, i * ready, ready)

        terms = [eight(add_ref, 0), None]
        for n in (1, 2):
            for t in range(splits[n], splits[n + 1], STORE):
                last = min(t + STORE, splits[n + 1])
                insert_tiles(range(t, last), terms[n - 1], part_ref, stage)
                write(stage, t, last - t)
                if terms[1] is None:
                    terms[1] = last_terms()
    with jax.named_scope("written"):
        pltpu.make_async_copy(stage, out_ref, sem).wait()


def solution(mesh):
    n_lon, n_lat = mesh.shape["lon"], mesh.shape["lat"]

    def local(tracers, kmt):
        nt, levels, rows, lanes = tracers.shape
        tiles = nt * levels
        most = (lanes - 2) // levels
        split = max(nt - most, nt // 2)
        cuts = (0, split // 6, min(split // 2, max(most - 2, 2)), split, nt)
        splits = (0, *cuts[2:])
        groups = tuple(b - a for a, b in zip(cuts, cuts[1:]))
        shares = layout(splits, levels, lanes)[-1]
        regs = sum(shares)
        assert levels == rows and groups[0] > 1 and cuts[2] % 2 == 0 and lanes & (lanes - 1) == 0

        def vmem(*shape):
            return pltpu.VMEM(shape, jnp.float32)

        parts = pl.pallas_call(
            functools.partial(kernel, (nt, levels, rows, lanes, n_lon, n_lat, groups)),
            out_shape=[
                vmem(tiles * rows, lanes),
                vmem(2 * levels * rows, lanes),
                vmem(3 * levels * rows, lanes),
                vmem(2 * shares[2] * rows, lanes),
            ],
            in_specs=[pl.BlockSpec(memory_space=pltpu.HBM), pl.BlockSpec(memory_space=pltpu.HBM)],
            out_specs=[pl.BlockSpec(memory_space=pltpu.VMEM)] * 4,
            scratch_shapes=[
                vmem(tiles + levels, rows, lanes),
                pltpu.VMEM((rows, lanes), jnp.int32),
                vmem(15 * levels * rows, lanes),
            ]
            + [vmem(regs * rows, lanes)] * 5
            + [vmem(2 * n * rows, lanes) for n in shares[:2]]
            + [vmem(tiles + rows, lanes)] * 2
            + [
                pltpu.SemaphoreType.DMA((7,)),
            ],
            compiler_params=pltpu.CompilerParams(collective_id=0, has_side_effects=True),
        )(tracers.reshape(tiles, rows, lanes), kmt)
        parts = [pltpu.with_memory_space_constraint(v, pltpu.VMEM) for v in parts]
        out = pl.pallas_call(
            functools.partial(finish, (nt, levels, rows, lanes, splits)),
            out_shape=jax.ShapeDtypeStruct((tiles * rows, lanes), jnp.float32),
            in_specs=[pl.BlockSpec(memory_space=pltpu.VMEM)] * 4,
            out_specs=pl.BlockSpec(memory_space=pltpu.HBM),
            scratch_shapes=[vmem(tiles * rows, lanes), pltpu.SemaphoreType.DMA],
        )(*parts)
        return out.reshape(nt, levels, rows, lanes)

    return jax.shard_map(
        local,
        mesh=mesh,
        in_specs=(P(None, None, "lat", "lon"), P("lat", "lon")),
        out_specs=P(None, None, "lat", "lon"),
        check_vma=False,
    )
```

```python
import functools

import jax
import jax.numpy as jnp
from jax import lax
from jax.experimental import pallas as pl
from jax.experimental.pallas import tpu as pltpu
from jax.sharding import PartitionSpec as P

THERMAL = 0.2
HALINE = 0.8
REDI = 0.1
SKEW = 0.05
SLOPE_MAX = 0.6
SLOPE_WIDTH = 0.2

MESH = pl.DeviceIdType.MESH
TOGETHER = 2
STORE = 2
C, E, W, N, S = range(5)


def taper(slope):
    return slope * 0.5 * (1.0 + jnp.tanh((SLOPE_MAX - jnp.abs(slope)) / SLOPE_WIDTH))


def column(rho, wet, up, dn):
    hi = wet * dn(wet)
    strat = (dn(rho) - rho) * hi
    return rho, wet, hi, up(hi), 0.5 * (strat + up(strat))


def line(c, p, m, up, dn):
    c_rho, c_wet, c_hi, c_lo, c_cell = c
    p_rho, p_wet, p_hi, p_lo, p_cell = p
    m_rho, m_wet, m_hi, m_lo, m_cell = m
    mp, mm = c_wet * p_wet, c_wet * m_wet
    sp = taper((p_rho - c_rho) * mp / jnp.maximum(0.5 * (p_cell + c_cell), 1.0))
    sm = taper((c_rho - m_rho) * mm / jnp.maximum(0.5 * (m_cell + c_cell), 1.0))
    cx = 0.5 * (sp + sm)
    sw = 0.5 * (cx + dn(cx))
    fh = ((REDI + SKEW) * 0.25) * sw * c_hi
    zh = REDI * (sw * sw) * c_hi
    fl, zl = up(fh), up(zh)
    pp = ((REDI - SKEW) * 0.25) * sp * mp
    pm = -((REDI - SKEW) * 0.25) * sm * mm
    own_p, own_m = mp * (fh - fl), mm * (fl - fh)
    mph, mmh = dn(mp) * fh, dn(mm) * fh
    mpl, mml = up(mp) * fl, up(mm) * fl
    q = pp + pm
    return (
        (mpl - mml - q * c_lo + zl,
         q * (c_lo - c_hi) - REDI * (mp + mm) - (own_p + own_m) - (zh + zl),
         mmh - mph + q * c_hi + zh),
        (-pp * p_lo - mpl, REDI * mp + pp * (p_lo - p_hi) + own_p, pp * p_hi + mph),
        (mml - pm * m_lo, REDI * mm + pm * (m_lo - m_hi) + own_m, pm * m_hi - mmh),
    )


def total(terms):
    result = terms[0]
    for term in terms[1:]:
        result = result + term
    return result


def pick(value, index):
    return jnp.take_along_axis(value, index, axis=1)


def up3(v):
    return jnp.concatenate([jnp.zeros_like(v[:1]), v[:-1]], axis=0)


def dn3(v):
    return jnp.concatenate([v[1:], jnp.zeros_like(v[:1])], axis=0)


def applied(c, v):
    return c[1] * v + c[0] * up3(v) + c[2] * dn3(v)


def layout(splits, levels, lanes):
    slots = tuple(b - a + (2 if a == 0 else 0) for a, b in zip(splits, splits[1:]))
    pers = tuple((lanes - 2) // slot for slot in slots)
    return slots, pers, tuple((levels + per - 1) // per for per in pers)


def tracer_of(lane, lanes, tracers):
    return jnp.minimum(lax.shift_right_logical(lane + 1, 1) & (lanes // 2 - 1), tracers - 1)


def both(refs, offs, at, reg):
    rows, lanes = at.shape
    span = pl.ds(reg * rows, rows)
    west_side = lax.broadcasted_iota(jnp.int32, at.shape, 1) & 1 == 0
    wraps = any(off not in (0, 1) for off in offs)
    index = [at + off & (lanes - 1) if wraps else at + off for off in offs]
    picked = [pick(ref[span, :], i) for ref, i in zip(refs, index)]
    return jnp.where(west_side, *picked)


def values_of(refs, offs, spot, per, slot, first, levels):
    return jnp.stack([both(refs, offs, k % per * slot + spot, first + k // per) for k in range(levels)])


def insert_tiles(which, terms, src, dst):
    levels, rows, lanes = terms.shape
    lane = lax.broadcasted_iota(jnp.int32, (rows, lanes), 1)
    sides = jnp.logical_or(lane == 0, lane == lanes - 1)
    for t in which:
        for k in range(levels):
            term = pltpu.roll(terms[k], (lanes - 2 * t) % lanes, 1)
            place = pl.ds((t * levels + k) * rows, rows)
            dst[place, :] = src[place, :] + jnp.where(sides, term, 0.0)


def kernel(sizes, x_ref, kmt_ref, out_ref, add_ref, tab_ref, halo2, *scratch):
    pl.run_scoped(
        functools.partial(body, sizes, x_ref, kmt_ref, out_ref, add_ref, tab_ref, halo2, *scratch),
        pltpu.SemaphoreType.DMA((len(sizes[-1]) + 1,)),
        pltpu.SemaphoreType.DMA((5,)),
    )


def body(
    sizes, x_ref, kmt_ref, out_ref, add_ref, tab_ref, halo2,
    xv, kmt_int, coef, wcol, ecol, inner_w, inner_e, relay, halo0, halo1, from_n, from_s,
    recv_sem, load_sem, send_sem,
):
    tracers, levels, rows, lanes, n_lon, n_lat, groups = sizes
    lon, lat = lax.axis_index("lon"), lax.axis_index("lat")
    at_top = lat == n_lat - 1
    below_top = jnp.logical_not(at_top)
    inner = lat > 0
    at_bottom = jnp.logical_not(inner)
    even_lat = jnp.logical_and(inner, jnp.logical_and(lat % 2 == 0, below_top))
    odd_lat = jnp.logical_and(lat > 1, lat % 2 == 1)
    relayed = jnp.logical_and(lon == 0, even_lat)
    relays = jnp.logical_and(lon == 0, odd_lat)
    far = jnp.logical_and(lon == n_lon - 1, even_lat)
    direct, near = jnp.logical_not(relayed), jnp.logical_not(far)
    early = jnp.logical_and(lon == 0, direct)
    late = jnp.logical_not(early)
    late_top, late_below = jnp.logical_and(late, at_top), jnp.logical_and(late, below_top)
    urgent = jnp.logical_and(jnp.logical_and(late_below, lon == n_lon - 1), lat % 2 == 0)
    patient = jnp.logical_and(late_below, jnp.logical_not(urgent))
    e_dev = (lax.rem(lon + 1, n_lon), lat)
    w_dev = (lax.rem(lon + n_lon - 1, n_lon), lat)
    n_dev, s_dev = (lon, lat + 1), (lon, lat - 1)
    lat_up, lat_down = lax.rem(lat + 1, n_lat), lax.rem(lat + n_lat - 1, n_lat)
    fold_dev = (n_lon - 1 - lon, lat)
    tiles = tracers * levels
    plane = levels * rows
    lead = levels
    ends = [sum(groups[:i]) for i in range(len(groups) + 1)]
    splits = (0, *ends[2:])
    split = splits[1]
    slots, pers, shares = layout(splits, levels, lanes)
    firsts = [sum(shares[:n]) for n in range(3)]
    kmt_at = pers[0] * slots[0]

    load_kmt = pltpu.make_async_copy(kmt_ref, kmt_int, load_sem.at[len(groups)])
    load_kmt.start()

    def load(first, count, i):
        return pltpu.make_async_copy(
            x_ref.at[pl.ds(first, count)], xv.at[pl.ds(lead + first, count)], load_sem.at[i]
        )

    for i in range(len(groups)):
        for t in range(ends[i], ends[i + 1]):
            load(t * levels, levels, i).start()
    loads = [load(ends[i] * levels, groups[i] * levels, i) for i in range(len(groups))]
    flat = xv.reshape((lead + tiles) * rows, lanes)

    barrier = pltpu.get_barrier_semaphore()

    def greet(dev):
        pl.semaphore_signal(barrier, inc=1, device_id=dev, device_id_type=MESH)

    with jax.named_scope("greet"):
        greet(w_dev)

        @pl.when(near)
        def _():
            greet(e_dev)

        @pl.when(far)
        def _():
            greet((0, lat_up))

        @pl.when(at_top)
        def _():
            greet(fold_dev)

        @pl.when(below_top)
        def _():
            greet(n_dev)

        @pl.when(inner)
        def _():
            greet(s_dev)

    lane = lax.broadcasted_iota(jnp.int32, (rows, lanes), 1)
    row = lax.broadcasted_iota(jnp.int32, (rows, lanes), 0)

    def send(src, dst, s, r, dev):
        return pltpu.make_async_remote_copy(
            src_ref=src, dst_ref=dst, send_sem=send_sem.at[s], recv_sem=recv_sem.at[r],
            device_id=dev, device_id_type=MESH,
        )

    def rows_of(r, span, dst, s, into, dev):
        return send(xv.at[span, r, :], dst.at[span], s, into, dev)

    starts = [lead - 1] + [lead + e * levels for e in ends[1:]]
    spans = [pl.ds(a, b - a) for a, b in zip(starts, starts[1:])]
    every = pl.ds(lead - 1, tiles + 1)
    fold = rows_of(rows - 1, every, from_n, 0, 0, fold_dev)
    folds = [
        rows_of(rows - 1, span, from_n, 0, 0, fold_dev)
        for span in spans
    ]
    to_n = rows_of(rows - 1, every, from_s, 0, 1, n_dev)
    to_s = rows_of(0, every, from_n, 1, 0, s_dev)
    cols = [pl.ds(f * rows, n * rows) for f, n in zip(firsts, shares)]
    halos = (halo0, halo1, halo2)
    wests = [h.at[pl.ds(0, n * rows)] for h, n in zip(halos, shares)]
    easts = [h.at[pl.ds(n * rows, n * rows)] for h, n in zip(halos, shares)]
    arrive = (2, 3, 5)
    far_dev = (n_lon - 1, lat_down)
    to_e = [send(ecol.at[c], wests[i], 2, arrive[i], e_dev) for i, c in enumerate(cols)]
    to_w = [send(wcol.at[c], easts[i], 3, arrive[i], w_dev) for i, c in enumerate(cols)]
    onward = [send(relay.at[c], easts[i], 4, arrive[i], far_dev) for i, c in enumerate(cols)]
    to_relay = send(wcol, relay, 3, 4, (lon, lat_up))
    got = [send(h, h, 2, r, e_dev) for h, r in zip(halos, arrive)]
    all_e, all_w, all_onward = (send(c, relay, s, 4, e_dev) for c, s in ((ecol, 2), (wcol, 3), (relay, 4)))

    def tile(t, k):
        return flat[pl.ds(lead * rows + t * plane + k * rows, rows), :]

    def density(k):
        return HALINE * tile(1, k) - THERMAL * tile(0, k)

    def where_is(t, k):
        n = sum(t >= s for s in splits[1:])
        return k % pers[n] * slots[n] + t - splits[n], firsts[n] + k // pers[n]

    def gather_columns(e_ref, w_ref, e_off, w_off, before=None, after=None):
        zeros = jnp.zeros((rows, lanes), jnp.float32)
        es, ws = [zeros] * sum(shares), [zeros] * sum(shares)

        def place(value, at, reg):
            value = pltpu.roll(value, at + 1, 1)
            es[reg] = jnp.where(lane == (at + e_off) % lanes, value, es[reg])
            ws[reg] = jnp.where(lane == (at + w_off) % lanes, value, ws[reg])

        for i in range(len(groups)):
            if before is not None:
                before(i)
            if i == 0:
                place(kmt_own, kmt_at, 0)
                for k in range(levels):
                    at, reg = where_is(0, k)
                    place(density(k), at + split, reg)
            for t in range(ends[i], ends[i + 1]):
                for k in range(levels):
                    place(tile(t, k), *where_is(t, k))
            if ends[i + 1] in splits:
                n = splits.index(ends[i + 1]) - 1
                for j in range(firsts[n], firsts[n] + shares[n]):
                    e_ref[pl.ds(j * rows, rows), :] = es[j]
                    w_ref[pl.ds(j * rows, rows), :] = ws[j]
                if after is not None:
                    after(n)

    def enter():
        @pl.when(at_bottom)
        def _():
            pl.semaphore_wait(barrier, 3)

        @pl.when(jnp.logical_and(inner, jnp.logical_not(jnp.logical_or(relayed, relays))))
        def _():
            pl.semaphore_wait(barrier, 4)

        @pl.when(relayed)
        def _():
            pl.semaphore_wait(barrier, 3)

        @pl.when(relays)
        def _():
            pl.semaphore_wait(barrier, 5)

    def send_inner_rows():
        @pl.when(below_top)
        def _():
            to_n.start()

        @pl.when(inner)
        def _():
            to_s.start()

    def before(i):
        with jax.named_scope(f"load{i}"):
            loads[i].wait()
        if i == 0:

            @pl.when(late_top)
            def _():
                enter()

        if i < len(groups) - 1:

            @pl.when(late_top)
            def _():
                folds[i].start()

    def send_part(n, who):
        @pl.when(who)
        def _():
            to_e[n].start()

        @pl.when(jnp.logical_and(who, direct))
        def _():
            to_w[n].start()

    def after(n):
        if n < 2:

            @pl.when(patient if n else urgent)
            def _():
                with jax.named_scope("barrier"):
                    enter()

        if n == 1:
            send_part(0, patient)
        send_part(n, late if n else jnp.logical_and(late, jnp.logical_not(patient)))

    with jax.named_scope("loadk"):
        load_kmt.wait()
    kmt_own = kmt_int[...].astype(jnp.float32)
    xv[lead - 1, :, :] = kmt_own
    gather_columns(ecol, wcol, 0, 1, before, after)
    with jax.named_scope("send"):

        @pl.when(relayed)
        def _():
            to_relay.start()

        @pl.when(late_top)
        def _():
            folds[-1].start()

        @pl.when(late)
        def _():
            send_inner_rows()

    with jax.named_scope("inner"):
        gather_columns(inner_e, inner_w, -1, 2)

        @pl.when(at_bottom)
        def _():
            for t in range(tracers + 1):
                from_s[pl.ds(t * levels, levels), :] = jnp.zeros((levels, lanes), jnp.float32)

    def put(d, dk, k, value):
        coef[pl.ds(((d * 3 + dk) * levels + k) * rows, rows), :] = value

    def piece_of(d, dk, k):
        return coef[pl.ds(((d * 3 + dk) * levels + k) * rows, rows), :]

    with jax.named_scope("coefs"):
        def shifted(v, by, axis):
            return jnp.stack([pltpu.roll(v[k], by, axis) for k in range(levels)])

        own_rho = jnp.stack([density(k) for k in range(levels)])
        own_wet = jnp.stack([(kmt_own > float(k)).astype(jnp.float32) for k in range(levels)])
        c3 = column(own_rho, own_wet, up3, dn3)

        def moved(by, axis):
            return tuple(shifted(v, by, axis) for v in c3)

        mid_lane = jnp.logical_and(lane > 0, lane < lanes - 1)
        xc, xe, xw = line(c3, moved(lanes - 1, 1), moved(1, 1), up3, dn3)
        for dk in range(3):
            for k in range(levels):
                put(E, dk, k, jnp.where(mid_lane, xe[dk][k], 0.0))
                put(W, dk, k, jnp.where(mid_lane, xw[dk][k], 0.0))
                put(C, dk, k, jnp.where(mid_lane, xc[dk][k], 0.0))
        mid_row = jnp.logical_and(row > 0, row < rows - 1)
        yc, yn, ys = line(c3, moved(rows - 1, 0), moved(1, 0), up3, dn3)
        for dk in range(3):
            for k in range(levels):
                put(N, dk, k, jnp.where(mid_row, yn[dk][k], 0.0))
                put(S, dk, k, jnp.where(mid_row, ys[dk][k], 0.0))
                core = piece_of(C, dk, k) + jnp.where(mid_row, yc[dk][k], 0.0)
                put(C, dk, k, core + 1.0 if dk == 1 else core)

    with jax.named_scope("main"):

        @pl.loop(0, tracers // TOGETHER)
        def _(i):
            fields = []
            for u in range(TOGETHER):
                base = pl.multiple_of(lead * rows + (i * TOGETHER + u) * plane, rows)
                field = []
                for k in range(levels):
                    own = flat[pl.ds(base + k * rows, rows), :]
                    field.append((
                        own, pltpu.roll(own, lanes - 1, 1), pltpu.roll(own, 1, 1),
                        pltpu.roll(own, rows - 1, 0), pltpu.roll(own, 1, 0),
                    ))
                fields.append(field)
            for k in range(levels):
                sums = [None] * TOGETHER
                for d in range(5):
                    for dk in range(3):
                        if not 0 <= k + dk - 1 < levels:
                            continue
                        c = piece_of(d, dk, k)
                        for u in range(TOGETHER):
                            term = c * fields[u][k + dk - 1][d]
                            sums[u] = term if sums[u] is None else sums[u] + term
                for u in range(TOGETHER):
                    base = pl.multiple_of((i * TOGETHER + u) * plane, rows)
                    out_ref[pl.ds(base + k * rows, rows), :] = sums[u]

    @pl.when(early)
    def _():
        with jax.named_scope("barrier"):
            enter()
        for copy in to_e + to_w:
            copy.start()
        send_inner_rows()

        @pl.when(at_top)
        def _():
            for copy in folds:
                copy.start()

    @pl.when(relays)
    def _():
        to_relay.wait_recv()
        for copy in onward:
            copy.start()

    level = lax.broadcasted_iota(jnp.int32, (levels, lanes), 0)
    level_f = level.astype(jnp.float32)

    def up_s(v):
        return jnp.where(level == 0, 0.0, pltpu.roll(v, 1, 0))

    def dn_s(v):
        return jnp.where(level == levels - 1, 0.0, pltpu.roll(v, levels - 1, 0))

    def at_row(t, r):
        return flat[pl.ds(lead * rows + t * plane + r, levels, stride=rows), :]

    def row_column(t0, t1, kmt):
        wet = (jnp.broadcast_to(kmt, (levels, lanes)) > level_f).astype(jnp.float32)
        return column(HALINE * t1 - THERMAL * t0, wet, up_s, dn_s)

    def own_row(r):
        return row_column(at_row(0, r), at_row(1, r), kmt_own[r : r + 1, :])

    def fix_rows(source, r, r_in, north, turn, parts):
        def halo(t):
            h = source[pl.ds(lead + t * levels, levels), :]
            return pick(h, lanes - 1 - lane) if turn else h

        first, last, wait = parts[0]
        wait()
        k = jnp.broadcast_to(source[pl.ds(lead - 1, 1), :], (rows, lanes))
        k = (pick(k, lanes - 1 - lane) if turn else k)[:1, :]
        out_c, in_c = row_column(halo(0), halo(1), k), own_row(r_in)
        p, m = (out_c, in_c) if north else (in_c, out_c)
        cc, cp, cm = line(own_row(r), p, m, up_s, dn_s)
        c_out, c_in = (cp, cm) if north else (cm, cp)
        table = (cc, c_out, c_in)
        lo = [pltpu.roll(c[0], levels - 1, 0) for c in table]
        mid = [c[1] for c in table]
        hi = [pltpu.roll(c[2], 1, 0) for c in table]
        for n, (first, last, wait) in enumerate(parts):
            if n:
                wait()
            count = last - first
            batch = next(b for b in (20, 10, 8, 5, 4, 3, 2, 1) if count % b == 0 and (turn or b <= 8))

            @pl.loop(0, count // batch)
            def _(i, first=first, batch=batch):
                for u in range(batch):
                    t = first + i * batch + u
                    values = (at_row(t, r), halo(t), at_row(t, r_in))
                    above = total([c * v for c, v in zip(lo, values)])
                    same = total([c * v for c, v in zip(mid, values)])
                    below = total([c * v for c, v in zip(hi, values)])
                    place = pl.ds(t * plane + r, levels, stride=rows)
                    out_ref[place, :] = (
                        out_ref[place, :] + same + pltpu.roll(above, 1, 0) + pltpu.roll(below, levels - 1, 0)
                    )

    def fix_n(turn):
        fix_rows(from_n, rows - 1, rows - 2, True, turn, [(0, tracers, to_s.wait_recv)])

    with jax.named_scope("fixs"):

        @pl.when(inner)
        def _():
            to_n.wait_recv()

        fix_rows(from_s, 0, 1, False, False, [(0, tracers, lambda: None)])

    with jax.named_scope("fixn"):

        @pl.when(below_top)
        def _():
            fix_n(False)

    spot = tracer_of(lane, lanes, tracers)

    def part_of(refs, offs, n, first=None):
        at = jnp.clip(spot - splits[n], 0, splits[n + 1] - splits[n] - 1)
        return values_of(refs, offs, at, pers[n], slots[n], firsts[n] if first is None else first, levels)

    def column_of(refs, offs):
        fixed = jnp.zeros((rows, lanes), jnp.int32)
        rho = jnp.stack([both(refs, offs, fixed + (where_is(0, k)[0] + split), where_is(0, k)[1])
                         for k in range(levels)])
        kmt = both(refs, offs, fixed + kmt_at, 0)
        wet = jnp.stack([(kmt > float(k)).astype(jnp.float32) for k in range(levels)])
        return column(rho, wet, up3, dn3)

    def joined(*args):
        a, b, c = (part_of(*args, n) for n in range(3))
        return jnp.stack([
            jnp.where(spot < splits[1], a[k], jnp.where(spot < splits[2], b[k], c[k])) for k in range(levels)
        ])

    with jax.named_scope("fixc0"):
        own_at, ins_at, outs_at = ((wcol, ecol), (1, 0)), ((inner_w, inner_e), (2, -1)), ((wests[0], easts[0]), (0, 1))
        own_c, ins_c = column_of(*own_at), column_of(*ins_at)
        own, ins = joined(*own_at), joined(*ins_at)
    with jax.named_scope("waitc"):
        got[0].wait_recv()
    with jax.named_scope("fixc1"):
        own_t, outs_t, ins_t = line(own_c, column_of(*outs_at), ins_c, up3, dn3)
        some = applied(own_t, own) + applied(ins_t, ins)
        full = some + applied(outs_t, part_of(*outs_at, 0))
    with jax.named_scope("waitc1"):
        got[1].wait_recv()
    with jax.named_scope("insert0"):
        more = some + applied(outs_t, part_of((wests[1], easts[1]), (0, 1), 1, 0))
        insert_tiles(range(split), full, out_ref, out_ref)
        for k in range(levels):
            add_ref[pl.ds(k * rows, rows), :] = more[k]
            add_ref[pl.ds((levels + k) * rows, rows), :] = some[k]
            for dk in range(3):
                tab_ref[pl.ds((dk * levels + k) * rows, rows), :] = outs_t[dk][k]

    with jax.named_scope("fixtop"):

        @pl.when(at_top)
        def _():
            fix_n(True)

    with jax.named_scope("end"):
        fold.wait_send()

        @pl.when(inner)
        def _():
            to_s.wait_send()

        all_e.wait_send()
        all_w.wait_send()

        @pl.when(relays)
        def _():
            all_onward.wait_send()

    with jax.named_scope("waitc2"):
        got[2].wait_recv()


def finish(sizes, part_ref, add_ref, tab_ref, halo_ref, out_ref, stage, sem):
    tracers, levels, rows, lanes, splits = sizes
    plane = levels * rows
    slots, pers, shares = layout(splits, levels, lanes)
    lane = lax.broadcasted_iota(jnp.int32, (rows, lanes), 1)
    spot = tracer_of(lane, lanes, tracers)
    half = shares[2] * rows

    def write(ref, first, count):
        span = pl.ds(pl.multiple_of(first * plane, plane), count * plane)
        pltpu.make_async_copy(ref.at[span], out_ref.at[span], sem).start()

    def eight(ref, n):
        return jnp.stack([ref[pl.ds((n * levels + k) * rows, rows), :] for k in range(levels)])

    def last_terms():
        refs = [halo_ref.at[pl.ds(i * half, half)] for i in range(2)]
        at = jnp.clip(spot - splits[2], 0, splits[3] - splits[2] - 1)
        values = values_of(refs, (0, 1), at, pers[2], slots[2], 0, levels)
        return eight(add_ref, 1) + applied([eight(tab_ref, dk) for dk in range(3)], values)

    with jax.named_scope("insert"):
        ready = splits[1] // 2

        @pl.loop(0, 2)
        def _(i):
            write(part_ref, i * ready, ready)

        terms = [eight(add_ref, 0), None]
        for n in (1, 2):
            for t in range(splits[n], splits[n + 1], STORE):
                last = min(t + STORE, splits[n + 1])
                insert_tiles(range(t, last), terms[n - 1], part_ref, stage)
                write(stage, t, last - t)
                if terms[1] is None:
                    terms[1] = last_terms()
    with jax.named_scope("written"):
        pltpu.make_async_copy(stage, out_ref, sem).wait()


def solution(mesh):
    n_lon, n_lat = mesh.shape["lon"], mesh.shape["lat"]

    def local(tracers, kmt):
        nt, levels, rows, lanes = tracers.shape
        tiles = nt * levels
        most = (lanes - 2) // levels
        split = max(nt - most, nt // 2)
        cuts = (0, split // 6, min(split // 2, max(most - 2, 2)), split, nt)
        splits = (0, *cuts[2:])
        groups = tuple(b - a for a, b in zip(cuts, cuts[1:]))
        shares = layout(splits, levels, lanes)[-1]
        regs = sum(shares)
        assert levels == rows and groups[0] > 1 and cuts[2] % 2 == 0 and lanes & (lanes - 1) == 0

        def vmem(*shape):
            return pltpu.VMEM(shape, jnp.float32)

        parts = pl.pallas_call(
            functools.partial(kernel, (nt, levels, rows, lanes, n_lon, n_lat, groups)),
            out_shape=[
                vmem(tiles * rows, lanes),
                vmem(2 * levels * rows, lanes),
                vmem(3 * levels * rows, lanes),
                vmem(2 * shares[2] * rows, lanes),
            ],
            in_specs=[pl.BlockSpec(memory_space=pltpu.HBM), pl.BlockSpec(memory_space=pltpu.HBM)],
            out_specs=[pl.BlockSpec(memory_space=pltpu.VMEM)] * 4,
            scratch_shapes=[
                vmem(tiles + levels, rows, lanes),
                pltpu.VMEM((rows, lanes), jnp.int32),
                vmem(15 * levels * rows, lanes),
            ]
            + [vmem(regs * rows, lanes)] * 5
            + [vmem(2 * n * rows, lanes) for n in shares[:2]]
            + [vmem(tiles + rows, lanes)] * 2
            + [
                pltpu.SemaphoreType.DMA((6,)),
            ],
            compiler_params=pltpu.CompilerParams(collective_id=0, has_side_effects=True),
        )(tracers.reshape(tiles, rows, lanes), kmt)
        parts = [pltpu.with_memory_space_constraint(v, pltpu.VMEM) for v in parts]
        out = pl.pallas_call(
            functools.partial(finish, (nt, levels, rows, lanes, splits)),
            out_shape=jax.ShapeDtypeStruct((tiles * rows, lanes), jnp.float32),
            in_specs=[pl.BlockSpec(memory_space=pltpu.VMEM)] * 4,
            out_specs=pl.BlockSpec(memory_space=pltpu.HBM),
            scratch_shapes=[vmem(tiles * rows, lanes), pltpu.SemaphoreType.DMA],
        )(*parts)
        return out.reshape(nt, levels, rows, lanes)

    return jax.shard_map(
        local,
        mesh=mesh,
        in_specs=(P(None, None, "lat", "lon"), P("lat", "lon")),
        out_specs=P(None, None, "lat", "lon"),
        check_vma=False,
    )
```

```python
import functools

import jax
import jax.numpy as jnp
from jax import lax
from jax.experimental import pallas as pl
from jax.experimental.pallas import tpu as pltpu
from jax.sharding import PartitionSpec as P

THERMAL = 0.2
HALINE = 0.8
REDI = 0.1
SKEW = 0.05
SLOPE_MAX = 0.6
SLOPE_WIDTH = 0.2

MESH = pl.DeviceIdType.MESH
TOGETHER = 2
STORE = 4
C, E, W, N, S = range(5)


def taper(slope):
    return slope * 0.5 * (1.0 + jnp.tanh((SLOPE_MAX - jnp.abs(slope)) / SLOPE_WIDTH))


def column(rho, wet, up, dn):
    hi = wet * dn(wet)
    strat = (dn(rho) - rho) * hi
    return rho, wet, hi, up(hi), 0.5 * (strat + up(strat))


def line(c, p, m, up, dn):
    c_rho, c_wet, c_hi, c_lo, c_cell = c
    p_rho, p_wet, p_hi, p_lo, p_cell = p
    m_rho, m_wet, m_hi, m_lo, m_cell = m
    mp, mm = c_wet * p_wet, c_wet * m_wet
    sp = taper((p_rho - c_rho) * mp / jnp.maximum(0.5 * (p_cell + c_cell), 1.0))
    sm = taper((c_rho - m_rho) * mm / jnp.maximum(0.5 * (m_cell + c_cell), 1.0))
    cx = 0.5 * (sp + sm)
    sw = 0.5 * (cx + dn(cx))
    fh = ((REDI + SKEW) * 0.25) * sw * c_hi
    zh = REDI * (sw * sw) * c_hi
    fl, zl = up(fh), up(zh)
    pp = ((REDI - SKEW) * 0.25) * sp * mp
    pm = -((REDI - SKEW) * 0.25) * sm * mm
    own_p, own_m = mp * (fh - fl), mm * (fl - fh)
    mph, mmh = dn(mp) * fh, dn(mm) * fh
    mpl, mml = up(mp) * fl, up(mm) * fl
    q = pp + pm
    return (
        (mpl - mml - q * c_lo + zl,
         q * (c_lo - c_hi) - REDI * (mp + mm) - (own_p + own_m) - (zh + zl),
         mmh - mph + q * c_hi + zh),
        (-pp * p_lo - mpl, REDI * mp + pp * (p_lo - p_hi) + own_p, pp * p_hi + mph),
        (mml - pm * m_lo, REDI * mm + pm * (m_lo - m_hi) + own_m, pm * m_hi - mmh),
    )


def total(terms):
    result = terms[0]
    for term in terms[1:]:
        result = result + term
    return result


def pick(value, index):
    return jnp.take_along_axis(value, index, axis=1)


def up3(v):
    return jnp.concatenate([jnp.zeros_like(v[:1]), v[:-1]], axis=0)


def dn3(v):
    return jnp.concatenate([v[1:], jnp.zeros_like(v[:1])], axis=0)


def applied(c, v):
    return c[1] * v + c[0] * up3(v) + c[2] * dn3(v)


def layout(splits, levels, lanes):
    slots = tuple(b - a + (2 if a == 0 else 0) for a, b in zip(splits, splits[1:]))
    pers = tuple((lanes - 2) // slot for slot in slots)
    return slots, pers, tuple((levels + per - 1) // per for per in pers)


def tracer_of(lane, lanes, tracers):
    return jnp.minimum(lax.shift_right_logical(lane + 1, 1) & (lanes // 2 - 1), tracers - 1)


def both(refs, offs, at, reg):
    rows, lanes = at.shape
    span = pl.ds(reg * rows, rows)
    west_side = lax.broadcasted_iota(jnp.int32, at.shape, 1) & 1 == 0
    wraps = any(off not in (0, 1) for off in offs)
    index = [at + off & (lanes - 1) if wraps else at + off for off in offs]
    picked = [pick(ref[span, :], i) for ref, i in zip(refs, index)]
    return jnp.where(west_side, *picked)


def values_of(refs, offs, spot, per, slot, first, levels):
    return jnp.stack([both(refs, offs, k % per * slot + spot, first + k // per) for k in range(levels)])


def insert_tiles(which, terms, src, dst):
    levels, rows, lanes = terms.shape
    lane = lax.broadcasted_iota(jnp.int32, (rows, lanes), 1)
    sides = jnp.logical_or(lane == 0, lane == lanes - 1)
    for t in which:
        for k in range(levels):
            term = pltpu.roll(terms[k], (lanes - 2 * t) % lanes, 1)
            place = pl.ds((t * levels + k) * rows, rows)
            dst[place, :] = src[place, :] + jnp.where(sides, term, 0.0)


def kernel(sizes, x_ref, kmt_ref, out_ref, add_ref, tab_ref, halo2, *scratch):
    pl.run_scoped(
        functools.partial(body, sizes, x_ref, kmt_ref, out_ref, add_ref, tab_ref, halo2, *scratch),
        pltpu.SemaphoreType.DMA((len(sizes[-1]) + 1,)),
        pltpu.SemaphoreType.DMA((5,)),
    )


def body(
    sizes, x_ref, kmt_ref, out_ref, add_ref, tab_ref, halo2,
    xv, kmt_int, coef, wcol, ecol, inner_w, inner_e, relay, halo0, halo1, from_n, from_s,
    recv_sem, load_sem, send_sem,
):
    tracers, levels, rows, lanes, n_lon, n_lat, groups = sizes
    lon, lat = lax.axis_index("lon"), lax.axis_index("lat")
    at_top = lat == n_lat - 1
    below_top = jnp.logical_not(at_top)
    inner = lat > 0
    at_bottom = jnp.logical_not(inner)
    even_lat = jnp.logical_and(inner, jnp.logical_and(lat % 2 == 0, below_top))
    odd_lat = jnp.logical_and(lat > 1, lat % 2 == 1)
    relayed = jnp.logical_and(lon == 0, even_lat)
    relays = jnp.logical_and(lon == 0, odd_lat)
    far = jnp.logical_and(lon == n_lon - 1, even_lat)
    direct, near = jnp.logical_not(relayed), jnp.logical_not(far)
    early = jnp.logical_and(lon == 0, direct)
    late = jnp.logical_not(early)
    late_top, late_below = jnp.logical_and(late, at_top), jnp.logical_and(late, below_top)
    urgent = jnp.logical_and(jnp.logical_and(late_below, lon == n_lon - 1), lat % 2 == 0)
    patient = jnp.logical_and(late_below, jnp.logical_not(urgent))
    e_dev = (lax.rem(lon + 1, n_lon), lat)
    w_dev = (lax.rem(lon + n_lon - 1, n_lon), lat)
    n_dev, s_dev = (lon, lat + 1), (lon, lat - 1)
    lat_up, lat_down = lax.rem(lat + 1, n_lat), lax.rem(lat + n_lat - 1, n_lat)
    fold_dev = (n_lon - 1 - lon, lat)
    tiles = tracers * levels
    plane = levels * rows
    lead = levels
    ends = [sum(groups[:i]) for i in range(len(groups) + 1)]
    splits = (0, *ends[2:])
    split = splits[1]
    slots, pers, shares = layout(splits, levels, lanes)
    firsts = [sum(shares[:n]) for n in range(3)]
    kmt_at = pers[0] * slots[0]

    load_kmt = pltpu.make_async_copy(kmt_ref, kmt_int, load_sem.at[len(groups)])
    load_kmt.start()

    def load(first, count, i):
        return pltpu.make_async_copy(
            x_ref.at[pl.ds(first, count)], xv.at[pl.ds(lead + first, count)], load_sem.at[i]
        )

    for i in range(len(groups)):
        for t in range(ends[i], ends[i + 1]):
            load(t * levels, levels, i).start()
    loads = [load(ends[i] * levels, groups[i] * levels, i) for i in range(len(groups))]
    flat = xv.reshape((lead + tiles) * rows, lanes)

    barrier = pltpu.get_barrier_semaphore()

    def greet(dev):
        pl.semaphore_signal(barrier, inc=1, device_id=dev, device_id_type=MESH)

    with jax.named_scope("greet"):
        greet(w_dev)

        @pl.when(near)
        def _():
            greet(e_dev)

        @pl.when(far)
        def _():
            greet((0, lat_up))

        @pl.when(at_top)
        def _():
            greet(fold_dev)

        @pl.when(below_top)
        def _():
            greet(n_dev)

        @pl.when(inner)
        def _():
            greet(s_dev)

    lane = lax.broadcasted_iota(jnp.int32, (rows, lanes), 1)
    row = lax.broadcasted_iota(jnp.int32, (rows, lanes), 0)

    def send(src, dst, s, r, dev):
        return pltpu.make_async_remote_copy(
            src_ref=src, dst_ref=dst, send_sem=send_sem.at[s], recv_sem=recv_sem.at[r],
            device_id=dev, device_id_type=MESH,
        )

    def rows_of(r, span, dst, s, into, dev):
        return send(xv.at[span, r, :], dst.at[span], s, into, dev)

    cut = lead + ends[-2] * levels
    starts = [lead - 1] + [lead + e * levels for e in ends[1:]]
    spans = [pl.ds(a, b - a) for a, b in zip(starts, starts[1:])]
    every = pl.ds(lead - 1, tiles + 1)
    halves = [(pl.ds(lead - 1, cut - lead + 1), 0), (spans[-1], 5)]
    fold = rows_of(rows - 1, every, from_n, 0, 0, fold_dev)
    folds = [
        rows_of(rows - 1, span, from_n, 0, 5 if i == len(spans) - 1 else 0, fold_dev)
        for i, span in enumerate(spans)
    ]
    to_n = rows_of(rows - 1, every, from_s, 0, 1, n_dev)
    to_s = rows_of(0, every, from_n, 1, 0, s_dev)
    to_ss = [rows_of(0, span, from_n, 1, r, s_dev) for span, r in halves]
    cols = [pl.ds(f * rows, n * rows) for f, n in zip(firsts, shares)]
    halos = (halo0, halo1, halo2)
    wests = [h.at[pl.ds(0, n * rows)] for h, n in zip(halos, shares)]
    easts = [h.at[pl.ds(n * rows, n * rows)] for h, n in zip(halos, shares)]
    arrive = (2, 3, 6)
    far_dev = (n_lon - 1, lat_down)
    to_e = [send(ecol.at[c], wests[i], 2, arrive[i], e_dev) for i, c in enumerate(cols)]
    to_w = [send(wcol.at[c], easts[i], 3, arrive[i], w_dev) for i, c in enumerate(cols)]
    onward = [send(relay.at[c], easts[i], 4, arrive[i], far_dev) for i, c in enumerate(cols)]
    to_relay = send(wcol, relay, 3, 4, (lon, lat_up))
    got = [send(h, h, 2, r, e_dev) for h, r in zip(halos, arrive)]
    all_e, all_w, all_onward = (send(c, relay, s, 4, e_dev) for c, s in ((ecol, 2), (wcol, 3), (relay, 4)))

    def tile(t, k):
        return flat[pl.ds(lead * rows + t * plane + k * rows, rows), :]

    def density(k):
        return HALINE * tile(1, k) - THERMAL * tile(0, k)

    def where_is(t, k):
        n = sum(t >= s for s in splits[1:])
        return k % pers[n] * slots[n] + t - splits[n], firsts[n] + k // pers[n]

    def gather_columns(e_ref, w_ref, e_off, w_off, before=None, after=None):
        zeros = jnp.zeros((rows, lanes), jnp.float32)
        es, ws = [zeros] * sum(shares), [zeros] * sum(shares)

        def place(value, at, reg):
            value = pltpu.roll(value, at + 1, 1)
            es[reg] = jnp.where(lane == (at + e_off) % lanes, value, es[reg])
            ws[reg] = jnp.where(lane == (at + w_off) % lanes, value, ws[reg])

        for i in range(len(groups)):
            if before is not None:
                before(i)
            if i == 0:
                place(kmt_own, kmt_at, 0)
                for k in range(levels):
                    at, reg = where_is(0, k)
                    place(density(k), at + split, reg)
            for t in range(ends[i], ends[i + 1]):
                for k in range(levels):
                    place(tile(t, k), *where_is(t, k))
            if ends[i + 1] in splits:
                n = splits.index(ends[i + 1]) - 1
                for j in range(firsts[n], firsts[n] + shares[n]):
                    e_ref[pl.ds(j * rows, rows), :] = es[j]
                    w_ref[pl.ds(j * rows, rows), :] = ws[j]
                if after is not None:
                    after(n)

    def enter():
        @pl.when(at_bottom)
        def _():
            pl.semaphore_wait(barrier, 3)

        @pl.when(jnp.logical_and(inner, jnp.logical_not(jnp.logical_or(relayed, relays))))
        def _():
            pl.semaphore_wait(barrier, 4)

        @pl.when(relayed)
        def _():
            pl.semaphore_wait(barrier, 3)

        @pl.when(relays)
        def _():
            pl.semaphore_wait(barrier, 5)

    def send_inner_rows():
        @pl.when(below_top)
        def _():
            to_n.start()

        @pl.when(inner)
        def _():
            for copy in to_ss:
                copy.start()

    def before(i):
        with jax.named_scope(f"load{i}"):
            loads[i].wait()
        if i == 0:

            @pl.when(late_top)
            def _():
                enter()

        if i < len(groups) - 1:

            @pl.when(late_top)
            def _():
                folds[i].start()

    def send_part(n, who):
        @pl.when(who)
        def _():
            to_e[n].start()

        @pl.when(jnp.logical_and(who, direct))
        def _():
            to_w[n].start()

    def after(n):
        if n < 2:

            @pl.when(patient if n else urgent)
            def _():
                with jax.named_scope("barrier"):
                    enter()

        if n == 1:
            send_part(0, patient)
        send_part(n, late if n else jnp.logical_and(late, jnp.logical_not(patient)))

    with jax.named_scope("loadk"):
        load_kmt.wait()
    kmt_own = kmt_int[...].astype(jnp.float32)
    xv[lead - 1, :, :] = kmt_own
    gather_columns(ecol, wcol, 0, 1, before, after)
    with jax.named_scope("send"):

        @pl.when(relayed)
        def _():
            to_relay.start()

        @pl.when(late_top)
        def _():
            folds[-1].start()

        @pl.when(late)
        def _():
            send_inner_rows()

    with jax.named_scope("inner"):
        gather_columns(inner_e, inner_w, -1, 2)

        @pl.when(at_bottom)
        def _():
            for t in range(tracers + 1):
                from_s[pl.ds(t * levels, levels), :] = jnp.zeros((levels, lanes), jnp.float32)

    def put(d, dk, k, value):
        coef[pl.ds(((d * 3 + dk) * levels + k) * rows, rows), :] = value

    def piece_of(d, dk, k):
        return coef[pl.ds(((d * 3 + dk) * levels + k) * rows, rows), :]

    with jax.named_scope("coefs"):
        def shifted(v, by, axis):
            return jnp.stack([pltpu.roll(v[k], by, axis) for k in range(levels)])

        own_rho = jnp.stack([density(k) for k in range(levels)])
        own_wet = jnp.stack([(kmt_own > float(k)).astype(jnp.float32) for k in range(levels)])
        c3 = column(own_rho, own_wet, up3, dn3)

        def moved(by, axis):
            return tuple(shifted(v, by, axis) for v in c3)

        mid_lane = jnp.logical_and(lane > 0, lane < lanes - 1)
        xc, xe, xw = line(c3, moved(lanes - 1, 1), moved(1, 1), up3, dn3)
        for dk in range(3):
            for k in range(levels):
                put(E, dk, k, jnp.where(mid_lane, xe[dk][k], 0.0))
                put(W, dk, k, jnp.where(mid_lane, xw[dk][k], 0.0))
                put(C, dk, k, jnp.where(mid_lane, xc[dk][k], 0.0))
        mid_row = jnp.logical_and(row > 0, row < rows - 1)
        yc, yn, ys = line(c3, moved(rows - 1, 0), moved(1, 0), up3, dn3)
        for dk in range(3):
            for k in range(levels):
                put(N, dk, k, jnp.where(mid_row, yn[dk][k], 0.0))
                put(S, dk, k, jnp.where(mid_row, ys[dk][k], 0.0))
                core = piece_of(C, dk, k) + jnp.where(mid_row, yc[dk][k], 0.0)
                put(C, dk, k, core + 1.0 if dk == 1 else core)

    with jax.named_scope("main"):

        @pl.loop(0, tracers // TOGETHER)
        def _(i):
            fields = []
            for u in range(TOGETHER):
                base = pl.multiple_of(lead * rows + (i * TOGETHER + u) * plane, rows)
                field = []
                for k in range(levels):
                    own = flat[pl.ds(base + k * rows, rows), :]
                    field.append((
                        own, pltpu.roll(own, lanes - 1, 1), pltpu.roll(own, 1, 1),
                        pltpu.roll(own, rows - 1, 0), pltpu.roll(own, 1, 0),
                    ))
                fields.append(field)
            for k in range(levels):
                sums = [None] * TOGETHER
                for d in range(5):
                    for dk in range(3):
                        if not 0 <= k + dk - 1 < levels:
                            continue
                        c = piece_of(d, dk, k)
                        for u in range(TOGETHER):
                            term = c * fields[u][k + dk - 1][d]
                            sums[u] = term if sums[u] is None else sums[u] + term
                for u in range(TOGETHER):
                    base = pl.multiple_of((i * TOGETHER + u) * plane, rows)
                    out_ref[pl.ds(base + k * rows, rows), :] = sums[u]

    @pl.when(early)
    def _():
        with jax.named_scope("barrier"):
            enter()
        for copy in to_e + to_w:
            copy.start()
        send_inner_rows()

        @pl.when(at_top)
        def _():
            for copy in folds:
                copy.start()

    @pl.when(relays)
    def _():
        to_relay.wait_recv()
        for copy in onward:
            copy.start()

    level = lax.broadcasted_iota(jnp.int32, (levels, lanes), 0)
    level_f = level.astype(jnp.float32)

    def up_s(v):
        return jnp.where(level == 0, 0.0, pltpu.roll(v, 1, 0))

    def dn_s(v):
        return jnp.where(level == levels - 1, 0.0, pltpu.roll(v, levels - 1, 0))

    def at_row(t, r):
        return flat[pl.ds(lead * rows + t * plane + r, levels, stride=rows), :]

    def row_column(t0, t1, kmt):
        wet = (jnp.broadcast_to(kmt, (levels, lanes)) > level_f).astype(jnp.float32)
        return column(HALINE * t1 - THERMAL * t0, wet, up_s, dn_s)

    def own_row(r):
        return row_column(at_row(0, r), at_row(1, r), kmt_own[r : r + 1, :])

    def fix_rows(source, r, r_in, north, turn, parts):
        def halo(t):
            h = source[pl.ds(lead + t * levels, levels), :]
            return pick(h, lanes - 1 - lane) if turn else h

        first, last, wait = parts[0]
        wait()
        k = jnp.broadcast_to(source[pl.ds(lead - 1, 1), :], (rows, lanes))
        k = (pick(k, lanes - 1 - lane) if turn else k)[:1, :]
        out_c, in_c = row_column(halo(0), halo(1), k), own_row(r_in)
        p, m = (out_c, in_c) if north else (in_c, out_c)
        cc, cp, cm = line(own_row(r), p, m, up_s, dn_s)
        c_out, c_in = (cp, cm) if north else (cm, cp)
        table = (cc, c_out, c_in)
        lo = [pltpu.roll(c[0], levels - 1, 0) for c in table]
        mid = [c[1] for c in table]
        hi = [pltpu.roll(c[2], 1, 0) for c in table]
        for n, (first, last, wait) in enumerate(parts):
            if n:
                wait()
            count = last - first
            batch = count if turn else next(b for b in (8, 5, 4, 3, 2, 1) if count % b == 0)

            @pl.loop(0, count // batch)
            def _(i, first=first, batch=batch):
                for u in range(batch):
                    t = first + i * batch + u
                    values = (at_row(t, r), halo(t), at_row(t, r_in))
                    above = total([c * v for c, v in zip(lo, values)])
                    same = total([c * v for c, v in zip(mid, values)])
                    below = total([c * v for c, v in zip(hi, values)])
                    place = pl.ds(t * plane + r, levels, stride=rows)
                    out_ref[place, :] = (
                        out_ref[place, :] + same + pltpu.roll(above, 1, 0) + pltpu.roll(below, levels - 1, 0)
                    )

    def fix_n(turn):
        parts = [(0, ends[-2], to_ss[0].wait_recv), (ends[-2], tracers, to_ss[1].wait_recv)]
        fix_rows(from_n, rows - 1, rows - 2, True, turn, parts)

    with jax.named_scope("fixs"):

        @pl.when(inner)
        def _():
            to_n.wait_recv()

        fix_rows(from_s, 0, 1, False, False, [(0, tracers, lambda: None)])

    with jax.named_scope("fixn"):

        @pl.when(below_top)
        def _():
            fix_n(False)

    spot = tracer_of(lane, lanes, tracers)

    def part_of(refs, offs, n, first=None):
        at = jnp.clip(spot - splits[n], 0, splits[n + 1] - splits[n] - 1)
        return values_of(refs, offs, at, pers[n], slots[n], firsts[n] if first is None else first, levels)

    def column_of(refs, offs):
        fixed = jnp.zeros((rows, lanes), jnp.int32)
        rho = jnp.stack([both(refs, offs, fixed + (where_is(0, k)[0] + split), where_is(0, k)[1])
                         for k in range(levels)])
        kmt = both(refs, offs, fixed + kmt_at, 0)
        wet = jnp.stack([(kmt > float(k)).astype(jnp.float32) for k in range(levels)])
        return column(rho, wet, up3, dn3)

    def joined(*args):
        a, b, c = (part_of(*args, n) for n in range(3))
        return jnp.stack([
            jnp.where(spot < splits[1], a[k], jnp.where(spot < splits[2], b[k], c[k])) for k in range(levels)
        ])

    with jax.named_scope("fixc0"):
        own_at, ins_at, outs_at = ((wcol, ecol), (1, 0)), ((inner_w, inner_e), (2, -1)), ((wests[0], easts[0]), (0, 1))
        own_c, ins_c = column_of(*own_at), column_of(*ins_at)
        own, ins = joined(*own_at), joined(*ins_at)
    with jax.named_scope("waitc"):
        got[0].wait_recv()
    with jax.named_scope("fixc1"):
        own_t, outs_t, ins_t = line(own_c, column_of(*outs_at), ins_c, up3, dn3)
        some = applied(own_t, own) + applied(ins_t, ins)
        full = some + applied(outs_t, part_of(*outs_at, 0))
    with jax.named_scope("waitc1"):
        got[1].wait_recv()
    with jax.named_scope("insert0"):
        more = some + applied(outs_t, part_of((wests[1], easts[1]), (0, 1), 1, 0))
        insert_tiles(range(split), full, out_ref, out_ref)
        for k in range(levels):
            add_ref[pl.ds(k * rows, rows), :] = more[k]
            add_ref[pl.ds((levels + k) * rows, rows), :] = some[k]
            for dk in range(3):
                tab_ref[pl.ds((dk * levels + k) * rows, rows), :] = outs_t[dk][k]

    with jax.named_scope("fixtop"):

        @pl.when(at_top)
        def _():
            fix_n(True)

    with jax.named_scope("end"):
        fold.wait_send()

        @pl.when(inner)
        def _():
            to_s.wait_send()

        all_e.wait_send()
        all_w.wait_send()

        @pl.when(relays)
        def _():
            all_onward.wait_send()

    with jax.named_scope("waitc2"):
        got[2].wait_recv()


def finish(sizes, part_ref, add_ref, tab_ref, halo_ref, out_ref, stage, sem):
    tracers, levels, rows, lanes, splits = sizes
    plane = levels * rows
    slots, pers, shares = layout(splits, levels, lanes)
    lane = lax.broadcasted_iota(jnp.int32, (rows, lanes), 1)
    spot = tracer_of(lane, lanes, tracers)
    half = shares[2] * rows

    def write(ref, first, count):
        span = pl.ds(pl.multiple_of(first * plane, plane), count * plane)
        pltpu.make_async_copy(ref.at[span], out_ref.at[span], sem).start()

    def eight(ref, n):
        return jnp.stack([ref[pl.ds((n * levels + k) * rows, rows), :] for k in range(levels)])

    def last_terms():
        refs = [halo_ref.at[pl.ds(i * half, half)] for i in range(2)]
        at = jnp.clip(spot - splits[2], 0, splits[3] - splits[2] - 1)
        values = values_of(refs, (0, 1), at, pers[2], slots[2], 0, levels)
        return eight(add_ref, 1) + applied([eight(tab_ref, dk) for dk in range(3)], values)

    with jax.named_scope("insert"):
        ready = splits[1] // 2

        @pl.loop(0, 2)
        def _(i):
            write(part_ref, i * ready, ready)

        terms = [eight(add_ref, 0), None]
        for n in (1, 2):
            for t in range(splits[n], splits[n + 1], STORE):
                last = min(t + STORE, splits[n + 1])
                insert_tiles(range(t, last), terms[n - 1], part_ref, stage)
                write(stage, t, last - t)
                if terms[1] is None:
                    terms[1] = last_terms()
    with jax.named_scope("written"):
        pltpu.make_async_copy(stage, out_ref, sem).wait()


def solution(mesh):
    n_lon, n_lat = mesh.shape["lon"], mesh.shape["lat"]

    def local(tracers, kmt):
        nt, levels, rows, lanes = tracers.shape
        tiles = nt * levels
        most = (lanes - 2) // levels
        split = max(nt - most, nt // 2)
        cuts = (0, split // 6, min(split // 2, max(most - 2, 2)), split, nt)
        splits = (0, *cuts[2:])
        groups = tuple(b - a for a, b in zip(cuts, cuts[1:]))
        shares = layout(splits, levels, lanes)[-1]
        regs = sum(shares)
        assert levels == rows and groups[0] > 1 and cuts[2] % 2 == 0 and lanes & (lanes - 1) == 0

        def vmem(*shape):
            return pltpu.VMEM(shape, jnp.float32)

        parts = pl.pallas_call(
            functools.partial(kernel, (nt, levels, rows, lanes, n_lon, n_lat, groups)),
            out_shape=[
                vmem(tiles * rows, lanes),
                vmem(2 * levels * rows, lanes),
                vmem(3 * levels * rows, lanes),
                vmem(2 * shares[2] * rows, lanes),
            ],
            in_specs=[pl.BlockSpec(memory_space=pltpu.HBM), pl.BlockSpec(memory_space=pltpu.HBM)],
            out_specs=[pl.BlockSpec(memory_space=pltpu.VMEM)] * 4,
            scratch_shapes=[
                vmem(tiles + levels, rows, lanes),
                pltpu.VMEM((rows, lanes), jnp.int32),
                vmem(15 * levels * rows, lanes),
            ]
            + [vmem(regs * rows, lanes)] * 5
            + [vmem(2 * n * rows, lanes) for n in shares[:2]]
            + [vmem(tiles + rows, lanes)] * 2
            + [
                pltpu.SemaphoreType.DMA((7,)),
            ],
            compiler_params=pltpu.CompilerParams(collective_id=0, has_side_effects=True),
        )(tracers.reshape(tiles, rows, lanes), kmt)
        parts = [pltpu.with_memory_space_constraint(v, pltpu.VMEM) for v in parts]
        out = pl.pallas_call(
            functools.partial(finish, (nt, levels, rows, lanes, splits)),
            out_shape=jax.ShapeDtypeStruct((tiles * rows, lanes), jnp.float32),
            in_specs=[pl.BlockSpec(memory_space=pltpu.VMEM)] * 4,
            out_specs=pl.BlockSpec(memory_space=pltpu.HBM),
            scratch_shapes=[vmem(tiles * rows, lanes), pltpu.SemaphoreType.DMA],
        )(*parts)
        return out.reshape(nt, levels, rows, lanes)

    return jax.shard_map(
        local,
        mesh=mesh,
        in_specs=(P(None, None, "lat", "lon"), P("lat", "lon")),
        out_specs=P(None, None, "lat", "lon"),
        check_vma=False,
    )
```
